32 devices in a mesh: seq: 8 (over y, x, core), wshard: 4 (over z).
Axes of the slice: x: 2, y: 2, z: 4, core: 2. Of those that a mesh axis runs over, the one named last changes fastest.
Arguments:
- block_in: bfloat16 [4, 2048, 1536], P('wshard', 'seq'), may hold values from -6 to 6
- cotangent: bfloat16 [4, 2048, 1536], P('wshard', 'seq'), may hold values from -6 to 6
- in_weight: float32 [1536, 6448], P(('seq', 'wshard')), may hold values from -0.15625 to 0.15625
- out_weight: float32 [3072, 1536], P(('seq', 'wshard')), may hold values from -0.109375 to 0.109375
- in_gain: float32 [1536], replicated, may hold values from 0.5 to 1.5
- out_gain: float32 [3072], replicated, may hold values from 0.5 to 1.5
- conv_inner: float32 [5, 3072], replicated, may hold values from -3 to 3
- conv_shared: float32 [5, 256], replicated, may hold values from -3 to 3
- head_params: float32 [3, 48], replicated, may hold values from -5 to 1.5, as said below
- first_in_weight: float32 [1536, 6448], P(('seq', 'wshard')), may hold values from -6 to 6
- first_out_weight: float32 [3072, 1536], P(('seq', 'wshard')), may hold values from -6 to 6
- first_in_gain: float32 [1536], replicated, may hold values from -6 to 6
- first_out_gain: float32 [3072], replicated, may hold values from -6 to 6
- first_conv_inner: float32 [5, 3072], replicated, may hold values from -6 to 6
- first_conv_shared: float32 [5, 256], replicated, may hold values from -6 to 6
- first_head_params: float32 [3, 48], replicated, may hold values from -6 to 6
- second_in_weight: float32 [1536, 6448], P(('seq', 'wshard')), may hold values from 0.01 to 1
- second_out_weight: float32 [3072, 1536], P(('seq', 'wshard')), may hold values from 0.01 to 1
- second_in_gain: float32 [1536], replicated, may hold values from 16.384 to 1638.4
- second_out_gain: float32 [3072], replicated, may hold values from 0.01 to 1
- second_conv_inner: float32 [5, 3072], replicated, may hold values from 0.01 to 1
- second_conv_shared: float32 [5, 256], replicated, may hold values from 0.01 to 1
- second_head_params: float32 [3, 48], replicated, may hold values from 0.01 to 1
Outputs:
- block_out: float32 [4, 2048, 1536], P('wshard', 'seq')
- grad_in: float32 [4, 2048, 1536], P('wshard', 'seq')
- grad_in_weight: float32 [1536, 6448], P(('seq', 'wshard'))
- grad_out_weight: float32 [3072, 1536], P(('seq', 'wshard'))
- grad_in_gain: float32 [1536], replicated
- grad_out_gain: float32 [3072], replicated
- grad_conv_inner: float32 [5, 3072], replicated
- grad_conv_shared: float32 [5, 256], replicated
- grad_head_params: float32 [3, 48], replicated
- new_in_weight: float32 [1536, 6448], P(('seq', 'wshard'))
- new_out_weight: float32 [3072, 1536], P(('seq', 'wshard'))
- updated_input_gain: float32 [1536], replicated
- new_out_gain: float32 [3072], replicated
- new_conv_inner: float32 [5, 3072], replicated
- new_conv_shared: float32 [5, 256], replicated
- new_head_params: float32 [3, 48], replicated
- new_first_in_weight: float32 [1536, 6448], P(('seq', 'wshard'))
- new_first_out_weight: float32 [3072, 1536], P(('seq', 'wshard'))
- new_first_in_gain: float32 [1536], replicated
- new_first_out_gain: float32 [3072], replicated
- new_first_conv_inner: float32 [5, 3072], replicated
- new_first_conv_shared: float32 [5, 256], replicated
- updated_head_first_moment: float32 [3, 48], replicated
- new_second_in_weight: float32 [1536, 6448], P(('seq', 'wshard'))
- new_second_out_weight: float32 [3072, 1536], P(('seq', 'wshard'))
- new_second_in_gain: float32 [1536], replicated
- new_second_out_gain: float32 [3072], replicated
- new_second_conv_inner: float32 [5, 3072], replicated
- new_second_conv_shared: float32 [5, 256], replicated
- new_second_head_params: float32 [2, 48], replicated
- new_second_skip: float32 [48], replicated
The draws below stay inside these ranges and needn't reach their ends.
Inputs may be any that keep to these rules, and one draw needn't show every extreme that they name: `head_params`: row 0 holds step biases, row 1 logarithms of decay rates, row 2 skip gains.
All inputs are finite; a program needn't handle non-finite values.
Results may differ from the reference program's by a relative error of at most 0.02.
The reference program's roundings to bfloat16 on the way count: a program that leaves them out, or rounds other values in their place, can miss the bound.
Values may be sent and summed in bfloat16 or wider, within the bound.
A program may use at most 256 MiB of HBM per device.

```python
import math
import jax
import jax.numpy as jnp
from jax import lax

D = 1536
H = 48
P_SIZE = 64
N_STATE = 128
BLOCK_LEN = 256
E = 3072
PROJ = 6448
SEQS = 4
L = 2048
N_SEQ = 8


def draw_head_params(key, part):
    keys = jax.random.split(key, 3)
    biases = jax.random.uniform(keys[0], (H,), jnp.float32, -4.5, -1.5)
    rates = jax.random.uniform(keys[1], (H,), jnp.float32, -4.6, 0.69)
    skips = jax.random.uniform(keys[2], (H,), jnp.float32, 0.5, 1.5)
    return jnp.stack([biases, rates, skips])


def level_of(stream_key, shape, shards, low, top_value):
    def one(dim, blocks):
        steps = jax.random.uniform(jax.random.fold_in(jax.random.fold_in(stream_key, 6), dim), (blocks,), jnp.float32, low / len(shards), top_value / len(shards))
        return jnp.repeat(jnp.exp(steps), shape[dim] // blocks).reshape((-1,) + (1,) * (len(shape) - dim - 1))

    level = one(*shards[0])
    for cut in shards[1:]:
        level = level * one(*cut)
    return level


def gaussian(own_key, extent, scale, most, shards=(), held_as=jnp.bfloat16):
    entries = scale * jax.random.normal(own_key, extent, jnp.float32)
    if shards:
        entries = entries * level_of(own_key, extent, shards, -0.22, 0.18)
    return jnp.clip(entries, -most, most).astype(held_as)


def setup_inputs(seed: int = 0) -> dict:
    key_list = jax.random.split(jax.random.key(seed), 24)
    return {
        "block_in": gaussian(key_list[0], (SEQS, L, D), 1.0, 6.0, ((0, 4), (1, 8))),
        "cotangent": gaussian(key_list[1], (SEQS, L, D), 1.0, 6.0, ((0, 4), (1, 8))),
        "in_weight": gaussian(key_list[2], (D, PROJ), D ** -0.5, 0.15625, ((0, 32),), jnp.float32),
        "out_weight": gaussian(key_list[3], (E, D), E ** -0.5, 0.109375, ((0, 32),), jnp.float32),
        "in_gain": jnp.clip(1.0 + 0.1 * jax.random.normal(key_list[4], (D,), jnp.float32), 0.5, 1.5),
        "out_gain": jnp.clip(1.0 + 0.1 * jax.random.normal(key_list[5], (E,), jnp.float32), 0.5, 1.5),
        "conv_inner": gaussian(key_list[6], (5, E), 4 ** -0.5, 3.0, (), jnp.float32),
        "conv_shared": gaussian(key_list[7], (5, 2 * N_STATE), 4 ** -0.5, 3.0, (), jnp.float32),
        "head_params": draw_head_params(jax.random.fold_in(key_list[23], 71), 0),
        "first_in_weight": gaussian(key_list[9], (D, PROJ), 1.0, 6.0, ((0, 32),), jnp.float32),
        "first_out_weight": gaussian(key_list[10], (E, D), 1.0, 6.0, ((0, 32),), jnp.float32),
        "first_in_gain": gaussian(key_list[11], (D,), 1.0, 6.0, (), jnp.float32),
        "first_out_gain": gaussian(key_list[12], (E,), 1.0, 6.0, (), jnp.float32),
        "first_conv_inner": gaussian(key_list[13], (5, E), 1.0, 6.0, (), jnp.float32),
        "first_conv_shared": gaussian(key_list[14], (5, 2 * N_STATE), 1.0, 6.0, (), jnp.float32),
        "first_head_params": gaussian(key_list[15], (3, H), 1.0, 6.0, (), jnp.float32),
        "second_in_weight": jnp.clip(jnp.exp(math.log(1.0) - 4.6051702 * jax.random.uniform(key_list[16], (D, PROJ), jnp.float32) ** level_of(key_list[16], (D, PROJ), ((0, 32),), -0.2, 0.2)), 0.01, 1.0),
        "second_out_weight": jnp.clip(jnp.exp(math.log(1.0) - 4.6051702 * jax.random.uniform(key_list[17], (E, D), jnp.float32) ** level_of(key_list[17], (E, D), ((0, 32),), -0.2, 0.2)), 0.01, 1.0),
        "second_in_gain": jnp.clip(jnp.exp(jax.random.uniform(key_list[18], (D,), jnp.float32, math.log(16.384), math.log(1638.4))), 16.384, 1638.4),
        "second_out_gain": jnp.clip(jnp.exp(jax.random.uniform(key_list[19], (E,), jnp.float32, math.log(0.01), math.log(1.0))), 0.01, 1.0),
        "second_conv_inner": jnp.clip(jnp.exp(jax.random.uniform(key_list[20], (5, E), jnp.float32, math.log(0.01), math.log(1.0))), 0.01, 1.0),
        "second_conv_shared": jnp.clip(jnp.exp(jax.random.uniform(key_list[21], (5, 2 * N_STATE), jnp.float32, math.log(0.01), math.log(1.0))), 0.01, 1.0),
        "second_head_params": jnp.clip(jnp.exp(jax.random.uniform(key_list[22], (3, H), jnp.float32, math.log(0.01), math.log(1.0))), 0.01, 1.0),
    }


norm_eps = 1e-05
beta_one = 0.9
beta_two = 0.95
adam_eps = 1e-08
adam_step = 3.0
weight_learning_rate = 0.01
matrix_decay = 0.1
small_rate = 0.1

def causal_conv(values, taps):
    length = values.shape[1]
    width = taps.shape[0] - 1
    padded = jnp.pad(values, ((0, 0), (width - 1, 0), (0, 0)))
    total = taps[width] + taps[0] * padded[:, 0:length]
    for shift in range(1, width):
        total = total + taps[shift] * padded[:, shift:shift + length]
    return total

def block_step(state, inputs):
    inner_part, step_part, learning_rate_piece, b_part, c_part = inputs
    high = lax.Precision.HIGHEST
    cumul = jnp.cumsum(learning_rate_piece, axis=1)
    scores = jnp.einsum('sin,sjn->sij', c_part, b_part, precision=high)
    rows = lax.broadcasted_iota(jnp.int32, (BLOCK_LEN, BLOCK_LEN), 0)
    cols = lax.broadcasted_iota(jnp.int32, (BLOCK_LEN, BLOCK_LEN), 1)
    lower = (rows >= cols)[None, :, :, None]
    spread = cumul[:, :, None, :] - cumul[:, None, :, :]
    decay = jnp.where(lower, jnp.exp(jnp.where(lower, spread, 0.0)), 0.0)
    weights = scores[..., None] * decay * step_part[:, None, :, :]
    within = jnp.einsum('sijh,sjhp->sihp', weights, inner_part, precision=high)
    carried = jnp.einsum('sin,shpn->sihp', c_part, state, precision=high) * jnp.exp(cumul)[..., None]
    tail = jnp.exp(cumul[:, -1:, :] - cumul) * step_part
    fresh = jnp.einsum('sjn,sjh,sjhp->shpn', b_part, tail, inner_part, precision=high)
    new_state = jnp.exp(cumul[:, -1, :])[:, :, None, None] * state + fresh
    return (new_state, within + carried)

def state_space(inner, step, rate, b_mat, c_mat):
    batch, length, heads, head_size = inner.shape
    blocks = length // BLOCK_LEN

    def blockify(values):
        return jnp.moveaxis(values.reshape((batch, blocks, BLOCK_LEN) + values.shape[2:]), 1, 0)
    start = jnp.zeros((batch, heads, head_size, b_mat.shape[2]), dtype=inner.dtype)
    _, outputs = lax.scan(jax.checkpoint(block_step), start, (blockify(inner), blockify(step), blockify(rate), blockify(b_mat), blockify(c_mat)))
    return jnp.moveaxis(outputs, 0, 1).reshape(batch, length, heads, head_size)

def mixer(gate_inner, shared, step_raw, conv_local, conv_common, head_local):
    batch, length = (gate_inner.shape[0], gate_inner.shape[1])
    heads = step_raw.shape[2]
    parts = gate_inner.reshape(batch, length, heads, 2, P_SIZE)
    gate_vals = parts[:, :, :, 0, :].reshape(batch, length, heads * P_SIZE)
    inner_vals = parts[:, :, :, 1, :].reshape(batch, length, heads * P_SIZE)
    inner_act = jax.nn.silu(causal_conv(inner_vals, conv_local))
    shared_act = jax.nn.silu(causal_conv(shared, conv_common))
    half = shared.shape[2] // 2
    step = jax.nn.softplus(step_raw + head_local[0])
    rate = -step * jnp.exp(head_local[1])
    inner_heads = inner_act.reshape(batch, length, heads, P_SIZE)
    output = state_space(inner_heads, step, rate, shared_act[..., :half], shared_act[..., half:])
    output = output + head_local[2][:, None] * inner_heads
    return output.reshape(batch, length, heads * P_SIZE) * jax.nn.silu(gate_vals)

def adamw(param, grad, first, second_moment, rate, decay):
    first_new = beta_one * first + (1.0 - beta_one) * grad
    second_new = beta_two * second_moment + (1.0 - beta_two) * grad * grad
    corrected = first_new / (1.0 - beta_one ** adam_step) / (jnp.sqrt(second_new / (1.0 - beta_two ** adam_step)) + adam_eps)
    return (param - rate * (corrected + decay * param), first_new, second_new)

def reference(block_in, cotangent, in_weight, out_weight, in_gain, out_gain, conv_inner, conv_shared, head_params, first_in_weight, first_out_weight, first_in_gain, first_out_gain, first_conv_inner, first_conv_shared, first_head_params, second_in_weight, second_out_weight, second_in_gain, second_out_gain, second_conv_inner, second_conv_shared, second_head_params):
    in_w16 = in_weight.astype(jnp.bfloat16)
    out_w16 = out_weight.astype(jnp.bfloat16)
    heads_dev = H // N_SEQ
    group_ids = jnp.arange(N_SEQ, dtype=jnp.int32)

    def one_sequence(totals, item):
        seq_in, seq_cot = item
        inputs = seq_in.astype(jnp.float32)
        rms_in = lax.rsqrt(lax.optimization_barrier(jnp.mean(inputs * inputs, axis=-1, keepdims=True)) + norm_eps)
        normed = (inputs * rms_in * in_gain).astype(jnp.bfloat16)
        projected = jnp.dot(normed, in_w16, preferred_element_type=jnp.float32).astype(jnp.bfloat16)
        gate_inner = projected[:, :2 * E]
        shared = projected[:, 2 * E:2 * E + 2 * N_STATE].astype(jnp.float32)[None]
        step_raw = projected[:, 2 * E + 2 * N_STATE:]

        def group_args(group):
            gate_part = lax.dynamic_slice_in_dim(gate_inner, (group * (heads_dev * 2 * P_SIZE)).astype(jnp.int32), heads_dev * 2 * P_SIZE, 1)
            step_part = lax.dynamic_slice_in_dim(step_raw, (group * heads_dev).astype(jnp.int32), heads_dev, 1)
            conv_part = lax.dynamic_slice_in_dim(conv_inner, (group * (heads_dev * P_SIZE)).astype(jnp.int32), heads_dev * P_SIZE, 1)
            head_part = lax.dynamic_slice_in_dim(head_params, (group * heads_dev).astype(jnp.int32), heads_dev, 1)
            return (gate_part.astype(jnp.float32)[None], shared, step_part.astype(jnp.float32)[None], conv_part, conv_shared, head_part)

        def group_forward(group):
            return mixer(*group_args(group))[0].astype(jnp.bfloat16)
        gated = jnp.transpose(lax.map(group_forward, group_ids), (1, 0, 2)).reshape(L, E)
        gated32 = gated.astype(jnp.float32)
        rms_out = lax.rsqrt(lax.optimization_barrier(jnp.mean(gated32 * gated32, axis=-1, keepdims=True)) + norm_eps)
        gnormed = (gated32 * rms_out * out_gain).astype(jnp.bfloat16)
        mixed = jnp.dot(gnormed, out_w16, preferred_element_type=jnp.float32)
        block_out = inputs + mixed
        d_gnormed = jnp.dot(seq_cot, out_w16.T, preferred_element_type=jnp.float32)
        d_out_gain = lax.optimization_barrier(jnp.sum(d_gnormed * gated32 * rms_out, axis=0))
        scaled = d_gnormed * out_gain
        d_gated = (rms_out * scaled - gated32 * rms_out ** 3 * lax.optimization_barrier(jnp.mean(scaled * gated32, axis=-1, keepdims=True))).astype(jnp.bfloat16)

        def group_backward(group):
            cotan_part = lax.dynamic_slice_in_dim(d_gated, (group * (heads_dev * P_SIZE)).astype(jnp.int32), heads_dev * P_SIZE, 1)
            pullback = jax.vjp(mixer, *group_args(group))[1]
            d_gate, d_shared, d_step, d_conv, d_common, d_head = pullback(cotan_part.astype(jnp.float32)[None])
            return (d_gate[0].astype(jnp.bfloat16), d_shared[0].astype(jnp.bfloat16), d_step[0].astype(jnp.bfloat16), d_conv, d_common, d_head)
        d_gate, d_shared, d_step, d_conv, d_common, d_head = lax.map(group_backward, group_ids)
        d_gate_inner = jnp.transpose(d_gate, (1, 0, 2)).reshape(L, 2 * E)
        d_step_all = jnp.transpose(d_step, (1, 0, 2)).reshape(L, H)
        d_shared_sum = lax.optimization_barrier(jnp.sum(d_shared.astype(jnp.float32), axis=0)).astype(jnp.bfloat16)
        projected_gradient = jnp.concatenate([d_gate_inner, d_shared_sum, d_step_all], axis=1)
        d_normed = jnp.dot(projected_gradient, in_w16.T, preferred_element_type=jnp.float32)
        d_in_gain = lax.optimization_barrier(jnp.sum(d_normed * inputs * rms_in, axis=0))
        scaled_in = d_normed * in_gain
        grad_in = seq_cot.astype(jnp.float32) + rms_in * scaled_in - inputs * rms_in ** 3 * lax.optimization_barrier(jnp.mean(scaled_in * inputs, axis=-1, keepdims=True))
        terms = (jnp.dot(normed.T, projected_gradient, preferred_element_type=jnp.float32), jnp.dot(gnormed.T, seq_cot, preferred_element_type=jnp.float32), d_in_gain, d_out_gain, jnp.transpose(d_conv, (1, 0, 2)).reshape(5, E), lax.optimization_barrier(jnp.sum(d_common, axis=0)), jnp.transpose(d_head, (1, 0, 2)).reshape(3, H))
        totals = tuple((total + term for total, term in zip(totals, terms)))
        return (totals, (block_out, grad_in))
    params = (in_weight, out_weight, in_gain, out_gain, conv_inner, conv_shared, head_params)
    start = tuple((jnp.zeros(param.shape, dtype=jnp.float32) for param in params))
    grads, (block_out, grad_in) = lax.scan(one_sequence, start, (block_in, cotangent))
    new_in_weight, new_first_in_weight, new_second_in_weight = adamw(in_weight, grads[0], first_in_weight, second_in_weight, weight_learning_rate, matrix_decay)
    new_out_weight, new_first_out_weight, new_second_out_weight = adamw(out_weight, grads[1], first_out_weight, second_out_weight, weight_learning_rate, matrix_decay)
    updated_input_gain, new_first_in_gain, new_second_in_gain = adamw(in_gain, grads[2], first_in_gain, second_in_gain, small_rate, 0.0)
    new_out_gain, new_first_out_gain, new_second_out_gain = adamw(out_gain, grads[3], first_out_gain, second_out_gain, small_rate, 0.0)
    new_conv_inner, new_first_conv_inner, new_second_conv_inner = adamw(conv_inner, grads[4], first_conv_inner, second_conv_inner, small_rate, 0.0)
    new_conv_shared, new_first_conv_shared, new_second_conv_shared = adamw(conv_shared, grads[5], first_conv_shared, second_conv_shared, small_rate, 0.0)
    new_head_params, updated_head_first_moment, head_second_all = adamw(head_params, grads[6], first_head_params, second_head_params, small_rate, 0.0)
    return (block_out, grad_in, grads[0], grads[1], grads[2], grads[3], grads[4], grads[5], grads[6], new_in_weight, new_out_weight, updated_input_gain, new_out_gain, new_conv_inner, new_conv_shared, new_head_params, new_first_in_weight, new_first_out_weight, new_first_in_gain, new_first_out_gain, new_first_conv_inner, new_first_conv_shared, updated_head_first_moment, new_second_in_weight, new_second_out_weight, new_second_in_gain, new_second_out_gain, new_second_conv_inner, new_second_conv_shared, head_second_all[0:2], head_second_all[2])
```

```python
import functools

import jax
import jax.numpy as jnp
from jax import lax
from jax.experimental import pallas as pl
from jax.experimental.pallas import tpu as pltpu
from jax.sharding import PartitionSpec as P

P_SIZE = 64
N_STATE = 128
LANES = 128
CHUNK = 128

norm_eps = 1e-05
beta_one = 0.9
beta_two = 0.95
adam_eps = 1e-08
adam_step = 3.0
weight_learning_rate = 0.01
matrix_decay = 0.1
small_rate = 0.1

f32 = jnp.float32
bf16 = jnp.bfloat16
NN = (((1,), (0,)), ((), ()))
NT = (((1,), (1,)), ((), ()))
TN = (((0,), (0,)), ((), ()))


def mm(a, b, dims):
    return lax.dot_general(a, b, dims, preferred_element_type=f32)


def mm_high(a, b):
    return lax.dot_general(
        a, b, NN, precision=lax.Precision.HIGHEST, preferred_element_type=f32
    )


def two_parts(a):
    hi = a.astype(bf16)
    return hi, (a - hi.astype(f32)).astype(bf16)


def mm3(a, b, dims):
    return mm(a[0], b[0], dims) + (mm(a[0], b[1], dims) + mm(a[1], b[0], dims))


def low_half(rows):
    return lax.broadcasted_iota(jnp.int32, (rows, LANES), 1) < P_SIZE


def split_pairs(values, heads):
    low = low_half(values.shape[0])
    gates, inners = [], []
    for h in range(0, heads, 2):
        a = values[:, h * LANES : (h + 1) * LANES]
        a_r = pltpu.roll(a, P_SIZE, 1)
        if h + 1 < heads:
            b = values[:, (h + 1) * LANES : (h + 2) * LANES]
            b_r = pltpu.roll(b, P_SIZE, 1)
            gates.append(jnp.where(low, a, b_r))
            inners.append(jnp.where(low, a_r, b))
        else:
            gates.append(a[:, :P_SIZE])
            inners.append(a_r[:, :P_SIZE])
    return jnp.concatenate(gates, axis=1), jnp.concatenate(inners, axis=1)


def join_pairs(gate, inner, heads):
    low = low_half(gate.shape[0])
    out = []
    for h in range(0, heads, 2):
        if h + 1 < heads:
            g = gate[:, h * P_SIZE : (h + 2) * P_SIZE]
            x = inner[:, h * P_SIZE : (h + 2) * P_SIZE]
            out.append(jnp.where(low, g, pltpu.roll(x, P_SIZE, 1)))
            out.append(jnp.where(low, pltpu.roll(g, P_SIZE, 1), x))
        else:
            out.append(
                jnp.concatenate(
                    [gate[:, h * P_SIZE :], inner[:, h * P_SIZE :]], axis=1
                )
            )
    return jnp.concatenate(out, axis=1)


def expand(cols, heads):
    rows = cols.shape[0]
    low = low_half(rows)
    out = []
    for h in range(0, heads, 2):
        if h + 1 < heads:
            one = jnp.broadcast_to(cols[:, h : h + 1], (rows, LANES))
            two = jnp.broadcast_to(cols[:, h + 1 : h + 2], (rows, LANES))
            out.append(jnp.where(low, one, two))
        else:
            out.append(jnp.broadcast_to(cols[:, h : h + 1], (rows, P_SIZE)))
    return jnp.concatenate(out, axis=1)


def pair_of(values, h, heads):
    first = h - h % 2
    return values[:, first * P_SIZE : min(first + 2, heads) * P_SIZE]


def merge_pairs(parts, heads):
    low = low_half(parts[0].shape[0])
    out = []
    for h in range(0, heads, 2):
        if h + 1 < heads:
            out.append(jnp.where(low, parts[h], parts[h + 1]))
        else:
            out.append(parts[h])
    return jnp.concatenate(out, axis=1)


def chunk_common(heads, main, small, cat, head_ref, taps_ref):
    rows = main.shape[0]
    gate, inner = split_pairs(main, heads)
    raw = jnp.concatenate([small[:, : 2 * N_STATE], inner], axis=1)
    cat[8 : 8 + rows] = raw
    conv = taps_ref[4:5] + taps_ref[0:1] * cat[5 : 5 + rows]
    for k in range(1, 4):
        conv = conv + taps_ref[k : k + 1] * cat[5 + k : 5 + k + rows]
    step_in = small[:, 2 * N_STATE :] + head_ref[0:1]
    dt = jnp.maximum(step_in, 0.0) + jnp.log1p(jnp.exp(-jnp.abs(step_in)))
    neg_rate = -jnp.exp(head_ref[1:2])
    decay_log = neg_rate * dt
    r = lax.broadcasted_iota(jnp.int32, (rows, rows), 0)
    c = lax.broadcasted_iota(jnp.int32, (rows, rows), 1)
    tri = jnp.where(r >= c, 1.0, 0.0).astype(f32)
    cumul = mm_high(tri, decay_log)
    return gate, conv, step_in, dt, neg_rate, decay_log, cumul, r, c


def fwd_kernel(
    heads, main_ref, small_ref, head_ref, taps_ref, gated_ref, y_ref, states_ref, state, cat
):
    rows = main_ref.shape[0]

    @pl.when(pl.program_id(0) == 0)
    def _():
        state[...] = jnp.zeros_like(state)
        cat[0:8] = jnp.zeros((8, cat.shape[1]), f32)

    gate, conv, _, dt, _, _, cumul, r, c = chunk_common(
        heads,
        main_ref[...].astype(f32),
        small_ref[...].astype(f32),
        cat,
        head_ref,
        taps_ref,
    )
    cat[0:8] = cat[rows : rows + 8]
    act = conv * jax.nn.sigmoid(conv)
    b2 = two_parts(act[:, :N_STATE])
    c2 = two_parts(act[:, N_STATE : 2 * N_STATE])
    inner = act[:, 2 * N_STATE :]
    scaled = inner * expand(dt, heads)
    scaled2 = two_parts(scaled)
    scores = mm3(c2, b2, NT)
    lower = r >= c
    cumul_t = cumul.T
    parts = []
    for h in range(heads):
        spread = cumul[:, h : h + 1] - cumul_t[h : h + 1, :]
        weights = two_parts(scores * jnp.exp(jnp.where(lower, spread, -1e30)))
        own = tuple(pair_of(part, h, heads) for part in scaled2)
        parts.append(mm3(weights, own, NN))
    s2 = two_parts(state[...])
    states_ref[0] = state[...]
    last = cumul[rows - 1 : rows]
    y = merge_pairs(parts, heads) + expand(jnp.exp(cumul), heads) * mm3(c2, s2, NN)
    y_ref[...] = y
    tail = expand(jnp.exp(last - cumul), heads)
    fresh = mm3(b2, two_parts(tail * scaled), TN)
    state[...] = expand(jnp.exp(last), heads) * state[...] + fresh
    full = y + expand(head_ref[2:3], heads) * inner
    gated_ref[...] = (full * (gate * jax.nn.sigmoid(gate))).astype(bf16)


def mixer_forward(main, small, head, taps, heads):
    length = main.shape[0]
    width = heads * P_SIZE
    count = length // CHUNK
    all_w = width + 2 * N_STATE
    return pl.pallas_call(
        functools.partial(fwd_kernel, heads),
        grid=(count,),
        in_specs=[
            pl.BlockSpec((CHUNK, 2 * width), lambda i: (i, 0)),
            pl.BlockSpec((CHUNK, 3 * LANES), lambda i: (i, 0)),
            pl.BlockSpec((8, LANES), lambda i: (0, 0)),
            pl.BlockSpec((8, all_w), lambda i: (0, 0)),
        ],
        out_specs=[
            pl.BlockSpec((CHUNK, width), lambda i: (i, 0)),
            pl.BlockSpec((CHUNK, width), lambda i: (i, 0)),
            pl.BlockSpec((1, N_STATE, width), lambda i: (i, 0, 0)),
        ],
        out_shape=[
            jax.ShapeDtypeStruct((length, width), bf16),
            jax.ShapeDtypeStruct((length, width), f32),
            jax.ShapeDtypeStruct((count, N_STATE, width), f32),
        ],
        scratch_shapes=[
            pltpu.VMEM((N_STATE, width), f32),
            pltpu.VMEM((CHUNK + 8, all_w), f32),
        ],
        name="mixer_forward",
    )(main, small, head, taps)


def bwd_kernel(
    heads,
    count,
    main_ref,
    small_ref,
    main_prev,
    small_prev,
    head_ref,
    taps_ref,
    y_ref,
    states_ref,
    dgated_ref,
    dmain_ref,
    dshared_ref,
    dstep_ref,
    dtaps_ref,
    dhead_ref,
    dstate,
    cat,
    dcat,
):
    rows, width = y_ref.shape
    step = pl.program_id(0)

    @pl.when(step == 0)
    def _():
        dstate[...] = jnp.zeros_like(dstate)
        dcat[rows : rows + 8] = jnp.zeros((8, dcat.shape[1]), f32)
        dtaps_ref[...] = jnp.zeros_like(dtaps_ref)
        dhead_ref[...] = jnp.zeros_like(dhead_ref)

    _, inner_prev = split_pairs(main_prev[8:16].astype(f32), heads)
    prev = jnp.concatenate(
        [small_prev[8:16].astype(f32)[:, : 2 * N_STATE], inner_prev], axis=1
    )
    cat[0:8] = jnp.where(step == count - 1, 0.0, prev)
    gate, conv, step_in, dt, neg_rate, decay_log, cumul, r, c = chunk_common(
        heads,
        main_ref[...].astype(f32),
        small_ref[...].astype(f32),
        cat,
        head_ref,
        taps_ref,
    )
    sig = jax.nn.sigmoid(conv)
    act = conv * sig
    dsilu = sig * (1.0 + conv * (1.0 - sig))
    b2 = two_parts(act[:, :N_STATE])
    c2 = two_parts(act[:, N_STATE : 2 * N_STATE])
    inner = act[:, 2 * N_STATE :]
    dt_x = expand(dt, heads)
    scaled = inner * dt_x
    scaled2 = two_parts(scaled)
    skip = expand(head_ref[2:3], heads)
    y = y_ref[...]
    sgate = jax.nn.sigmoid(gate)
    dgated = dgated_ref[...].astype(f32)
    dgate = dgated * (y + skip * inner) * (sgate * (1.0 + gate * (1.0 - sgate)))
    dy = dgated * (gate * sgate)
    dy2 = two_parts(dy)

    scores_t = mm3(b2, c2, NT)
    upper = c >= r
    cumul_t = cumul.T
    low = low_half(rows)
    parts = []
    dscores_t = None
    for h in range(heads):
        spread = cumul_t[h : h + 1, :] - cumul[:, h : h + 1]
        decay = jnp.exp(jnp.where(upper, spread, -1e30))
        weights = two_parts(scores_t * decay)
        dy_pair = tuple(pair_of(part, h, heads) for part in dy2)
        parts.append(mm3(weights, dy_pair, NN))
        own = pair_of(scaled, h, heads)
        if own.shape[1] == LANES:
            own = jnp.where(low == (h % 2 == 0), own, 0.0)
        term = mm3(two_parts(own), dy_pair, NT) * decay
        dscores_t = term if dscores_t is None else dscores_t + term
    s_in = states_ref[0]
    s2 = two_parts(s_in)
    ds = dstate[...]
    ds2 = two_parts(ds)
    last = cumul[rows - 1 : rows]
    tail = expand(jnp.exp(last - cumul), heads)
    ecum = expand(jnp.exp(cumul), heads)
    elast = expand(jnp.exp(last), heads)
    tail_b = tail * mm3(b2, ds2, NN)
    z = merge_pairs(parts, heads) + tail_b
    extra = jnp.sum(tail_b * scaled, axis=0, keepdims=True) + elast * jnp.sum(
        ds * s_in, axis=0, keepdims=True
    )
    at_end = lax.broadcasted_iota(jnp.int32, (rows, width), 0) == rows - 1
    u = dy * y - scaled * z + jnp.where(at_end, extra, 0.0)
    pick = (
        lax.broadcasted_iota(jnp.int32, (width, LANES), 0) // P_SIZE
        == lax.broadcasted_iota(jnp.int32, (width, LANES), 1)
    ).astype(f32)
    dcumul = mm_high(u, pick)
    suffix = jnp.where(c >= r, 1.0, 0.0).astype(f32)
    ddecay = mm_high(suffix, dcumul)
    dstep = (mm_high(inner * z, pick) + neg_rate * ddecay) * jax.nn.sigmoid(step_in)
    dstep_ref[...] = dstep.astype(bf16)
    dhead_ref[0:1] += jnp.sum(dstep, axis=0, keepdims=True)
    dhead_ref[1:2] += jnp.sum(decay_log * ddecay, axis=0, keepdims=True)

    dinner = dt_x * z + skip * dy
    dscores2 = two_parts(dscores_t)
    edy2 = two_parts(ecum * dy)
    db = mm3(dscores2, c2, NN) + mm3(two_parts(tail * scaled), ds2, NT)
    dc = mm3(dscores2, b2, TN) + mm3(edy2, s2, NT)
    dstate[...] = elast * ds + mm3(c2, edy2, TN)

    dconv = jnp.concatenate([db, dc, dinner], axis=1) * dsilu
    dcat[0:rows] = dconv
    draw = taps_ref[3:4] * dconv
    for k in range(3):
        draw = draw + taps_ref[k : k + 1] * dcat[3 - k : 3 - k + rows]
    for k in range(4):
        dtaps_ref[k : k + 1] += jnp.sum(
            dconv * cat[5 + k : 5 + k + rows], axis=0, keepdims=True
        )
    dtaps_ref[4:5] += jnp.sum(dconv, axis=0, keepdims=True)
    dtaps_ref[5:6, 2 * N_STATE :] += jnp.sum(dy * inner, axis=0, keepdims=True)
    dcat[rows : rows + 8] = dconv[0:8]
    dshared_ref[...] = draw[:, : 2 * N_STATE].T.astype(bf16)
    dmain_ref[...] = join_pairs(dgate, draw[:, 2 * N_STATE :], heads).astype(bf16)


def mixer_backward(main, small, head, taps, y, states, dgated, heads):
    length, width = y.shape
    count = length // CHUNK
    all_w = width + 2 * N_STATE
    per = CHUNK // 16

    def at(i):
        return (count - 1 - i, 0)

    def before(i):
        return (jnp.maximum((count - 1 - i) * per - 1, 0), 0)

    def fixed(i):
        return (0, 0)

    return pl.pallas_call(
        functools.partial(bwd_kernel, heads, count),
        grid=(count,),
        in_specs=[
            pl.BlockSpec((CHUNK, 2 * width), at),
            pl.BlockSpec((CHUNK, 3 * LANES), at),
            pl.BlockSpec((16, 2 * width), before),
            pl.BlockSpec((16, 3 * LANES), before),
            pl.BlockSpec((8, LANES), fixed),
            pl.BlockSpec((8, all_w), fixed),
            pl.BlockSpec((CHUNK, width), at),
            pl.BlockSpec((1, N_STATE, width), lambda i: (count - 1 - i, 0, 0)),
            pl.BlockSpec((CHUNK, width), at),
        ],
        out_specs=[
            pl.BlockSpec((CHUNK, 2 * width), at),
            pl.BlockSpec((2 * N_STATE, CHUNK), lambda i: (0, count - 1 - i)),
            pl.BlockSpec((CHUNK, LANES), at),
            pl.BlockSpec((8, all_w), fixed),
            pl.BlockSpec((8, LANES), fixed),
        ],
        out_shape=[
            jax.ShapeDtypeStruct((length, 2 * width), bf16),
            jax.ShapeDtypeStruct((2 * N_STATE, length), bf16),
            jax.ShapeDtypeStruct((length, LANES), bf16),
            jax.ShapeDtypeStruct((8, all_w), f32),
            jax.ShapeDtypeStruct((8, LANES), f32),
        ],
        scratch_shapes=[
            pltpu.VMEM((N_STATE, width), f32),
            pltpu.VMEM((CHUNK + 8, all_w), f32),
            pltpu.VMEM((CHUNK + 8, all_w), f32),
        ],
        name="mixer_backward",
    )(main, small, main, small, head, taps, y, states, dgated)


MESH = pl.DeviceIdType.MESH


def greet(peers, count):
    barrier = pltpu.get_barrier_semaphore()
    for peer in peers:
        pl.semaphore_signal(barrier, inc=1, device_id=peer, device_id_type=MESH)
    pl.semaphore_wait(barrier, count)


def wire(src, dst, send, recv, peer):
    return pltpu.make_async_remote_copy(
        src_ref=src,
        dst_ref=dst,
        send_sem=send,
        recv_sem=recv,
        device_id=peer,
        device_id_type=MESH,
    )


def weights_kernel(n_seq, n_wsh, main, small, outw, w_main, w_small, w_out, *sems):
    send_a, recv_a, send_b, recv_b, send_c, recv_c, send_d, recv_d, send_e, recv_e, own = sems
    s = lax.axis_index("seq")
    w = lax.axis_index("wshard")
    row = [(lax.rem(s + k, n_seq), w) for k in range(1, n_seq)]
    col = [(s, lax.rem(w + j, n_wsh)) for j in range(1, n_wsh)]
    greet(row + col, n_seq + n_wsh - 2)
    first = [
        wire(main.at[peer[0]], w_main.at[s, w], send_a.at[k], recv_a.at[k], peer)
        for k, peer in enumerate(row)
    ]
    spread = [
        wire(small, w_small.at[s, w], send_b.at[j], recv_b.at[j], peer)
        for j, peer in enumerate(col)
    ]
    outs = [
        wire(outw, w_out.at[w], send_c.at[j], recv_c.at[j], peer)
        for j, peer in enumerate(col)
    ]
    mine = [
        pltpu.make_async_copy(main.at[s], w_main.at[s, w], own.at[0]),
        pltpu.make_async_copy(small, w_small.at[s, w], own.at[1]),
        pltpu.make_async_copy(outw, w_out.at[w], own.at[2]),
    ]
    for copy in mine[:2] + first + spread:
        copy.start()
    mine[0].wait()
    for copy in first:
        copy.wait_recv()
    second = [
        wire(w_main.at[:, w], w_main.at[:, w], send_d.at[j], recv_d.at[j], peer)
        for j, peer in enumerate(col)
    ]
    for copy in second:
        copy.start()
    mine[1].wait()
    for copy in spread:
        copy.wait_recv()
    third = [
        wire(w_small.at[s], w_small.at[s], send_e.at[k], recv_e.at[k], peer)
        for k, peer in enumerate(row)
    ]
    for copy in third + [mine[2]] + outs:
        copy.start()
    mine[2].wait()
    for copy in first + spread:
        copy.wait_send()
    for copy in second + third + outs:
        copy.wait()


def spread_weights(main, small, outw, n_seq, n_wsh):
    rows_in, cols = main.shape[1:]
    anywhere = pl.BlockSpec(memory_space=pl.ANY)
    dma = pltpu.SemaphoreType.DMA
    a, c = n_seq - 1, n_wsh - 1
    return pl.pallas_call(
        functools.partial(weights_kernel, n_seq, n_wsh),
        in_specs=[anywhere] * 3,
        out_specs=[anywhere] * 3,
        out_shape=[
            jax.ShapeDtypeStruct((n_seq, n_wsh, rows_in, cols), bf16),
            jax.ShapeDtypeStruct((n_seq, n_wsh) + small.shape, bf16),
            jax.ShapeDtypeStruct((n_wsh,) + outw.shape, bf16),
        ],
        scratch_shapes=[
            dma((n,)) for n in (a, a, c, c, c, c, c, c, a, a, 3)
        ],
        compiler_params=pltpu.CompilerParams(collective_id=0, has_side_effects=True),
        cost_estimate=pl.CostEstimate(
            flops=0, bytes_accessed=200_000_000, transcendentals=0
        ),
        name="spread_weights",
    )(main, small, outw)


def swap_kernel(plan, n_seq, n_wsh, *refs):
    n = len(plan)
    ins, outs, sems = refs[:n], refs[n : 2 * n], refs[2 * n :]
    s = lax.axis_index("seq")
    w = lax.axis_index("wshard")
    total = n_seq * n_wsh
    me_all = s * n_wsh + w
    size = {"seq": n_seq, "wshard": n_wsh, "both": total}
    me_of = {"seq": s, "wshard": w, "both": me_all}

    def peer_at(axis, k):
        if axis == "seq":
            index = lax.rem(s + k, n_seq)
            return index, (index, w)
        if axis == "wshard":
            index = lax.rem(w + k, n_wsh)
            return index, (s, index)
        index = lax.rem(me_all + k, total)
        return index, (lax.div(index, n_wsh), lax.rem(index, n_wsh))

    def block(kind, ref, index):
        if kind == "all":
            return ref
        return ref.at[index] if kind == 0 else ref.at[:, index]

    def copy_of(i, k):
        kind, axis = plan[i]
        index, peer = peer_at(axis, k)
        return wire(
            block(kind, ins[i], index),
            outs[i].at[me_of[axis]],
            sems[3 * i].at[k],
            sems[3 * i + 1].at[k],
            peer,
        )

    widest = "both" if any(axis == "both" for _, axis in plan) else plan[0][1]
    barrier = pltpu.get_barrier_semaphore()

    def hail(k, _):
        pl.semaphore_signal(
            barrier, inc=1, device_id=peer_at(widest, k)[1], device_id_type=MESH
        )
        return 0

    lax.fori_loop(1, size[widest], hail, 0)
    pl.semaphore_wait(barrier, size[widest] - 1)
    own = []
    for i, (kind, axis) in enumerate(plan):
        me = me_of[axis]
        own.append(
            pltpu.make_async_copy(
                block(kind, ins[i], me), outs[i].at[me], sems[3 * i + 2].at[0]
            )
        )

        def begin(k, _, i=i):
            copy_of(i, k).start()
            return 0

        lax.fori_loop(1, size[axis], begin, 0)
    for copy in own:
        copy.start()
    for i, (kind, axis) in enumerate(plan):
        own[i].wait()

        def finish(k, _, i=i):
            copy_of(i, k).wait()
            return 0

        lax.fori_loop(1, size[axis], finish, 0)


def swap(arrays, plan, n_seq, n_wsh, collective_id, name):
    anywhere = pl.BlockSpec(memory_space=pl.ANY)
    size = {"seq": n_seq, "wshard": n_wsh, "both": n_seq * n_wsh}
    shapes, sems = [], []
    for x, (kind, axis) in zip(arrays, plan):
        n = size[axis]
        shape = x.shape
        if kind == 0:
            shape = shape[1:]
        elif kind == 1:
            shape = shape[:1] + shape[2:]
        shapes.append(jax.ShapeDtypeStruct((n,) + shape, x.dtype))
        sems += [
            pltpu.SemaphoreType.DMA((n,)),
            pltpu.SemaphoreType.DMA((n,)),
            pltpu.SemaphoreType.DMA((1,)),
        ]
    return pl.pallas_call(
        functools.partial(swap_kernel, plan, n_seq, n_wsh),
        in_specs=[anywhere] * len(arrays),
        out_specs=[anywhere] * len(arrays),
        out_shape=shapes,
        scratch_shapes=sems,
        compiler_params=pltpu.CompilerParams(
            collective_id=collective_id, has_side_effects=True
        ),
        name=name,
    )(*arrays)


def stats_kernel(n_seq, x_ref, out_ref, slots, send, recv):
    s = lax.axis_index("seq")
    w = lax.axis_index("wshard")
    row = [(lax.rem(s + k, n_seq), w) for k in range(1, n_seq)]
    greet(row, n_seq - 1)
    copies = [
        wire(x_ref, slots.at[s], send.at[k], recv.at[k], peer)
        for k, peer in enumerate(row)
    ]
    for copy in copies:
        copy.start()
    slots[s] = x_ref[...]
    for copy in copies:
        copy.wait()
    total = slots[0]
    for k in range(1, n_seq):
        total = total + slots[k]
    out_ref[...] = total


def sum_over_seq(x, n_seq):
    vmem = pl.BlockSpec(memory_space=pltpu.VMEM)
    dma = pltpu.SemaphoreType.DMA
    return pl.pallas_call(
        functools.partial(stats_kernel, n_seq),
        in_specs=[vmem],
        out_specs=vmem,
        out_shape=jax.ShapeDtypeStruct(x.shape, f32),
        scratch_shapes=[
            pltpu.VMEM((n_seq,) + x.shape, f32),
            dma((n_seq - 1,)),
            dma((n_seq - 1,)),
        ],
        compiler_params=pltpu.CompilerParams(collective_id=1, has_side_effects=True),
        name="sum_over_seq",
    )(x)


def adamw(param, grad, first, second_moment, rate, decay):
    first_new = beta_one * first + (1.0 - beta_one) * grad
    second_new = beta_two * second_moment + (1.0 - beta_two) * grad * grad
    corrected = (
        first_new
        / (1.0 - beta_one**adam_step)
        / (jnp.sqrt(second_new / (1.0 - beta_two**adam_step)) + adam_eps)
    )
    return (param - rate * (corrected + decay * param), first_new, second_new)


def local(
    block_in,
    cotangent,
    in_weight,
    out_weight,
    in_gain,
    out_gain,
    conv_inner,
    conv_shared,
    head_params,
    first_in_weight,
    first_out_weight,
    first_in_gain,
    first_out_gain,
    first_conv_inner,
    first_conv_shared,
    first_head_params,
    second_in_weight,
    second_out_weight,
    second_in_gain,
    second_out_gain,
    second_conv_inner,
    second_conv_shared,
    second_head_params,
):
    seq_index = lax.axis_index("seq")
    wsh_index = lax.axis_index("wshard")
    n_seq = lax.axis_size("seq")
    n_wsh = lax.axis_size("wshard")
    rows_in, cols_in = in_weight.shape
    rows_out = out_weight.shape[0]
    tokens, width_in = block_in.shape[1:]
    heads = head_params.shape[1] // n_seq
    width = heads * P_SIZE
    inner_all = out_gain.shape[0]
    share = 2 * N_STATE // n_seq

    inputs = block_in[0].astype(f32)
    rms_in = lax.rsqrt(jnp.mean(inputs * inputs, axis=-1, keepdims=True) + norm_eps)
    normed = (inputs * rms_in * in_gain).astype(bf16)
    normed_all = lax.all_gather(normed, "seq", axis=0, tiled=True)
    cot = cotangent[0]
    cot_all = lax.all_gather(cot, "seq", axis=0, tiled=True)
    in_w16 = in_weight.astype(bf16)
    main_send = in_w16[:, : 2 * inner_all].reshape(rows_in, n_seq, 2 * width)
    main_send = jnp.swapaxes(main_send, 0, 1)
    small_send = in_w16[:, 2 * inner_all :]
    small_send = jnp.pad(small_send, ((0, 0), (0, -small_send.shape[1] % LANES)))
    w_main, w_small, w_out = spread_weights(
        main_send, small_send, out_weight.astype(bf16), n_seq, n_wsh
    )
    w_main = w_main.reshape(width_in, 2 * width)
    w_small = w_small.reshape(width_in, small_send.shape[1])
    w_out = w_out.reshape(width, width_in)
    w_shared = w_small[:, : 2 * N_STATE]
    w_step = lax.dynamic_slice_in_dim(w_small, 2 * N_STATE + seq_index * heads, heads, 1)
    w_share = lax.dynamic_slice_in_dim(w_small, seq_index * share, share, 1)
    w_ext = jnp.pad(
        jnp.concatenate([w_share, w_step], axis=1), ((0, 0), (0, LANES - share - heads))
    )
    w_step = jnp.pad(w_step, ((0, 0), (0, LANES - heads)))

    main = mm(normed_all, w_main, NN).astype(bf16)
    small = mm(normed_all, jnp.concatenate([w_shared, w_step], axis=1), NN).astype(bf16)
    head_local = lax.dynamic_slice_in_dim(head_params, seq_index * heads, heads, 1)
    head = jnp.pad(head_local, ((0, 5), (0, LANES - heads)))
    conv_local = lax.dynamic_slice_in_dim(conv_inner, seq_index * width, width, 1)
    taps = jnp.pad(jnp.concatenate([conv_shared, conv_local], axis=1), ((0, 3), (0, 0)))
    gain_local = lax.dynamic_slice_in_dim(out_gain, seq_index * width, width, 0)
    gated, y, states = mixer_forward(main, small, head, taps, heads)
    d_gnormed = mm(cot_all, w_out, NT)
    gated32 = gated.astype(f32)
    scaled = d_gnormed * gain_local
    stats = jnp.stack(
        [jnp.sum(gated32 * gated32, axis=-1), jnp.sum(scaled * gated32, axis=-1)]
    )
    stats = sum_over_seq(stats.reshape(-1, LANES), n_seq).reshape(stats.shape)
    rms_out = lax.rsqrt(stats[0] / inner_all + norm_eps)[:, None]
    mean_sg = (stats[1] / inner_all)[:, None]
    gnormed = (gated32 * rms_out * gain_local).astype(bf16)
    d_gated = (rms_out * scaled - gated32 * rms_out**3 * mean_sg).astype(bf16)
    d_out_gain = jnp.sum(d_gnormed * gated32 * rms_out, axis=0)

    g_out = mm(gnormed, cot_all, TN)
    grad_out_weight = lax.dynamic_slice_in_dim(g_out, wsh_index * rows_out, rows_out, 0)
    for j in range(1, n_wsh):
        to = lax.rem(wsh_index + j, n_wsh)
        part = lax.dynamic_slice_in_dim(g_out, to * rows_out, rows_out, 0)
        grad_out_weight = grad_out_weight + lax.ppermute(
            part, "wshard", [(i, (i + j) % n_wsh) for i in range(n_wsh)]
        )
    mixed = lax.psum_scatter(
        mm(gnormed, w_out, NN).astype(bf16), "seq", scatter_dimension=0, tiled=True
    )
    block_out = (inputs + mixed.astype(f32))[None]
    dmain, dshared_t, dstep, dtaps, dhead = mixer_backward(
        main, small, head, taps, y, states, d_gated, heads
    )

    (shared_parts,) = swap(
        (dshared_t.reshape(n_seq, share, -1),), ((0, "seq"),), n_seq, n_wsh, 2, "swap_shared"
    )
    shared_sum = jnp.sum(shared_parts.astype(f32), axis=0).astype(bf16)
    d_ext = jnp.pad(
        jnp.concatenate([shared_sum.T, dstep[:, :heads]], axis=1),
        ((0, 0), (0, LANES - share - heads)),
    )
    d_normed = mm(dmain, w_main, NT) + mm(d_ext, w_ext, NT)
    d_normed = lax.psum_scatter(
        d_normed.astype(bf16), "seq", scatter_dimension=0, tiled=True
    ).astype(f32)

    g_main = mm(normed_all, dmain, TN).astype(bf16).reshape(n_seq, n_wsh, rows_in, 2 * width)
    g_ext = mm(normed_all, d_ext, TN).astype(bf16).reshape(n_seq, n_wsh, rows_in, LANES)
    g_main, g_ext = swap(
        (g_main, g_ext), ((1, "wshard"), (1, "wshard")), n_seq, n_wsh, 3, "swap_grads"
    )
    g_main = jnp.sum(g_main.astype(f32), axis=0).astype(bf16)
    g_ext = jnp.sum(g_ext.astype(f32), axis=0).astype(bf16)

    d_in_gain = jnp.sum(d_normed * inputs * rms_in, axis=0)
    scaled_in = d_normed * in_gain
    grad_in = (
        cot.astype(f32)
        + rms_in * scaled_in
        - inputs * rms_in**3 * jnp.mean(scaled_in * inputs, axis=-1, keepdims=True)
    )[None]

    d_skip = dtaps[5, 2 * N_STATE :].reshape(heads, P_SIZE).sum(-1)
    d_head = jnp.concatenate([dhead[:2, :heads], d_skip[None]], axis=0)
    pieces = (
        d_in_gain,
        dtaps[:5, : 2 * N_STATE],
        d_out_gain,
        dtaps[:5, 2 * N_STATE :],
        d_head,
    )
    flat = jnp.concatenate([p.reshape(-1) for p in pieces])
    flat = jnp.pad(flat, (0, -flat.shape[0] % (8 * LANES))).reshape(-1, LANES)
    g_main, g_ext, flat = swap(
        (g_main, g_ext, flat),
        ((0, "seq"), (0, "seq"), ("all", "both")),
        n_seq,
        n_wsh,
        4,
        "swap_last",
    )
    g_main = jnp.swapaxes(g_main, 0, 1).reshape(rows_in, 2 * inner_all)
    g_ext = jnp.swapaxes(g_ext, 0, 1)
    grad_in_weight = jnp.concatenate(
        [
            g_main,
            g_ext[:, :, :share].reshape(rows_in, 2 * N_STATE),
            g_ext[:, :, share : share + heads].reshape(rows_in, heads * n_seq),
        ],
        axis=1,
    ).astype(f32)
    flat = jnp.sum(flat.reshape(n_seq, n_wsh, -1), axis=1)
    sums, at = [], 0
    for p in pieces:
        sums.append(flat[:, at : at + p.size].reshape((n_seq,) + p.shape))
        at += p.size
    grad_in_gain = jnp.sum(sums[0], axis=0)
    grad_conv_shared = jnp.sum(sums[1], axis=0)
    grad_out_gain = sums[2].reshape(-1)
    grad_conv_inner = jnp.swapaxes(sums[3], 0, 1).reshape(conv_inner.shape)
    grad_head_params = jnp.swapaxes(sums[4], 0, 1).reshape(head_params.shape)
    new_in_weight, new_first_in_weight, new_second_in_weight = adamw(
        in_weight,
        grad_in_weight,
        first_in_weight,
        second_in_weight,
        weight_learning_rate,
        matrix_decay,
    )
    new_out_weight, new_first_out_weight, new_second_out_weight = adamw(
        out_weight,
        grad_out_weight,
        first_out_weight,
        second_out_weight,
        weight_learning_rate,
        matrix_decay,
    )
    updated_input_gain, new_first_in_gain, new_second_in_gain = adamw(
        in_gain, grad_in_gain, first_in_gain, second_in_gain, small_rate, 0.0
    )
    new_out_gain, new_first_out_gain, new_second_out_gain = adamw(
        out_gain, grad_out_gain, first_out_gain, second_out_gain, small_rate, 0.0
    )
    new_conv_inner, new_first_conv_inner, new_second_conv_inner = adamw(
        conv_inner, grad_conv_inner, first_conv_inner, second_conv_inner, small_rate, 0.0
    )
    new_conv_shared, new_first_conv_shared, new_second_conv_shared = adamw(
        conv_shared, grad_conv_shared, first_conv_shared, second_conv_shared, small_rate, 0.0
    )
    new_head_params, updated_head_first_moment, head_second_all = adamw(
        head_params, grad_head_params, first_head_params, second_head_params, small_rate, 0.0
    )
    return (
        block_out,
        grad_in,
        grad_in_weight,
        grad_out_weight,
        grad_in_gain,
        grad_out_gain,
        grad_conv_inner,
        grad_conv_shared,
        grad_head_params,
        new_in_weight,
        new_out_weight,
        updated_input_gain,
        new_out_gain,
        new_conv_inner,
        new_conv_shared,
        new_head_params,
        new_first_in_weight,
        new_first_out_weight,
        new_first_in_gain,
        new_first_out_gain,
        new_first_conv_inner,
        new_first_conv_shared,
        updated_head_first_moment,
        new_second_in_weight,
        new_second_out_weight,
        new_second_in_gain,
        new_second_out_gain,
        new_second_conv_inner,
        new_second_conv_shared,
        head_second_all[0:2],
        head_second_all[2],
    )


def solution(mesh):
    return jax.shard_map(
        local,
        mesh=mesh,
        in_specs=(
            P("wshard", "seq", None),
            P("wshard", "seq", None),
            P(("seq", "wshard"), None),
            P(("seq", "wshard"), None),
            P(),
            P(),
            P(),
            P(),
            P(),
            P(("seq", "wshard"), None),
            P(("seq", "wshard"), None),
            P(),
            P(),
            P(),
            P(),
            P(),
            P(("seq", "wshard"), None),
            P(("seq", "wshard"), None),
            P(),
            P(),
            P(),
            P(),
            P(),
        ),
        out_specs=(
            P("wshard", "seq", None),
            P("wshard", "seq", None),
            P(("seq", "wshard"), None),
            P(("seq", "wshard"), None),
            P(),
            P(),
            P(),
            P(),
            P(),
            P(("seq", "wshard"), None),
            P(("seq", "wshard"), None),
            P(),
            P(),
            P(),
            P(),
            P(),
            P(("seq", "wshard"), None),
            P(("seq", "wshard"), None),
            P(),
            P(),
            P(),
            P(),
            P(),
            P(("seq", "wshard"), None),
            P(("seq", "wshard"), None),
            P(),
            P(),
            P(),
            P(),
            P(),
            P(),
        ),
        check_vma=False,
    )
```

```python
import functools

import jax
import jax.numpy as jnp
from jax import lax
from jax.experimental import pallas as pl
from jax.experimental.pallas import tpu as pltpu
from jax.sharding import PartitionSpec as P

P_SIZE = 64
N_STATE = 128
LANES = 128
CHUNK = 128
STEP_ROWS = 16

norm_eps = 1e-05
beta_one = 0.9
beta_two = 0.95
adam_eps = 1e-08
adam_step = 3.0
weight_learning_rate = 0.01
matrix_decay = 0.1
small_rate = 0.1

f32 = jnp.float32
bf16 = jnp.bfloat16
NN = (((1,), (0,)), ((), ()))
NT = (((1,), (1,)), ((), ()))
TN = (((0,), (0,)), ((), ()))


def mm(a, b, dims):
    return lax.dot_general(a, b, dims, preferred_element_type=f32)


def mm_high(a, b):
    return lax.dot_general(
        a, b, NN, precision=lax.Precision.HIGHEST, preferred_element_type=f32
    )


def two_parts(a):
    hi = a.astype(bf16)
    return hi, (a - hi.astype(f32)).astype(bf16)


def mm3(a, b, dims):
    return mm(a[0], b[0], dims) + (mm(a[0], b[1], dims) + mm(a[1], b[0], dims))


def low_half(rows):
    return lax.broadcasted_iota(jnp.int32, (rows, LANES), 1) < P_SIZE


def split_pairs(values, heads):
    low = low_half(values.shape[0])
    gates, inners = [], []
    for h in range(0, heads, 2):
        a = values[:, h * LANES : (h + 1) * LANES]
        a_r = pltpu.roll(a, P_SIZE, 1)
        if h + 1 < heads:
            b = values[:, (h + 1) * LANES : (h + 2) * LANES]
            b_r = pltpu.roll(b, P_SIZE, 1)
            gates.append(jnp.where(low, a, b_r))
            inners.append(jnp.where(low, a_r, b))
        else:
            gates.append(a[:, :P_SIZE])
            inners.append(a_r[:, :P_SIZE])
    return jnp.concatenate(gates, axis=1), jnp.concatenate(inners, axis=1)


def join_pairs(gate, inner, heads):
    low = low_half(gate.shape[0])
    out = []
    for h in range(0, heads, 2):
        if h + 1 < heads:
            g = gate[:, h * P_SIZE : (h + 2) * P_SIZE]
            x = inner[:, h * P_SIZE : (h + 2) * P_SIZE]
            out.append(jnp.where(low, g, pltpu.roll(x, P_SIZE, 1)))
            out.append(jnp.where(low, pltpu.roll(g, P_SIZE, 1), x))
        else:
            out.append(
                jnp.concatenate(
                    [gate[:, h * P_SIZE :], inner[:, h * P_SIZE :]], axis=1
                )
            )
    return jnp.concatenate(out, axis=1)


def expand(cols, heads):
    rows = cols.shape[0]
    low = low_half(rows)
    out = []
    for h in range(0, heads, 2):
        if h + 1 < heads:
            one = jnp.broadcast_to(cols[:, h : h + 1], (rows, LANES))
            two = jnp.broadcast_to(cols[:, h + 1 : h + 2], (rows, LANES))
            out.append(jnp.where(low, one, two))
        else:
            out.append(jnp.broadcast_to(cols[:, h : h + 1], (rows, P_SIZE)))
    return jnp.concatenate(out, axis=1)


def pair_of(values, h, heads):
    first = h - h % 2
    return values[:, first * P_SIZE : min(first + 2, heads) * P_SIZE]


def merge_pairs(parts, heads):
    low = low_half(parts[0].shape[0])
    out = []
    for h in range(0, heads, 2):
        if h + 1 < heads:
            out.append(jnp.where(low, parts[h], parts[h + 1]))
        else:
            out.append(parts[h])
    return jnp.concatenate(out, axis=1)


def chunk_common(heads, main, small, cat, head_ref, taps_ref):
    rows = main.shape[0]
    gate, inner = split_pairs(main, heads)
    raw = jnp.concatenate([small[:, : 2 * N_STATE], inner], axis=1)
    cat[8 : 8 + rows] = raw
    conv = taps_ref[4:5] + taps_ref[0:1] * cat[5 : 5 + rows]
    for k in range(1, 4):
        conv = conv + taps_ref[k : k + 1] * cat[5 + k : 5 + k + rows]
    step_in = small[:, 2 * N_STATE :] + head_ref[0:1]
    dt = jnp.maximum(step_in, 0.0) + jnp.log1p(jnp.exp(-jnp.abs(step_in)))
    neg_rate = -jnp.exp(head_ref[1:2])
    decay_log = neg_rate * dt
    r = lax.broadcasted_iota(jnp.int32, (rows, rows), 0)
    c = lax.broadcasted_iota(jnp.int32, (rows, rows), 1)
    tri = jnp.where(r >= c, 1.0, 0.0).astype(f32)
    cumul = mm_high(tri, decay_log)
    return gate, conv, step_in, dt, neg_rate, decay_log, cumul, r, c


def fwd_kernel(
    heads, main_ref, small_ref, head_ref, taps_ref, gated_ref, y_ref, states_ref, state, cat
):
    rows = main_ref.shape[0]

    @pl.when(pl.program_id(0) == 0)
    def _():
        state[...] = jnp.zeros_like(state)
        cat[0:8] = jnp.zeros((8, cat.shape[1]), f32)

    gate, conv, _, dt, _, _, cumul, r, c = chunk_common(
        heads,
        main_ref[...].astype(f32),
        small_ref[...].astype(f32),
        cat,
        head_ref,
        taps_ref,
    )
    cat[0:8] = cat[rows : rows + 8]
    act = conv * jax.nn.sigmoid(conv)
    b2 = two_parts(act[:, :N_STATE])
    c2 = two_parts(act[:, N_STATE : 2 * N_STATE])
    inner = act[:, 2 * N_STATE :]
    scaled = inner * expand(dt, heads)
    scaled2 = two_parts(scaled)
    scores = mm3(c2, b2, NT)
    lower = r >= c
    cumul_t = cumul.T
    parts = []
    for h in range(heads):
        spread = cumul[:, h : h + 1] - cumul_t[h : h + 1, :]
        weights = two_parts(scores * jnp.exp(jnp.where(lower, spread, -1e30)))
        own = tuple(pair_of(part, h, heads) for part in scaled2)
        parts.append(mm3(weights, own, NN))
    s2 = two_parts(state[...])
    states_ref[0] = state[...]
    last = cumul[rows - 1 : rows]
    y = merge_pairs(parts, heads) + expand(jnp.exp(cumul), heads) * mm3(c2, s2, NN)
    y_ref[...] = y
    tail = expand(jnp.exp(last - cumul), heads)
    fresh = mm3(b2, two_parts(tail * scaled), TN)
    state[...] = expand(jnp.exp(last), heads) * state[...] + fresh
    full = y + expand(head_ref[2:3], heads) * inner
    gated_ref[...] = (full * (gate * jax.nn.sigmoid(gate))).astype(bf16)


def mixer_forward(main, small, head, taps, heads):
    length = main.shape[0]
    width = heads * P_SIZE
    count = length // CHUNK
    all_w = width + 2 * N_STATE
    return pl.pallas_call(
        functools.partial(fwd_kernel, heads),
        grid=(count,),
        in_specs=[
            pl.BlockSpec((CHUNK, 2 * width), lambda i: (i, 0)),
            pl.BlockSpec((CHUNK, 3 * LANES), lambda i: (i, 0)),
            pl.BlockSpec((8, LANES), lambda i: (0, 0)),
            pl.BlockSpec((8, all_w), lambda i: (0, 0)),
        ],
        out_specs=[
            pl.BlockSpec((CHUNK, width), lambda i: (i, 0)),
            pl.BlockSpec((CHUNK, width), lambda i: (i, 0)),
            pl.BlockSpec((1, N_STATE, width), lambda i: (i, 0, 0)),
        ],
        out_shape=[
            jax.ShapeDtypeStruct((length, width), bf16),
            jax.ShapeDtypeStruct((length, width), f32),
            jax.ShapeDtypeStruct((count, N_STATE, width), f32),
        ],
        scratch_shapes=[
            pltpu.VMEM((N_STATE, width), f32),
            pltpu.VMEM((CHUNK + 8, all_w), f32),
        ],
        name="mixer_forward",
    )(main, small, head, taps)


def bwd_kernel(
    heads,
    count,
    main_ref,
    small_ref,
    main_prev,
    small_prev,
    head_ref,
    taps_ref,
    y_ref,
    states_ref,
    dgated_ref,
    dmain_ref,
    dshared_ref,
    dstep_ref,
    dtaps_ref,
    dhead_ref,
    dstate,
    cat,
    dcat,
):
    rows, width = y_ref.shape
    step = pl.program_id(0)

    @pl.when(step == 0)
    def _():
        dstate[...] = jnp.zeros_like(dstate)
        dcat[rows : rows + 8] = jnp.zeros((8, dcat.shape[1]), f32)
        dtaps_ref[...] = jnp.zeros_like(dtaps_ref)
        dhead_ref[...] = jnp.zeros_like(dhead_ref)

    _, inner_prev = split_pairs(main_prev[8:16].astype(f32), heads)
    prev = jnp.concatenate(
        [small_prev[8:16].astype(f32)[:, : 2 * N_STATE], inner_prev], axis=1
    )
    cat[0:8] = jnp.where(step == count - 1, 0.0, prev)
    gate, conv, step_in, dt, neg_rate, decay_log, cumul, r, c = chunk_common(
        heads,
        main_ref[...].astype(f32),
        small_ref[...].astype(f32),
        cat,
        head_ref,
        taps_ref,
    )
    sig = jax.nn.sigmoid(conv)
    act = conv * sig
    dsilu = sig * (1.0 + conv * (1.0 - sig))
    b2 = two_parts(act[:, :N_STATE])
    c2 = two_parts(act[:, N_STATE : 2 * N_STATE])
    inner = act[:, 2 * N_STATE :]
    dt_x = expand(dt, heads)
    scaled = inner * dt_x
    scaled2 = two_parts(scaled)
    skip = expand(head_ref[2:3], heads)
    y = y_ref[...]
    sgate = jax.nn.sigmoid(gate)
    dgated = dgated_ref[...].astype(f32)
    dgate = dgated * (y + skip * inner) * (sgate * (1.0 + gate * (1.0 - sgate)))
    dy = dgated * (gate * sgate)
    dy2 = two_parts(dy)

    scores_t = mm3(b2, c2, NT)
    upper = c >= r
    cumul_t = cumul.T
    low = low_half(rows)
    parts = []
    dscores_t = None
    for h in range(heads):
        spread = cumul_t[h : h + 1, :] - cumul[:, h : h + 1]
        decay = jnp.exp(jnp.where(upper, spread, -1e30))
        weights = two_parts(scores_t * decay)
        dy_pair = tuple(pair_of(part, h, heads) for part in dy2)
        parts.append(mm3(weights, dy_pair, NN))
        own = pair_of(scaled, h, heads)
        if own.shape[1] == LANES:
            own = jnp.where(low == (h % 2 == 0), own, 0.0)
        term = mm3(two_parts(own), dy_pair, NT) * decay
        dscores_t = term if dscores_t is None else dscores_t + term
    s_in = states_ref[0]
    s2 = two_parts(s_in)
    ds = dstate[...]
    ds2 = two_parts(ds)
    last = cumul[rows - 1 : rows]
    tail = expand(jnp.exp(last - cumul), heads)
    ecum = expand(jnp.exp(cumul), heads)
    elast = expand(jnp.exp(last), heads)
    tail_b = tail * mm3(b2, ds2, NN)
    z = merge_pairs(parts, heads) + tail_b
    extra = jnp.sum(tail_b * scaled, axis=0, keepdims=True) + elast * jnp.sum(
        ds * s_in, axis=0, keepdims=True
    )
    at_end = lax.broadcasted_iota(jnp.int32, (rows, width), 0) == rows - 1
    u = dy * y - scaled * z + jnp.where(at_end, extra, 0.0)
    pick = (
        lax.broadcasted_iota(jnp.int32, (width, LANES), 0) // P_SIZE
        == lax.broadcasted_iota(jnp.int32, (width, LANES), 1)
    ).astype(f32)
    dcumul = mm_high(u, pick)
    suffix = jnp.where(c >= r, 1.0, 0.0).astype(f32)
    ddecay = mm_high(suffix, dcumul)
    dstep = (mm_high(inner * z, pick) + neg_rate * ddecay) * jax.nn.sigmoid(step_in)
    dstep_ref[...] = dstep.T[: dstep_ref.shape[0]].astype(bf16)
    dhead_ref[0:1] += jnp.sum(dstep, axis=0, keepdims=True)
    dhead_ref[1:2] += jnp.sum(decay_log * ddecay, axis=0, keepdims=True)

    dinner = dt_x * z + skip * dy
    dscores2 = two_parts(dscores_t)
    edy2 = two_parts(ecum * dy)
    db = mm3(dscores2, c2, NN) + mm3(two_parts(tail * scaled), ds2, NT)
    dc = mm3(dscores2, b2, TN) + mm3(edy2, s2, NT)
    dstate[...] = elast * ds + mm3(c2, edy2, TN)

    dconv = jnp.concatenate([db, dc, dinner], axis=1) * dsilu
    dcat[0:rows] = dconv
    draw = taps_ref[3:4] * dconv
    for k in range(3):
        draw = draw + taps_ref[k : k + 1] * dcat[3 - k : 3 - k + rows]
    for k in range(4):
        dtaps_ref[k : k + 1] += jnp.sum(
            dconv * cat[5 + k : 5 + k + rows], axis=0, keepdims=True
        )
    dtaps_ref[4:5] += jnp.sum(dconv, axis=0, keepdims=True)
    dtaps_ref[5:6, 2 * N_STATE :] += jnp.sum(dy * inner, axis=0, keepdims=True)
    dcat[rows : rows + 8] = dconv[0:8]
    dshared_ref[...] = draw[:, : 2 * N_STATE].T.astype(bf16)
    dmain_ref[...] = join_pairs(dgate, draw[:, 2 * N_STATE :], heads).astype(bf16)


def mixer_backward(main, small, head, taps, y, states, dgated, heads):
    length, width = y.shape
    count = length // CHUNK
    all_w = width + 2 * N_STATE
    per = CHUNK // 16

    def at(i):
        return (count - 1 - i, 0)

    def before(i):
        return (jnp.maximum((count - 1 - i) * per - 1, 0), 0)

    def fixed(i):
        return (0, 0)

    return pl.pallas_call(
        functools.partial(bwd_kernel, heads, count),
        grid=(count,),
        in_specs=[
            pl.BlockSpec((CHUNK, 2 * width), at),
            pl.BlockSpec((CHUNK, 3 * LANES), at),
            pl.BlockSpec((16, 2 * width), before),
            pl.BlockSpec((16, 3 * LANES), before),
            pl.BlockSpec((8, LANES), fixed),
            pl.BlockSpec((8, all_w), fixed),
            pl.BlockSpec((CHUNK, width), at),
            pl.BlockSpec((1, N_STATE, width), lambda i: (count - 1 - i, 0, 0)),
            pl.BlockSpec((CHUNK, width), at),
        ],
        out_specs=[
            pl.BlockSpec((CHUNK, 2 * width), at),
            pl.BlockSpec((2 * N_STATE, CHUNK), lambda i: (0, count - 1 - i)),
            pl.BlockSpec((STEP_ROWS, CHUNK), lambda i: (0, count - 1 - i)),
            pl.BlockSpec((8, all_w), fixed),
            pl.BlockSpec((8, LANES), fixed),
        ],
        out_shape=[
            jax.ShapeDtypeStruct((length, 2 * width), bf16),
            jax.ShapeDtypeStruct((2 * N_STATE, length), bf16),
            jax.ShapeDtypeStruct((STEP_ROWS, length), bf16),
            jax.ShapeDtypeStruct((8, all_w), f32),
            jax.ShapeDtypeStruct((8, LANES), f32),
        ],
        scratch_shapes=[
            pltpu.VMEM((N_STATE, width), f32),
            pltpu.VMEM((CHUNK + 8, all_w), f32),
            pltpu.VMEM((CHUNK + 8, all_w), f32),
        ],
        name="mixer_backward",
    )(main, small, main, small, head, taps, y, states, dgated)


MESH = pl.DeviceIdType.MESH


def greet(peers, count):
    barrier = pltpu.get_barrier_semaphore()
    for peer in peers:
        pl.semaphore_signal(barrier, inc=1, device_id=peer, device_id_type=MESH)
    pl.semaphore_wait(barrier, count)


def wire(src, dst, send, recv, peer):
    return pltpu.make_async_remote_copy(
        src_ref=src,
        dst_ref=dst,
        send_sem=send,
        recv_sem=recv,
        device_id=peer,
        device_id_type=MESH,
    )


def weights_kernel(n_seq, n_wsh, main, small, w_main, w_small, *sems):
    send_a, recv_a, send_b, recv_b, send_e, recv_e, send_r, recv_r, send_l, recv_l, own = sems
    s = lax.axis_index("seq")
    w = lax.axis_index("wshard")
    row = [(lax.rem(s + k, n_seq), w) for k in range(1, n_seq)]
    col = [(s, lax.rem(w + j, n_wsh)) for j in range(1, n_wsh)]
    greet(row + col, n_seq + n_wsh - 2)
    first = [
        wire(main.at[peer[0]], w_main.at[s, w], send_a.at[k], recv_a.at[k], peer)
        for k, peer in enumerate(row)
    ]
    spread = [
        wire(small, w_small.at[s, w], send_b.at[j], recv_b.at[j], peer)
        for j, peer in enumerate(col)
    ]
    third = [
        wire(w_small.at[s], w_small.at[s], send_e.at[k], recv_e.at[k], peer)
        for k, peer in enumerate(row)
    ]
    mine = [
        pltpu.make_async_copy(main.at[s], w_main.at[s, w], own.at[0]),
        pltpu.make_async_copy(small, w_small.at[s, w], own.at[1]),
    ]

    def right(t):
        block = w_main.at[:, jnp.maximum(w - t, 0)]
        peer = (s, jnp.minimum(w + 1, n_wsh - 1))
        return wire(block, block, send_r.at[t], recv_r.at[t], peer)

    def left(t):
        block = w_main.at[:, jnp.minimum(w + t, n_wsh - 1)]
        peer = (s, jnp.maximum(w - 1, 0))
        return wire(block, block, send_l.at[t], recv_l.at[t], peer)

    for copy in mine + first + spread:
        copy.start()
    mine[0].wait()
    for copy in first:
        copy.wait_recv()
    last = n_wsh - 1
    for t in range(n_wsh):
        if t > 0:
            pl.when(w >= t)(lambda t=t: right(t - 1).wait_recv())
        if t < last:
            pl.when((w >= t) & (w < last))(lambda t=t: right(t).start())
        if t > 0:
            pl.when(w + t <= last)(lambda t=t: left(t - 1).wait_recv())
        if t < last:
            pl.when((w + t <= last) & (w > 0))(lambda t=t: left(t).start())
        if t == 0:
            mine[1].wait()
            for copy in spread:
                copy.wait_recv()
            for copy in third:
                copy.start()
    for copy in first + spread:
        copy.wait_send()
    for copy in third:
        copy.wait()
    for t in range(last):
        pl.when((w >= t) & (w < last))(lambda t=t: right(t).wait_send())
        pl.when((w + t <= last) & (w > 0))(lambda t=t: left(t).wait_send())


def spread_weights(main, small, n_seq, n_wsh):
    rows_in, cols = main.shape[1:]
    anywhere = pl.BlockSpec(memory_space=pl.ANY)
    dma = pltpu.SemaphoreType.DMA
    a, c = n_seq - 1, n_wsh - 1
    return pl.pallas_call(
        functools.partial(weights_kernel, n_seq, n_wsh),
        in_specs=[anywhere] * 2,
        out_specs=[anywhere] * 2,
        out_shape=[
            jax.ShapeDtypeStruct((n_seq, n_wsh, rows_in, cols), bf16),
            jax.ShapeDtypeStruct((n_seq, n_wsh) + small.shape, bf16),
        ],
        scratch_shapes=[dma((n,)) for n in (a, a, c, c, a, a, c, c, c, c, 2)],
        compiler_params=pltpu.CompilerParams(collective_id=0, has_side_effects=True),
        cost_estimate=pl.CostEstimate(
            flops=0, bytes_accessed=200_000_000, transcendentals=0
        ),
        name="spread_weights",
    )(main, small)


def swap_kernel(plan, n_seq, n_wsh, *refs):
    n = len(plan)
    ins, outs, sems = refs[:n], refs[n : 2 * n], refs[2 * n :]
    s = lax.axis_index("seq")
    w = lax.axis_index("wshard")
    total = n_seq * n_wsh
    me_all = s * n_wsh + w
    size = {"seq": n_seq, "wshard": n_wsh, "both": total}
    me_of = {"seq": s, "wshard": w, "both": me_all}

    def peer_at(axis, k):
        if axis == "seq":
            index = lax.rem(s + k, n_seq)
            return index, (index, w)
        if axis == "wshard":
            index = lax.rem(w + k, n_wsh)
            return index, (s, index)
        index = lax.rem(me_all + k, total)
        return index, (lax.div(index, n_wsh), lax.rem(index, n_wsh))

    def block(kind, ref, index):
        if kind == "all":
            return ref
        return ref.at[index] if kind == 0 else ref.at[:, index]

    def copy_of(i, k):
        kind, axis = plan[i]
        index, peer = peer_at(axis, k)
        return wire(
            block(kind, ins[i], index),
            outs[i].at[me_of[axis]],
            sems[3 * i].at[k],
            sems[3 * i + 1].at[k],
            peer,
        )

    widest = "both" if any(axis == "both" for _, axis in plan) else plan[0][1]
    barrier = pltpu.get_barrier_semaphore()

    def hail(k, _):
        pl.semaphore_signal(
            barrier, inc=1, device_id=peer_at(widest, k)[1], device_id_type=MESH
        )
        return 0

    lax.fori_loop(1, size[widest], hail, 0)
    pl.semaphore_wait(barrier, size[widest] - 1)
    own = []
    for i, (kind, axis) in enumerate(plan):
        me = me_of[axis]
        own.append(
            pltpu.make_async_copy(
                block(kind, ins[i], me), outs[i].at[me], sems[3 * i + 2].at[0]
            )
        )

        def begin(k, _, i=i):
            copy_of(i, k).start()
            return 0

        lax.fori_loop(1, size[axis], begin, 0)
    for copy in own:
        copy.start()
    for i, (kind, axis) in enumerate(plan):
        own[i].wait()

        def finish(k, _, i=i):
            copy_of(i, k).wait()
            return 0

        lax.fori_loop(1, size[axis], finish, 0)


def swap(arrays, plan, n_seq, n_wsh, collective_id, name):
    anywhere = pl.BlockSpec(memory_space=pl.ANY)
    size = {"seq": n_seq, "wshard": n_wsh, "both": n_seq * n_wsh}
    shapes, sems = [], []
    for x, (kind, axis) in zip(arrays, plan):
        n = size[axis]
        shape = x.shape
        if kind == 0:
            shape = shape[1:]
        elif kind == 1:
            shape = shape[:1] + shape[2:]
        shapes.append(jax.ShapeDtypeStruct((n,) + shape, x.dtype))
        sems += [
            pltpu.SemaphoreType.DMA((n,)),
            pltpu.SemaphoreType.DMA((n,)),
            pltpu.SemaphoreType.DMA((1,)),
        ]
    return pl.pallas_call(
        functools.partial(swap_kernel, plan, n_seq, n_wsh),
        in_specs=[anywhere] * len(arrays),
        out_specs=[anywhere] * len(arrays),
        out_shape=shapes,
        scratch_shapes=sems,
        compiler_params=pltpu.CompilerParams(
            collective_id=collective_id, has_side_effects=True
        ),
        name=name,
    )(*arrays)


def stats_kernel(n_seq, x_ref, out_ref, slots, send, recv):
    s = lax.axis_index("seq")
    w = lax.axis_index("wshard")
    row = [(lax.rem(s + k, n_seq), w) for k in range(1, n_seq)]
    greet(row, n_seq - 1)
    copies = [
        wire(x_ref, slots.at[s], send.at[k], recv.at[k], peer)
        for k, peer in enumerate(row)
    ]
    for copy in copies:
        copy.start()
    slots[s] = x_ref[...]
    for copy in copies:
        copy.wait()
    total = slots[0]
    for k in range(1, n_seq):
        total = total + slots[k]
    out_ref[...] = total


def sum_over_seq(x, n_seq):
    vmem = pl.BlockSpec(memory_space=pltpu.VMEM)
    dma = pltpu.SemaphoreType.DMA
    return pl.pallas_call(
        functools.partial(stats_kernel, n_seq),
        in_specs=[vmem],
        out_specs=vmem,
        out_shape=jax.ShapeDtypeStruct(x.shape, f32),
        scratch_shapes=[
            pltpu.VMEM((n_seq,) + x.shape, f32),
            dma((n_seq - 1,)),
            dma((n_seq - 1,)),
        ],
        compiler_params=pltpu.CompilerParams(collective_id=1, has_side_effects=True),
        name="sum_over_seq",
    )(x)


def adamw(param, grad, first, second_moment, rate, decay):
    first_new = beta_one * first + (1.0 - beta_one) * grad
    second_new = beta_two * second_moment + (1.0 - beta_two) * grad * grad
    corrected = (
        first_new
        / (1.0 - beta_one**adam_step)
        / (jnp.sqrt(second_new / (1.0 - beta_two**adam_step)) + adam_eps)
    )
    return (param - rate * (corrected + decay * param), first_new, second_new)


def local(
    block_in,
    cotangent,
    in_weight,
    out_weight,
    in_gain,
    out_gain,
    conv_inner,
    conv_shared,
    head_params,
    first_in_weight,
    first_out_weight,
    first_in_gain,
    first_out_gain,
    first_conv_inner,
    first_conv_shared,
    first_head_params,
    second_in_weight,
    second_out_weight,
    second_in_gain,
    second_out_gain,
    second_conv_inner,
    second_conv_shared,
    second_head_params,
):
    seq_index = lax.axis_index("seq")
    wsh_index = lax.axis_index("wshard")
    n_seq = lax.axis_size("seq")
    n_wsh = lax.axis_size("wshard")
    rows_in, cols_in = in_weight.shape
    rows_out = out_weight.shape[0]
    tokens, width_in = block_in.shape[1:]
    heads = head_params.shape[1] // n_seq
    width = heads * P_SIZE
    inner_all = out_gain.shape[0]
    share = 2 * N_STATE // n_seq

    inputs = block_in[0].astype(f32)
    rms_in = lax.rsqrt(jnp.mean(inputs * inputs, axis=-1, keepdims=True) + norm_eps)
    normed = (inputs * rms_in * in_gain).astype(bf16)
    normed_all = lax.all_gather(normed, "seq", axis=0, tiled=True)
    cot = cotangent[0]
    cot_all = lax.all_gather(cot, "seq", axis=0, tiled=True)
    in_w16 = in_weight.astype(bf16)
    main_send = in_w16[:, : 2 * inner_all].reshape(rows_in, n_seq, 2 * width)
    main_send = jnp.swapaxes(main_send, 0, 1)
    small_send = in_w16[:, 2 * inner_all :]
    small_send = jnp.pad(small_send, ((0, 0), (0, -small_send.shape[1] % LANES)))
    w_main, w_small = spread_weights(main_send, small_send, n_seq, n_wsh)
    out_w16, w_main = lax.optimization_barrier((out_weight.astype(bf16), w_main))
    w_main = w_main.reshape(width_in, 2 * width)
    w_small = w_small.reshape(width_in, small_send.shape[1])
    w_out = jnp.zeros((n_wsh,) + out_w16.shape, bf16)
    w_out = lax.dynamic_update_index_in_dim(w_out, out_w16, wsh_index, 0)
    for j in range(1, n_wsh):
        got = lax.ppermute(out_w16, "wshard", [(i, (i + j) % n_wsh) for i in range(n_wsh)])
        w_out = lax.dynamic_update_index_in_dim(
            w_out, got, lax.rem(wsh_index - j + n_wsh, n_wsh), 0
        )
    w_out = w_out.reshape(width, width_in)

    def pick(first, count, width_to):
        col = lax.broadcasted_iota(jnp.int32, (w_small.shape[1], width_to), 0)
        lane = lax.broadcasted_iota(jnp.int32, (w_small.shape[1], width_to), 1)
        return jnp.where((col == lane + first) & (lane < count), 1.0, 0.0)

    first_step = 2 * N_STATE + seq_index * heads
    to_step = pick(first_step, heads, LANES)
    to_fwd = jnp.concatenate([pick(0, 2 * N_STATE, 2 * N_STATE), to_step], axis=1)
    to_ext = jnp.concatenate(
        [pick(seq_index * share, share, share), to_step[:, :STEP_ROWS]], axis=1
    )
    w_fwd = mm(w_small, to_fwd.astype(bf16), NN).astype(bf16)
    w_ext = mm(w_small, to_ext.astype(bf16), NN).astype(bf16)

    main = mm(normed_all, w_main, NN).astype(bf16)
    small = mm(normed_all, w_fwd, NN).astype(bf16)
    head_local = lax.dynamic_slice_in_dim(head_params, seq_index * heads, heads, 1)
    head = jnp.pad(head_local, ((0, 5), (0, LANES - heads)))
    conv_local = lax.dynamic_slice_in_dim(conv_inner, seq_index * width, width, 1)
    taps = jnp.pad(jnp.concatenate([conv_shared, conv_local], axis=1), ((0, 3), (0, 0)))
    gain_local = lax.dynamic_slice_in_dim(out_gain, seq_index * width, width, 0)
    gated, y, states = mixer_forward(main, small, head, taps, heads)
    d_gnormed = mm(cot_all, w_out, NT)
    gated32 = gated.astype(f32)
    scaled = d_gnormed * gain_local
    stats = jnp.stack(
        [jnp.sum(gated32 * gated32, axis=-1), jnp.sum(scaled * gated32, axis=-1)]
    )
    stats = sum_over_seq(stats.reshape(-1, LANES), n_seq).reshape(stats.shape)
    rms_out = lax.rsqrt(stats[0] / inner_all + norm_eps)[:, None]
    mean_sg = (stats[1] / inner_all)[:, None]
    gnormed = (gated32 * rms_out * gain_local).astype(bf16)
    d_gated = (rms_out * scaled - gated32 * rms_out**3 * mean_sg).astype(bf16)
    d_out_gain = jnp.sum(d_gnormed * gated32 * rms_out, axis=0)

    g_out = mm(gnormed, cot_all, TN)
    mixed = mm(gnormed, w_out, NN).astype(bf16)
    g_out, mixed, d_gated = lax.optimization_barrier((g_out, mixed, d_gated))
    mixed = lax.psum_scatter(mixed, "seq", scatter_dimension=0, tiled=True)
    block_out = (inputs + mixed.astype(f32))[None]
    grad_out_weight = lax.dynamic_slice_in_dim(g_out, wsh_index * rows_out, rows_out, 0)
    for j in range(1, n_wsh):
        to = lax.rem(wsh_index + j, n_wsh)
        part = lax.dynamic_slice_in_dim(g_out, to * rows_out, rows_out, 0)
        grad_out_weight = grad_out_weight + lax.ppermute(
            part, "wshard", [(i, (i + j) % n_wsh) for i in range(n_wsh)]
        )
    dmain, dshared_t, dstep_t, dtaps, dhead = mixer_backward(
        main, small, head, taps, y, states, d_gated, heads
    )

    (shared_parts,) = swap(
        (dshared_t.reshape(n_seq, share, -1),), ((0, "seq"),), n_seq, n_wsh, 2, "swap_shared"
    )
    shared_sum = jnp.sum(shared_parts.astype(f32), axis=0).astype(bf16)
    d_ext = jnp.concatenate([shared_sum, dstep_t], axis=0)
    d_normed = mm(dmain, w_main, NT) + lax.dot_general(
        d_ext, w_ext, (((0,), (1,)), ((), ())), preferred_element_type=f32
    )
    d_normed = lax.psum_scatter(
        d_normed.astype(bf16), "seq", scatter_dimension=0, tiled=True
    ).astype(f32)

    g_main = mm(normed_all, dmain, TN).astype(bf16).reshape(n_seq, n_wsh, rows_in, 2 * width)
    g_ext = lax.dot_general(
        normed_all, d_ext, (((0,), (1,)), ((), ())), preferred_element_type=f32
    ).astype(bf16)
    g_ext = jnp.pad(g_ext, ((0, 0), (0, -g_ext.shape[1] % LANES)))
    g_ext = g_ext.reshape(n_seq, n_wsh, rows_in, LANES)

    def pack(parts):
        flat = jnp.concatenate([p.reshape(-1) for p in parts])
        return jnp.pad(flat, (0, -flat.shape[0] % (8 * LANES))).reshape(-1, LANES)

    d_skip = dtaps[5, 2 * N_STATE :].reshape(heads, P_SIZE).sum(-1)
    d_head = jnp.concatenate([dhead[:2, :heads], d_skip[None]], axis=0)
    pieces = (dtaps[:5, : 2 * N_STATE], d_out_gain, dtaps[:5, 2 * N_STATE :], d_head)
    g_main, g_ext, flat = swap(
        (g_main, g_ext, pack(pieces)),
        ((1, "wshard"), (1, "wshard"), ("all", "wshard")),
        n_seq,
        n_wsh,
        3,
        "swap_grads",
    )
    g_main = jnp.sum(g_main.astype(f32), axis=0).astype(bf16)
    g_ext = jnp.sum(g_ext.astype(f32), axis=0).astype(bf16)
    flat = jnp.sum(flat, axis=0)

    d_in_gain = jnp.sum(d_normed * inputs * rms_in, axis=0)
    scaled_in = d_normed * in_gain
    grad_in = (
        cot.astype(f32)
        + rms_in * scaled_in
        - inputs * rms_in**3 * jnp.mean(scaled_in * inputs, axis=-1, keepdims=True)
    )[None]

    g_main, g_ext, flat, in_gain_parts = swap(
        (g_main, g_ext, flat, pack((d_in_gain,))),
        ((0, "seq"), (0, "seq"), ("all", "seq"), ("all", "both")),
        n_seq,
        n_wsh,
        4,
        "swap_last",
    )
    g_main = jnp.swapaxes(g_main, 0, 1).reshape(rows_in, 2 * inner_all)
    g_ext = jnp.swapaxes(g_ext, 0, 1)
    grad_in_weight = jnp.concatenate(
        [
            g_main,
            g_ext[:, :, :share].reshape(rows_in, 2 * N_STATE),
            g_ext[:, :, share : share + heads].reshape(rows_in, heads * n_seq),
        ],
        axis=1,
    ).astype(f32)
    grad_in_gain = jnp.sum(in_gain_parts, axis=0).reshape(-1)[:width_in]
    flat = flat.reshape(n_seq, -1)
    sums, at = [], 0
    for p in pieces:
        sums.append(flat[:, at : at + p.size].reshape((n_seq,) + p.shape))
        at += p.size
    grad_conv_shared = jnp.sum(sums[0], axis=0)
    grad_out_gain = sums[1].reshape(-1)
    grad_conv_inner = jnp.swapaxes(sums[2], 0, 1).reshape(conv_inner.shape)
    grad_head_params = jnp.swapaxes(sums[3], 0, 1).reshape(head_params.shape)
    new_in_weight, new_first_in_weight, new_second_in_weight = adamw(
        in_weight,
        grad_in_weight,
        first_in_weight,
        second_in_weight,
        weight_learning_rate,
        matrix_decay,
    )
    new_out_weight, new_first_out_weight, new_second_out_weight = adamw(
        out_weight,
        grad_out_weight,
        first_out_weight,
        second_out_weight,
        weight_learning_rate,
        matrix_decay,
    )
    updated_input_gain, new_first_in_gain, new_second_in_gain = adamw(
        in_gain, grad_in_gain, first_in_gain, second_in_gain, small_rate, 0.0
    )
    new_out_gain, new_first_out_gain, new_second_out_gain = adamw(
        out_gain, grad_out_gain, first_out_gain, second_out_gain, small_rate, 0.0
    )
    new_conv_inner, new_first_conv_inner, new_second_conv_inner = adamw(
        conv_inner, grad_conv_inner, first_conv_inner, second_conv_inner, small_rate, 0.0
    )
    new_conv_shared, new_first_conv_shared, new_second_conv_shared = adamw(
        conv_shared, grad_conv_shared, first_conv_shared, second_conv_shared, small_rate, 0.0
    )
    new_head_params, updated_head_first_moment, head_second_all = adamw(
        head_params, grad_head_params, first_head_params, second_head_params, small_rate, 0.0
    )
    return (
        block_out,
        grad_in,
        grad_in_weight,
        grad_out_weight,
        grad_in_gain,
        grad_out_gain,
        grad_conv_inner,
        grad_conv_shared,
        grad_head_params,
        new_in_weight,
        new_out_weight,
        updated_input_gain,
        new_out_gain,
        new_conv_inner,
        new_conv_shared,
        new_head_params,
        new_first_in_weight,
        new_first_out_weight,
        new_first_in_gain,
        new_first_out_gain,
        new_first_conv_inner,
        new_first_conv_shared,
        updated_head_first_moment,
        new_second_in_weight,
        new_second_out_weight,
        new_second_in_gain,
        new_second_out_gain,
        new_second_conv_inner,
        new_second_conv_shared,
        head_second_all[0:2],
        head_second_all[2],
    )


def solution(mesh):
    return jax.shard_map(
        local,
        mesh=mesh,
        in_specs=(
            P("wshard", "seq", None),
            P("wshard", "seq", None),
            P(("seq", "wshard"), None),
            P(("seq", "wshard"), None),
            P(),
            P(),
            P(),
            P(),
            P(),
            P(("seq", "wshard"), None),
            P(("seq", "wshard"), None),
            P(),
            P(),
            P(),
            P(),
            P(),
            P(("seq", "wshard"), None),
            P(("seq", "wshard"), None),
            P(),
            P(),
            P(),
            P(),
            P(),
        ),
        out_specs=(
            P("wshard", "seq", None),
            P("wshard", "seq", None),
            P(("seq", "wshard"), None),
            P(("seq", "wshard"), None),
            P(),
            P(),
            P(),
            P(),
            P(),
            P(("seq", "wshard"), None),
            P(("seq", "wshard"), None),
            P(),
            P(),
            P(),
            P(),
            P(),
            P(("seq", "wshard"), None),
            P(("seq", "wshard"), None),
            P(),
            P(),
            P(),
            P(),
            P(),
            P(("seq", "wshard"), None),
            P(("seq", "wshard"), None),
            P(),
            P(),
            P(),
            P(),
            P(),
            P(),
        ),
        check_vma=False,
    )
```

```python
import functools

import jax
import jax.numpy as jnp
from jax import lax
from jax.experimental import pallas as pl
from jax.experimental.pallas import tpu as pltpu
from jax.sharding import PartitionSpec as P


P_SIZE = 64
N_STATE = 128
LANES = 128
CHUNK = 128
STEP_ROWS = 16

norm_eps = 1e-05
beta_one = 0.9
beta_two = 0.95
adam_eps = 1e-08
adam_step = 3.0
weight_learning_rate = 0.01
matrix_decay = 0.1
small_rate = 0.1


f32 = jnp.float32
bf16 = jnp.bfloat16
NN = (((1,), (0,)), ((), ()))
NT = (((1,), (1,)), ((), ()))
TN = (((0,), (0,)), ((), ()))


def mm(a, b, dims):
    return lax.dot_general(a, b, dims, preferred_element_type=f32)


def mm_high(a, b):
    return lax.dot_general(
        a, b, NN, precision=lax.Precision.HIGHEST, preferred_element_type=f32
    )


def two_parts(a):
    hi = a.astype(bf16)
    return hi, (a - hi.astype(f32)).astype(bf16)


def mm3(a, b, dims):
    return mm(a[0], b[0], dims) + (mm(a[0], b[1], dims) + mm(a[1], b[0], dims))


def low_half(rows):
    return lax.broadcasted_iota(jnp.int32, (rows, LANES), 1) < P_SIZE


def split_pairs(values, heads):
    low = low_half(values.shape[0])
    gates, inners = [], []
    for h in range(0, heads, 2):
        a = values[:, h * LANES : (h + 1) * LANES]
        a_r = pltpu.roll(a, P_SIZE, 1)
        if h + 1 < heads:
            b = values[:, (h + 1) * LANES : (h + 2) * LANES]
            b_r = pltpu.roll(b, P_SIZE, 1)
            gates.append(jnp.where(low, a, b_r))
            inners.append(jnp.where(low, a_r, b))
        else:
            gates.append(a[:, :P_SIZE])
            inners.append(a_r[:, :P_SIZE])
    return jnp.concatenate(gates, axis=1), jnp.concatenate(inners, axis=1)


def join_pairs(gate, inner, heads):
    low = low_half(gate.shape[0])
    out = []
    for h in range(0, heads, 2):
        if h + 1 < heads:
            g = gate[:, h * P_SIZE : (h + 2) * P_SIZE]
            x = inner[:, h * P_SIZE : (h + 2) * P_SIZE]
            out.append(jnp.where(low, g, pltpu.roll(x, P_SIZE, 1)))
            out.append(jnp.where(low, pltpu.roll(g, P_SIZE, 1), x))
        else:
            out.append(
                jnp.concatenate(
                    [gate[:, h * P_SIZE :], inner[:, h * P_SIZE :]], axis=1
                )
            )
    return jnp.concatenate(out, axis=1)


def expand(cols, heads):
    rows = cols.shape[0]
    low = low_half(rows)
    out = []
    for h in range(0, heads, 2):
        if h + 1 < heads:
            one = jnp.broadcast_to(cols[:, h : h + 1], (rows, LANES))
            two = jnp.broadcast_to(cols[:, h + 1 : h + 2], (rows, LANES))
            out.append(jnp.where(low, one, two))
        else:
            out.append(jnp.broadcast_to(cols[:, h : h + 1], (rows, P_SIZE)))
    return jnp.concatenate(out, axis=1)


def pair_of(values, h, heads):
    first = h - h % 2
    return values[:, first * P_SIZE : min(first + 2, heads) * P_SIZE]


def merge_pairs(parts, heads):
    low = low_half(parts[0].shape[0])
    out = []
    for h in range(0, heads, 2):
        if h + 1 < heads:
            out.append(jnp.where(low, parts[h], parts[h + 1]))
        else:
            out.append(parts[h])
    return jnp.concatenate(out, axis=1)


def chunk_common(heads, main, small, cat, head_ref, taps_ref):
    rows = main.shape[0]
    gate, inner = split_pairs(main, heads)
    raw = jnp.concatenate([small[:, : 2 * N_STATE], inner], axis=1)
    cat[8 : 8 + rows] = raw
    conv = taps_ref[4:5] + taps_ref[0:1] * cat[5 : 5 + rows]
    for k in range(1, 4):
        conv = conv + taps_ref[k : k + 1] * cat[5 + k : 5 + k + rows]
    step_in = small[:, 2 * N_STATE :] + head_ref[0:1]
    dt = jnp.maximum(step_in, 0.0) + jnp.log1p(jnp.exp(-jnp.abs(step_in)))
    neg_rate = -jnp.exp(head_ref[1:2])
    decay_log = neg_rate * dt
    r = lax.broadcasted_iota(jnp.int32, (rows, rows), 0)
    c = lax.broadcasted_iota(jnp.int32, (rows, rows), 1)
    tri = jnp.where(r >= c, 1.0, 0.0).astype(f32)
    cumul = mm_high(tri, decay_log)
    return gate, conv, step_in, dt, neg_rate, decay_log, cumul, r, c


def fwd_kernel(
    heads, main_ref, small_ref, head_ref, taps_ref, gated_ref, y_ref, states_ref, state, cat
):
    rows = main_ref.shape[0]

    @pl.when(pl.program_id(0) == 0)
    def _():
        state[...] = jnp.zeros_like(state)
        cat[0:8] = jnp.zeros((8, cat.shape[1]), f32)

    gate, conv, _, dt, _, _, cumul, r, c = chunk_common(
        heads,
        main_ref[...].astype(f32),
        small_ref[...].astype(f32),
        cat,
        head_ref,
        taps_ref,
    )
    cat[0:8] = cat[rows : rows + 8]
    act = conv * jax.nn.sigmoid(conv)
    b2 = two_parts(act[:, :N_STATE])
    c2 = two_parts(act[:, N_STATE : 2 * N_STATE])
    inner = act[:, 2 * N_STATE :]
    scaled = inner * expand(dt, heads)
    scaled2 = two_parts(scaled)
    scores = mm3(c2, b2, NT)
    lower = r >= c
    cumul_t = cumul.T
    parts = []
    for h in range(heads):
        spread = cumul[:, h : h + 1] - cumul_t[h : h + 1, :]
        weights = two_parts(scores * jnp.exp(jnp.where(lower, spread, -1e30)))
        own = tuple(pair_of(part, h, heads) for part in scaled2)
        parts.append(mm3(weights, own, NN))
    s2 = two_parts(state[...])
    states_ref[0] = state[...]
    last = cumul[rows - 1 : rows]
    y = merge_pairs(parts, heads) + expand(jnp.exp(cumul), heads) * mm3(c2, s2, NN)
    y_ref[...] = y
    tail = expand(jnp.exp(last - cumul), heads)
    fresh = mm3(b2, two_parts(tail * scaled), TN)
    state[...] = expand(jnp.exp(last), heads) * state[...] + fresh
    full = y + expand(head_ref[2:3], heads) * inner
    gated_ref[...] = (full * (gate * jax.nn.sigmoid(gate))).astype(bf16)


def mixer_forward(main, small, head, taps, heads):
    length = main.shape[0]
    width = heads * P_SIZE
    count = length // CHUNK
    all_w = width + 2 * N_STATE
    return pl.pallas_call(
        functools.partial(fwd_kernel, heads),
        grid=(count,),
        in_specs=[
            pl.BlockSpec((CHUNK, 2 * width), lambda i: (i, 0)),
            pl.BlockSpec((CHUNK, 3 * LANES), lambda i: (i, 0)),
            pl.BlockSpec((8, LANES), lambda i: (0, 0)),
            pl.BlockSpec((8, all_w), lambda i: (0, 0)),
        ],
        out_specs=[
            pl.BlockSpec((CHUNK, width), lambda i: (i, 0)),
            pl.BlockSpec((CHUNK, width), lambda i: (i, 0)),
            pl.BlockSpec((1, N_STATE, width), lambda i: (i, 0, 0)),
        ],
        out_shape=[
            jax.ShapeDtypeStruct((length, width), bf16),
            jax.ShapeDtypeStruct((length, width), f32),
            jax.ShapeDtypeStruct((count, N_STATE, width), f32),
        ],
        scratch_shapes=[
            pltpu.VMEM((N_STATE, width), f32),
            pltpu.VMEM((CHUNK + 8, all_w), f32),
        ],
        cost_estimate=pl.CostEstimate(
            flops=0, bytes_accessed=70_000_000, transcendentals=0
        ),
        name="mixer_forward",
    )(main, small, head, taps)


def bwd_kernel(
    heads,
    count,
    main_ref,
    small_ref,
    main_prev,
    small_prev,
    head_ref,
    taps_ref,
    y_ref,
    states_ref,
    dgated_ref,
    dmain_ref,
    dshared_ref,
    dstep_ref,
    dtaps_ref,
    dhead_ref,
    dstate,
    cat,
    dcat,
):
    rows, width = y_ref.shape
    step = pl.program_id(0)

    @pl.when(step == 0)
    def _():
        dstate[...] = jnp.zeros_like(dstate)
        dcat[rows : rows + 8] = jnp.zeros((8, dcat.shape[1]), f32)
        dtaps_ref[...] = jnp.zeros_like(dtaps_ref)
        dhead_ref[...] = jnp.zeros_like(dhead_ref)

    _, inner_prev = split_pairs(main_prev[8:16].astype(f32), heads)
    prev = jnp.concatenate(
        [small_prev[8:16].astype(f32)[:, : 2 * N_STATE], inner_prev], axis=1
    )
    cat[0:8] = jnp.where(step == count - 1, 0.0, prev)
    gate, conv, step_in, dt, neg_rate, decay_log, cumul, r, c = chunk_common(
        heads,
        main_ref[...].astype(f32),
        small_ref[...].astype(f32),
        cat,
        head_ref,
        taps_ref,
    )
    sig = jax.nn.sigmoid(conv)
    act = conv * sig
    dsilu = sig * (1.0 + conv * (1.0 - sig))
    b2 = two_parts(act[:, :N_STATE])
    c2 = two_parts(act[:, N_STATE : 2 * N_STATE])
    inner = act[:, 2 * N_STATE :]
    dt_x = expand(dt, heads)
    scaled = inner * dt_x
    scaled2 = two_parts(scaled)
    skip = expand(head_ref[2:3], heads)
    y = y_ref[...]
    sgate = jax.nn.sigmoid(gate)
    dgated = dgated_ref[...].astype(f32)
    dgate = dgated * (y + skip * inner) * (sgate * (1.0 + gate * (1.0 - sgate)))
    dy = dgated * (gate * sgate)
    dy2 = two_parts(dy)

    scores_t = mm3(b2, c2, NT)
    upper = c >= r
    cumul_t = cumul.T
    low = low_half(rows)
    parts = []
    dscores_t = None
    for h in range(heads):
        spread = cumul_t[h : h + 1, :] - cumul[:, h : h + 1]
        decay = jnp.exp(jnp.where(upper, spread, -1e30))
        weights = two_parts(scores_t * decay)
        dy_pair = tuple(pair_of(part, h, heads) for part in dy2)
        parts.append(mm3(weights, dy_pair, NN))
        own = pair_of(scaled, h, heads)
        if own.shape[1] == LANES:
            own = jnp.where(low == (h % 2 == 0), own, 0.0)
        term = mm3(two_parts(own), dy_pair, NT) * decay
        dscores_t = term if dscores_t is None else dscores_t + term
    s_in = states_ref[0]
    s2 = two_parts(s_in)
    ds = dstate[...]
    ds2 = two_parts(ds)
    last = cumul[rows - 1 : rows]
    tail = expand(jnp.exp(last - cumul), heads)
    ecum = expand(jnp.exp(cumul), heads)
    elast = expand(jnp.exp(last), heads)
    tail_b = tail * mm3(b2, ds2, NN)
    z = merge_pairs(parts, heads) + tail_b
    extra = jnp.sum(tail_b * scaled, axis=0, keepdims=True) + elast * jnp.sum(
        ds * s_in, axis=0, keepdims=True
    )
    at_end = lax.broadcasted_iota(jnp.int32, (rows, width), 0) == rows - 1
    u = dy * y - scaled * z + jnp.where(at_end, extra, 0.0)
    pick = (
        lax.broadcasted_iota(jnp.int32, (width, LANES), 0) // P_SIZE
        == lax.broadcasted_iota(jnp.int32, (width, LANES), 1)
    ).astype(f32)
    dcumul = mm_high(u, pick)
    suffix = jnp.where(c >= r, 1.0, 0.0).astype(f32)
    ddecay = mm_high(suffix, dcumul)
    dstep = (mm_high(inner * z, pick) + neg_rate * ddecay) * jax.nn.sigmoid(step_in)
    dstep_ref[...] = dstep.T[: dstep_ref.shape[0]].astype(bf16)
    dhead_ref[0:1] += jnp.sum(dstep, axis=0, keepdims=True)
    dhead_ref[1:2] += jnp.sum(decay_log * ddecay, axis=0, keepdims=True)

    dinner = dt_x * z + skip * dy
    dscores2 = two_parts(dscores_t)
    edy2 = two_parts(ecum * dy)
    db = mm3(dscores2, c2, NN) + mm3(two_parts(tail * scaled), ds2, NT)
    dc = mm3(dscores2, b2, TN) + mm3(edy2, s2, NT)
    dstate[...] = elast * ds + mm3(c2, edy2, TN)

    dconv = jnp.concatenate([db, dc, dinner], axis=1) * dsilu
    dcat[0:rows] = dconv
    draw = taps_ref[3:4] * dconv
    for k in range(3):
        draw = draw + taps_ref[k : k + 1] * dcat[3 - k : 3 - k + rows]
    for k in range(4):
        dtaps_ref[k : k + 1] += jnp.sum(
            dconv * cat[5 + k : 5 + k + rows], axis=0, keepdims=True
        )
    dtaps_ref[4:5] += jnp.sum(dconv, axis=0, keepdims=True)
    dtaps_ref[5:6, 2 * N_STATE :] += jnp.sum(dy * inner, axis=0, keepdims=True)
    dcat[rows : rows + 8] = dconv[0:8]
    dshared_ref[...] = draw[:, : 2 * N_STATE].T.astype(bf16)
    dmain_ref[...] = join_pairs(dgate, draw[:, 2 * N_STATE :], heads).astype(bf16)


def mixer_backward(main, small, head, taps, y, states, dgated, heads):
    length, width = y.shape
    count = length // CHUNK
    all_w = width + 2 * N_STATE
    per = CHUNK // 16

    def at(i):
        return (count - 1 - i, 0)

    def before(i):
        return (jnp.maximum((count - 1 - i) * per - 1, 0), 0)

    def fixed(i):
        return (0, 0)

    return pl.pallas_call(
        functools.partial(bwd_kernel, heads, count),
        grid=(count,),
        in_specs=[
            pl.BlockSpec((CHUNK, 2 * width), at),
            pl.BlockSpec((CHUNK, 3 * LANES), at),
            pl.BlockSpec((16, 2 * width), before),
            pl.BlockSpec((16, 3 * LANES), before),
            pl.BlockSpec((8, LANES), fixed),
            pl.BlockSpec((8, all_w), fixed),
            pl.BlockSpec((CHUNK, width), at),
            pl.BlockSpec((1, N_STATE, width), lambda i: (count - 1 - i, 0, 0)),
            pl.BlockSpec((CHUNK, width), at),
        ],
        out_specs=[
            pl.BlockSpec((CHUNK, 2 * width), at),
            pl.BlockSpec((2 * N_STATE, CHUNK), lambda i: (0, count - 1 - i)),
            pl.BlockSpec((STEP_ROWS, CHUNK), lambda i: (0, count - 1 - i)),
            pl.BlockSpec((8, all_w), fixed),
            pl.BlockSpec((8, LANES), fixed),
        ],
        out_shape=[
            jax.ShapeDtypeStruct((length, 2 * width), bf16),
            jax.ShapeDtypeStruct((2 * N_STATE, length), bf16),
            jax.ShapeDtypeStruct((STEP_ROWS, length), bf16),
            jax.ShapeDtypeStruct((8, all_w), f32),
            jax.ShapeDtypeStruct((8, LANES), f32),
        ],
        scratch_shapes=[
            pltpu.VMEM((N_STATE, width), f32),
            pltpu.VMEM((CHUNK + 8, all_w), f32),
            pltpu.VMEM((CHUNK + 8, all_w), f32),
        ],
        cost_estimate=pl.CostEstimate(
            flops=0, bytes_accessed=160_000_000, transcendentals=0
        ),
        name="mixer_backward",
    )(main, small, main, small, head, taps, y, states, dgated)


MESH = pl.DeviceIdType.MESH


def greet(peers, count):
    barrier = pltpu.get_barrier_semaphore()
    for peer in peers:
        pl.semaphore_signal(barrier, inc=1, device_id=peer, device_id_type=MESH)
    pl.semaphore_wait(barrier, count)


def wire(src, dst, send, recv, peer):
    return pltpu.make_async_remote_copy(
        src_ref=src,
        dst_ref=dst,
        send_sem=send,
        recv_sem=recv,
        device_id=peer,
        device_id_type=MESH,
    )


def weights_kernel(n_seq, n_wsh, main, small, w_main, w_small, *sems):
    send_a, recv_a, send_b, recv_b, send_e, recv_e, send_r, recv_r, send_l, recv_l, own = sems
    s = lax.axis_index("seq")
    w = lax.axis_index("wshard")
    row = [(lax.rem(s + k, n_seq), w) for k in range(1, n_seq)]
    col = [(s, lax.rem(w + j, n_wsh)) for j in range(1, n_wsh)]
    greet(row + col, n_seq + n_wsh - 2)
    first = [
        wire(main.at[peer[0]], w_main.at[s, w], send_a.at[k], recv_a.at[k], peer)
        for k, peer in enumerate(row)
    ]
    spread = [
        wire(small, w_small.at[s, w], send_b.at[j], recv_b.at[j], peer)
        for j, peer in enumerate(col)
    ]
    third = [
        wire(w_small.at[s], w_small.at[s], send_e.at[k], recv_e.at[k], peer)
        for k, peer in enumerate(row)
    ]
    mine = [
        pltpu.make_async_copy(main.at[s], w_main.at[s, w], own.at[0]),
        pltpu.make_async_copy(small, w_small.at[s, w], own.at[1]),
    ]

    def right(t):
        block = w_main.at[:, jnp.maximum(w - t, 0)]
        peer = (s, jnp.minimum(w + 1, n_wsh - 1))
        return wire(block, block, send_r.at[t], recv_r.at[t], peer)

    def left(t):
        block = w_main.at[:, jnp.minimum(w + t, n_wsh - 1)]
        peer = (s, jnp.maximum(w - 1, 0))
        return wire(block, block, send_l.at[t], recv_l.at[t], peer)

    for copy in mine + first + spread:
        copy.start()
    mine[0].wait()
    for copy in first:
        copy.wait_recv()
    last = n_wsh - 1
    for t in range(n_wsh):
        if t > 0:
            pl.when(w >= t)(lambda t=t: right(t - 1).wait_recv())
        if t < last:
            pl.when((w >= t) & (w < last))(lambda t=t: right(t).start())
        if t > 0:
            pl.when(w + t <= last)(lambda t=t: left(t - 1).wait_recv())
        if t < last:
            pl.when((w + t <= last) & (w > 0))(lambda t=t: left(t).start())
        if t == 0:
            mine[1].wait()
            for copy in spread:
                copy.wait_recv()
            for copy in third:
                copy.start()
    for copy in first + spread:
        copy.wait_send()
    for copy in third:
        copy.wait()
    for t in range(last):
        pl.when((w >= t) & (w < last))(lambda t=t: right(t).wait_send())
        pl.when((w + t <= last) & (w > 0))(lambda t=t: left(t).wait_send())


def spread_weights(main, small, n_seq, n_wsh):
    rows_in, cols = main.shape[1:]
    anywhere = pl.BlockSpec(memory_space=pl.ANY)
    dma = pltpu.SemaphoreType.DMA
    a, c = n_seq - 1, n_wsh - 1
    return pl.pallas_call(
        functools.partial(weights_kernel, n_seq, n_wsh),
        in_specs=[anywhere] * 2,
        out_specs=[anywhere] * 2,
        out_shape=[
            jax.ShapeDtypeStruct((n_seq, n_wsh, rows_in, cols), bf16),
            jax.ShapeDtypeStruct((n_seq, n_wsh) + small.shape, bf16),
        ],
        scratch_shapes=[dma((n,)) for n in (a, a, c, c, a, a, c, c, c, c, 2)],
        compiler_params=pltpu.CompilerParams(collective_id=0, has_side_effects=True),
        cost_estimate=pl.CostEstimate(
            flops=0, bytes_accessed=200_000_000, transcendentals=0
        ),
        name="spread_weights",
    )(main, small)


def swap_kernel(plan, n_seq, n_wsh, *refs):
    n = len(plan)
    ins, outs, sems = refs[:n], refs[n : 2 * n], refs[2 * n :]
    s = lax.axis_index("seq")
    w = lax.axis_index("wshard")
    total = n_seq * n_wsh
    me_all = s * n_wsh + w
    size = {"seq": n_seq, "wshard": n_wsh, "both": total}
    me_of = {"seq": s, "wshard": w, "both": me_all}

    def peer_at(axis, k):
        if axis == "seq":
            index = lax.rem(s + k, n_seq)
            return index, (index, w)
        if axis == "wshard":
            index = lax.rem(w + k, n_wsh)
            return index, (s, index)
        index = lax.rem(me_all + k, total)
        return index, (lax.div(index, n_wsh), lax.rem(index, n_wsh))

    def block(kind, ref, index):
        if kind == "all":
            return ref
        return ref.at[index] if kind == 0 else ref.at[:, index]

    def copy_of(i, k):
        kind, axis = plan[i]
        index, peer = peer_at(axis, k)
        return wire(
            block(kind, ins[i], index),
            outs[i].at[me_of[axis]],
            sems[3 * i].at[k],
            sems[3 * i + 1].at[k],
            peer,
        )

    widest = "both" if any(axis == "both" for _, axis in plan) else plan[0][1]
    barrier = pltpu.get_barrier_semaphore()

    def hail(k, _):
        pl.semaphore_signal(
            barrier, inc=1, device_id=peer_at(widest, k)[1], device_id_type=MESH
        )
        return 0

    lax.fori_loop(1, size[widest], hail, 0)
    pl.semaphore_wait(barrier, size[widest] - 1)
    own = []
    for i, (kind, axis) in enumerate(plan):
        me = me_of[axis]
        own.append(
            pltpu.make_async_copy(
                block(kind, ins[i], me), outs[i].at[me], sems[3 * i + 2].at[0]
            )
        )

        def begin(k, _, i=i):
            copy_of(i, k).start()
            return 0

        lax.fori_loop(1, size[axis], begin, 0)
    for copy in own:
        copy.start()
    for i, (kind, axis) in enumerate(plan):
        own[i].wait()

        def finish(k, _, i=i):
            copy_of(i, k).wait()
            return 0

        lax.fori_loop(1, size[axis], finish, 0)


def swap(arrays, plan, n_seq, n_wsh, collective_id):
    anywhere = pl.BlockSpec(memory_space=pl.ANY)
    size = {"seq": n_seq, "wshard": n_wsh, "both": n_seq * n_wsh}
    shapes, sems = [], []
    for x, (kind, axis) in zip(arrays, plan):
        n = size[axis]
        shape = x.shape
        if kind == 0:
            shape = shape[1:]
        elif kind == 1:
            shape = shape[:1] + shape[2:]
        shapes.append(jax.ShapeDtypeStruct((n,) + shape, x.dtype))
        sems += [
            pltpu.SemaphoreType.DMA((n,)),
            pltpu.SemaphoreType.DMA((n,)),
            pltpu.SemaphoreType.DMA((1,)),
        ]
    return pl.pallas_call(
        functools.partial(swap_kernel, plan, n_seq, n_wsh),
        in_specs=[anywhere] * len(arrays),
        out_specs=[anywhere] * len(arrays),
        out_shape=shapes,
        scratch_shapes=sems,
        compiler_params=pltpu.CompilerParams(
            collective_id=collective_id, has_side_effects=True
        ),
    )(*arrays)


def stats_kernel(n_seq, x_ref, out_ref, slots, send, recv):
    s = lax.axis_index("seq")
    w = lax.axis_index("wshard")
    row = [(lax.rem(s + k, n_seq), w) for k in range(1, n_seq)]
    greet(row, n_seq - 1)
    copies = [
        wire(x_ref, slots.at[s], send.at[k], recv.at[k], peer)
        for k, peer in enumerate(row)
    ]
    for copy in copies:
        copy.start()
    slots[s] = x_ref[...]
    for copy in copies:
        copy.wait()
    total = slots[0]
    for k in range(1, n_seq):
        total = total + slots[k]
    out_ref[...] = total


def sum_over_seq(x, n_seq):
    vmem = pl.BlockSpec(memory_space=pltpu.VMEM)
    dma = pltpu.SemaphoreType.DMA
    return pl.pallas_call(
        functools.partial(stats_kernel, n_seq),
        in_specs=[vmem],
        out_specs=vmem,
        out_shape=jax.ShapeDtypeStruct(x.shape, f32),
        scratch_shapes=[
            pltpu.VMEM((n_seq,) + x.shape, f32),
            dma((n_seq - 1,)),
            dma((n_seq - 1,)),
        ],
        compiler_params=pltpu.CompilerParams(collective_id=1, has_side_effects=True),
        name="sum_over_seq",
    )(x)


def adamw(param, grad, first, second_moment, rate, decay):
    first_new = beta_one * first + (1.0 - beta_one) * grad
    second_new = beta_two * second_moment + (1.0 - beta_two) * grad * grad
    corrected = (
        first_new
        / (1.0 - beta_one**adam_step)
        / (jnp.sqrt(second_new / (1.0 - beta_two**adam_step)) + adam_eps)
    )
    return (param - rate * (corrected + decay * param), first_new, second_new)


def shift(x, j, n_wsh):
    return lax.ppermute(x, "wshard", [(i, (i + j) % n_wsh) for i in range(n_wsh)])


def adam_kernel(count, g_ref, ext_ref, p_ref, m_ref, v_ref, grad_ref, *out_refs):
    at_ext = pl.program_id(0) == count
    grad = jnp.where(at_ext, ext_ref[...].astype(f32), g_ref[0].astype(f32))
    grad_ref[...] = grad
    news = adamw(
        p_ref[...], grad, m_ref[...], v_ref[...], weight_learning_rate, matrix_decay
    )
    for ref, new in zip(out_refs, news):
        ref[...] = new


def adam_in(g_main, g_ext, param, first, second):
    count, rows, cols = g_main.shape
    wide = pl.BlockSpec((rows, cols), lambda i: (0, i))
    return pl.pallas_call(
        functools.partial(adam_kernel, count),
        grid=(count + 1,),
        in_specs=[
            pl.BlockSpec((1, rows, cols), lambda i: (jnp.minimum(i, count - 1), 0, 0)),
            pl.BlockSpec((rows, cols), lambda i: (0, 0)),
            wide,
            wide,
            wide,
        ],
        out_specs=[wide] * 4,
        out_shape=[jax.ShapeDtypeStruct(param.shape, f32)] * 4,
        name="adam_in",
    )(g_main, g_ext, param, first, second)


def local(
    block_in,
    cotangent,
    in_weight,
    out_weight,
    in_gain,
    out_gain,
    conv_inner,
    conv_shared,
    head_params,
    first_in_weight,
    first_out_weight,
    first_in_gain,
    first_out_gain,
    first_conv_inner,
    first_conv_shared,
    first_head_params,
    second_in_weight,
    second_out_weight,
    second_in_gain,
    second_out_gain,
    second_conv_inner,
    second_conv_shared,
    second_head_params,
):
    seq_index = lax.axis_index("seq")
    wsh_index = lax.axis_index("wshard")
    n_seq = lax.axis_size("seq")
    n_wsh = lax.axis_size("wshard")
    rows_in, _ = in_weight.shape
    rows_out = out_weight.shape[0]
    _, width_in = block_in.shape[1:]
    heads = head_params.shape[1] // n_seq
    width = heads * P_SIZE
    inner_all = out_gain.shape[0]
    share = 2 * N_STATE // n_seq

    inputs = block_in[0].astype(f32)
    rms_in = lax.rsqrt(jnp.mean(inputs * inputs, axis=-1, keepdims=True) + norm_eps)
    normed = (inputs * rms_in * in_gain).astype(bf16)
    normed_all = lax.all_gather(normed, "seq", axis=0, tiled=True)
    cot = cotangent[0]
    cot_all = lax.all_gather(cot, "seq", axis=0, tiled=True)
    in_w16 = in_weight.astype(bf16)
    main_send = in_w16[:, : 2 * inner_all].reshape(rows_in, n_seq, 2 * width)
    main_send = jnp.swapaxes(main_send, 0, 1)
    small_send = in_w16[:, 2 * inner_all :]
    small_send = jnp.pad(small_send, ((0, 0), (0, -small_send.shape[1] % LANES)))
    w_main, w_small = spread_weights(main_send, small_send, n_seq, n_wsh)
    out_w16, w_main = lax.optimization_barrier((out_weight.astype(bf16), w_main))
    w_main = w_main.reshape(width_in, 2 * width)
    w_small = w_small.reshape(width_in, small_send.shape[1])
    w_out = jnp.zeros((n_wsh,) + out_w16.shape, bf16)
    w_out = lax.dynamic_update_index_in_dim(w_out, out_w16, wsh_index, 0)
    for j in range(1, n_wsh):
        got = shift(out_w16, j, n_wsh)
        w_out = lax.dynamic_update_index_in_dim(
            w_out, got, lax.rem(wsh_index - j + n_wsh, n_wsh), 0
        )
    w_out = w_out.reshape(width, width_in)

    def pick(first, count, width_to):
        col = lax.broadcasted_iota(jnp.int32, (w_small.shape[1], width_to), 0)
        lane = lax.broadcasted_iota(jnp.int32, (w_small.shape[1], width_to), 1)
        return jnp.where((col == lane + first) & (lane < count), 1.0, 0.0)

    first_step = 2 * N_STATE + seq_index * heads
    to_step = pick(first_step, heads, LANES)
    to_fwd = jnp.concatenate([pick(0, 2 * N_STATE, 2 * N_STATE), to_step], axis=1)
    to_ext = jnp.concatenate(
        [pick(seq_index * share, share, share), to_step[:, :STEP_ROWS]], axis=1
    )
    w_fwd = mm(w_small, to_fwd.astype(bf16), NN).astype(bf16)
    w_ext = mm(w_small, to_ext.astype(bf16), NN).astype(bf16)

    main = mm(normed_all, w_main, NN).astype(bf16)
    small = mm(normed_all, w_fwd, NN).astype(bf16)
    head_local = lax.dynamic_slice_in_dim(head_params, seq_index * heads, heads, 1)
    head = jnp.pad(head_local, ((0, 5), (0, LANES - heads)))
    conv_local = lax.dynamic_slice_in_dim(conv_inner, seq_index * width, width, 1)
    taps = jnp.pad(jnp.concatenate([conv_shared, conv_local], axis=1), ((0, 3), (0, 0)))
    gain_local = lax.dynamic_slice_in_dim(out_gain, seq_index * width, width, 0)
    gated, y, states = mixer_forward(main, small, head, taps, heads)
    d_gnormed = mm(cot_all, w_out, NT)
    gated32 = gated.astype(f32)
    scaled = d_gnormed * gain_local
    stats = jnp.stack(
        [jnp.sum(gated32 * gated32, axis=-1), jnp.sum(scaled * gated32, axis=-1)]
    )
    stats = sum_over_seq(stats.reshape(-1, LANES), n_seq).reshape(stats.shape)
    rms_out = lax.rsqrt(stats[0] / inner_all + norm_eps)[:, None]
    mean_sg = (stats[1] / inner_all)[:, None]
    gnormed = (gated32 * rms_out * gain_local).astype(bf16)
    d_gated = (rms_out * scaled - gated32 * rms_out**3 * mean_sg).astype(bf16)
    d_out_gain = jnp.sum(d_gnormed * gated32 * rms_out, axis=0)

    g_out = mm(gnormed, cot_all, TN)
    mixed = mm(gnormed, w_out, NN).astype(bf16)
    g_out, mixed, d_gated = lax.optimization_barrier((g_out, mixed, d_gated))
    mixed = lax.psum_scatter(mixed, "seq", scatter_dimension=0, tiled=True)
    grad_out_weight = lax.dynamic_slice_in_dim(g_out, wsh_index * rows_out, rows_out, 0)
    for j in range(1, n_wsh):
        to = lax.rem(wsh_index + j, n_wsh)
        part = lax.dynamic_slice_in_dim(g_out, to * rows_out, rows_out, 0)
        grad_out_weight = grad_out_weight + shift(part, j, n_wsh)
    dmain, dshared_t, dstep_t, dtaps, dhead = mixer_backward(
        main, small, head, taps, y, states, d_gated, heads
    )

    g_main = mm(normed_all, dmain, TN)
    d_gain_part = jnp.sum(g_main * w_main.astype(f32), axis=1)
    g_main = g_main.astype(bf16).reshape(n_seq, n_wsh, rows_in, 2 * width)
    g_parts = [lax.dynamic_index_in_dim(g_main, wsh_index, 1, keepdims=False)]
    for j in range(1, n_wsh):
        to = lax.rem(wsh_index + j, n_wsh)
        part = lax.dynamic_index_in_dim(g_main, to, 1, keepdims=False)
        g_parts.append(shift(part, j, n_wsh))

    (shared_parts,) = swap(
        (dshared_t.reshape(n_seq, share, -1),), ((0, "seq"),), n_seq, n_wsh, 2
    )
    shared_sum = jnp.sum(shared_parts.astype(f32), axis=0).astype(bf16)
    d_ext = jnp.concatenate([shared_sum, dstep_t], axis=0)
    d_normed = mm(dmain, w_main, NT) + lax.dot_general(
        d_ext, w_ext, (((0,), (1,)), ((), ())), preferred_element_type=f32
    )
    d_normed, mixed = lax.optimization_barrier((d_normed.astype(bf16), mixed))
    block_out = (inputs + mixed.astype(f32))[None]
    d_normed = lax.psum_scatter(d_normed, "seq", scatter_dimension=0, tiled=True)
    d_normed = d_normed.astype(f32)
    scaled_in = d_normed * in_gain
    grad_in = (
        cot.astype(f32)
        + rms_in * scaled_in
        - inputs * rms_in**3 * jnp.mean(scaled_in * inputs, axis=-1, keepdims=True)
    )[None]

    g_ext = lax.dot_general(
        normed_all, d_ext, (((0,), (1,)), ((), ())), preferred_element_type=f32
    )
    d_gain_part = d_gain_part + jnp.sum(g_ext * w_ext.astype(f32), axis=1)
    g_ext = jnp.pad(g_ext.astype(bf16), ((0, 0), (0, -g_ext.shape[1] % LANES)))
    g_ext = g_ext.reshape(n_seq, n_wsh, rows_in, LANES)

    d_skip = dtaps[5, 2 * N_STATE :].reshape(heads, P_SIZE).sum(-1)
    d_head = jnp.concatenate([dhead[:2, :heads], d_skip[None]], axis=0)
    pieces = (
        d_gain_part,
        dtaps[:5, : 2 * N_STATE],
        d_out_gain,
        dtaps[:5, 2 * N_STATE :],
        d_head,
    )
    flat = jnp.concatenate([p.reshape(-1) for p in pieces])
    flat = jnp.pad(flat, (0, -flat.shape[0] % (8 * LANES))).reshape(-1, LANES)
    g_ext, flat = swap(
        (g_ext, flat), ((1, "wshard"), ("all", "wshard")), n_seq, n_wsh, 3
    )
    g_ext = jnp.sum(g_ext.astype(f32), axis=0)
    (flat,) = swap((jnp.sum(flat, axis=0),), (("all", "seq"),), n_seq, n_wsh, 4)
    flat = flat.reshape(n_seq, -1)
    sums, at = [], 0
    for p in pieces:
        sums.append(flat[:, at : at + p.size].reshape((n_seq,) + p.shape))
        at += p.size
    grad_in_gain = jnp.sum(sums[0], axis=0) / in_gain
    grad_conv_shared = jnp.sum(sums[1], axis=0)
    grad_out_gain = sums[2].reshape(-1)
    grad_conv_inner = jnp.swapaxes(sums[3], 0, 1).reshape(conv_inner.shape)
    grad_head_params = jnp.swapaxes(sums[4], 0, 1).reshape(head_params.shape)

    g_main = g_parts[0].astype(f32)
    for part in g_parts[1:]:
        g_main = g_main + part.astype(f32)
    g_main, g_ext = swap(
        (g_main.astype(bf16), g_ext.astype(bf16)),
        ((0, "seq"), (0, "seq")),
        n_seq,
        n_wsh,
        5,
    )
    g_ext = jnp.swapaxes(g_ext, 0, 1)
    g_ext = jnp.concatenate(
        [
            g_ext[:, :, :share].reshape(rows_in, 2 * N_STATE),
            g_ext[:, :, share : share + heads].reshape(rows_in, heads * n_seq),
        ],
        axis=1,
    )
    g_ext = jnp.pad(g_ext, ((0, 0), (0, 2 * width - g_ext.shape[1])))
    grad_in_weight, new_in_weight, new_first_in_weight, new_second_in_weight = adam_in(
        g_main, g_ext, in_weight, first_in_weight, second_in_weight
    )
    new_out_weight, new_first_out_weight, new_second_out_weight = adamw(
        out_weight,
        grad_out_weight,
        first_out_weight,
        second_out_weight,
        weight_learning_rate,
        matrix_decay,
    )
    updated_input_gain, new_first_in_gain, new_second_in_gain = adamw(
        in_gain, grad_in_gain, first_in_gain, second_in_gain, small_rate, 0.0
    )
    new_out_gain, new_first_out_gain, new_second_out_gain = adamw(
        out_gain, grad_out_gain, first_out_gain, second_out_gain, small_rate, 0.0
    )
    new_conv_inner, new_first_conv_inner, new_second_conv_inner = adamw(
        conv_inner, grad_conv_inner, first_conv_inner, second_conv_inner, small_rate, 0.0
    )
    new_conv_shared, new_first_conv_shared, new_second_conv_shared = adamw(
        conv_shared, grad_conv_shared, first_conv_shared, second_conv_shared, small_rate, 0.0
    )
    new_head_params, updated_head_first_moment, head_second_all = adamw(
        head_params, grad_head_params, first_head_params, second_head_params, small_rate, 0.0
    )
    return (
        block_out,
        grad_in,
        grad_in_weight,
        grad_out_weight,
        grad_in_gain,
        grad_out_gain,
        grad_conv_inner,
        grad_conv_shared,
        grad_head_params,
        new_in_weight,
        new_out_weight,
        updated_input_gain,
        new_out_gain,
        new_conv_inner,
        new_conv_shared,
        new_head_params,
        new_first_in_weight,
        new_first_out_weight,
        new_first_in_gain,
        new_first_out_gain,
        new_first_conv_inner,
        new_first_conv_shared,
        updated_head_first_moment,
        new_second_in_weight,
        new_second_out_weight,
        new_second_in_gain,
        new_second_out_gain,
        new_second_conv_inner,
        new_second_conv_shared,
        head_second_all[0:2],
        head_second_all[2],
    )


def solution(mesh):
    return jax.shard_map(
        local,
        mesh=mesh,
        in_specs=(
            P("wshard", "seq", None),
            P("wshard", "seq", None),
            P(("seq", "wshard"), None),
            P(("seq", "wshard"), None),
            P(),
            P(),
            P(),
            P(),
            P(),
            P(("seq", "wshard"), None),
            P(("seq", "wshard"), None),
            P(),
            P(),
            P(),
            P(),
            P(),
            P(("seq", "wshard"), None),
            P(("seq", "wshard"), None),
            P(),
            P(),
            P(),
            P(),
            P(),
        ),
        out_specs=(
            P("wshard", "seq", None),
            P("wshard", "seq", None),
            P(("seq", "wshard"), None),
            P(("seq", "wshard"), None),
            P(),
            P(),
            P(),
            P(),
            P(),
            P(("seq", "wshard"), None),
            P(("seq", "wshard"), None),
            P(),
            P(),
            P(),
            P(),
            P(),
            P(("seq", "wshard"), None),
            P(("seq", "wshard"), None),
            P(),
            P(),
            P(),
            P(),
            P(),
            P(("seq", "wshard"), None),
            P(("seq", "wshard"), None),
            P(),
            P(),
            P(),
            P(),
            P(),
            P(),
        ),
        check_vma=False,
    )
```

```python
import functools

import jax
import jax.numpy as jnp
from jax import lax
from jax.experimental import pallas as pl
from jax.experimental.pallas import tpu as pltpu
from jax.sharding import PartitionSpec as P


P_SIZE = 64
N_STATE = 128
LANES = 128
CHUNK = 128
STEP_ROWS = 16

norm_eps = 1e-05
beta_one = 0.9
beta_two = 0.95
adam_eps = 1e-08
adam_step = 3.0
weight_learning_rate = 0.01
matrix_decay = 0.1
small_rate = 0.1


f32 = jnp.float32
bf16 = jnp.bfloat16
NN = (((1,), (0,)), ((), ()))
NT = (((1,), (1,)), ((), ()))
TN = (((0,), (0,)), ((), ()))


def mm(a, b, dims):
    return lax.dot_general(a, b, dims, preferred_element_type=f32)


def mm_high(a, b):
    return lax.dot_general(
        a, b, NN, precision=lax.Precision.HIGHEST, preferred_element_type=f32
    )


def two_parts(a):
    hi = a.astype(bf16)
    return hi, (a - hi.astype(f32)).astype(bf16)


def mm3(a, b, dims):
    return mm(a[0], b[0], dims) + (mm(a[0], b[1], dims) + mm(a[1], b[0], dims))


def low_half(rows):
    return lax.broadcasted_iota(jnp.int32, (rows, LANES), 1) < P_SIZE


def split_pairs(values, heads):
    low = low_half(values.shape[0])
    gates, inners = [], []
    for h in range(0, heads, 2):
        a = values[:, h * LANES : (h + 1) * LANES]
        a_r = pltpu.roll(a, P_SIZE, 1)
        if h + 1 < heads:
            b = values[:, (h + 1) * LANES : (h + 2) * LANES]
            b_r = pltpu.roll(b, P_SIZE, 1)
            gates.append(jnp.where(low, a, b_r))
            inners.append(jnp.where(low, a_r, b))
        else:
            gates.append(a[:, :P_SIZE])
            inners.append(a_r[:, :P_SIZE])
    return jnp.concatenate(gates, axis=1), jnp.concatenate(inners, axis=1)


def join_pairs(gate, inner, heads):
    low = low_half(gate.shape[0])
    out = []
    for h in range(0, heads, 2):
        if h + 1 < heads:
            g = gate[:, h * P_SIZE : (h + 2) * P_SIZE]
            x = inner[:, h * P_SIZE : (h + 2) * P_SIZE]
            out.append(jnp.where(low, g, pltpu.roll(x, P_SIZE, 1)))
            out.append(jnp.where(low, pltpu.roll(g, P_SIZE, 1), x))
        else:
            out.append(
                jnp.concatenate(
                    [gate[:, h * P_SIZE :], inner[:, h * P_SIZE :]], axis=1
                )
            )
    return jnp.concatenate(out, axis=1)


def expand(cols, heads, offset=0):
    rows = cols.shape[0]
    cols = cols[:, offset : offset + heads]
    low = low_half(rows)
    out = []
    for h in range(0, heads, 2):
        if h + 1 < heads:
            one = jnp.broadcast_to(cols[:, h : h + 1], (rows, LANES))
            two = jnp.broadcast_to(cols[:, h + 1 : h + 2], (rows, LANES))
            out.append(jnp.where(low, one, two))
        else:
            out.append(jnp.broadcast_to(cols[:, h : h + 1], (rows, P_SIZE)))
    return jnp.concatenate(out, axis=1)


def pair_of(values, h, heads):
    first = h - h % 2
    return values[:, first * P_SIZE : min(first + 2, heads) * P_SIZE]


def merge_pairs(parts, heads):
    low = low_half(parts[0].shape[0])
    out = []
    for h in range(0, heads, 2):
        if h + 1 < heads:
            out.append(jnp.where(low, parts[h], parts[h + 1]))
        else:
            out.append(parts[h])
    return jnp.concatenate(out, axis=1)


def chunk_common(heads, main, small, cat, head_ref, taps_ref):
    rows = main.shape[0]
    gate, inner = split_pairs(main, heads)
    raw = jnp.concatenate([small[:, : 2 * N_STATE], inner], axis=1)
    cat[8 : 8 + rows] = raw
    conv = taps_ref[4:5] + taps_ref[0:1] * cat[5 : 5 + rows]
    for k in range(1, 4):
        conv = conv + taps_ref[k : k + 1] * cat[5 + k : 5 + k + rows]
    step_in = small[:, 2 * N_STATE :] + head_ref[0:1]
    dt = jnp.maximum(step_in, 0.0) + jnp.log1p(jnp.exp(-jnp.abs(step_in)))
    neg_rate = -jnp.exp(head_ref[1:2])
    decay_log = neg_rate * dt
    r = lax.broadcasted_iota(jnp.int32, (rows, rows), 0)
    c = lax.broadcasted_iota(jnp.int32, (rows, rows), 1)
    tri = jnp.where(r >= c, 1.0, 0.0).astype(f32)
    cumul = mm_high(tri, decay_log)
    return gate, conv, step_in, dt, neg_rate, decay_log, cumul, r, c


def fwd_kernel(
    heads, main_ref, small_ref, head_ref, taps_ref, gated_ref, y_ref, states_ref, state, cat
):
    rows = main_ref.shape[0]

    @pl.when(pl.program_id(0) == 0)
    def _():
        state[...] = jnp.zeros_like(state)
        cat[0:8] = jnp.zeros((8, cat.shape[1]), f32)

    gate, conv, _, dt, _, _, cumul, r, c = chunk_common(
        heads,
        main_ref[...].astype(f32),
        small_ref[...].astype(f32),
        cat,
        head_ref,
        taps_ref,
    )
    cat[0:8] = cat[rows : rows + 8]
    act = conv * jax.nn.sigmoid(conv)
    b2 = two_parts(act[:, :N_STATE])
    c2 = two_parts(act[:, N_STATE : 2 * N_STATE])
    inner = act[:, 2 * N_STATE :]
    scaled = inner * expand(dt, heads)
    scaled2 = two_parts(scaled)
    scores = mm3(c2, b2, NT)
    lower = r >= c
    cumul_t = cumul.T
    parts = []
    for h in range(heads):
        spread = cumul[:, h : h + 1] - cumul_t[h : h + 1, :]
        weights = two_parts(scores * jnp.exp(jnp.where(lower, spread, -1e30)))
        own = tuple(pair_of(part, h, heads) for part in scaled2)
        parts.append(mm3(weights, own, NN))
    s2 = two_parts(state[...])
    states_ref[0] = state[...]
    last = cumul[rows - 1 : rows]
    y = merge_pairs(parts, heads) + expand(jnp.exp(cumul), heads) * mm3(c2, s2, NN)
    y_ref[...] = y
    tail = expand(jnp.exp(last - cumul), heads)
    fresh = mm3(b2, two_parts(tail * scaled), TN)
    state[...] = expand(jnp.exp(last), heads) * state[...] + fresh
    full = y + expand(head_ref[2:3], heads) * inner
    gated_ref[...] = (full * (gate * jax.nn.sigmoid(gate))).astype(bf16)


def mixer_forward(main, small, head, taps, heads):
    length = main.shape[0]
    width = heads * P_SIZE
    count = length // CHUNK
    all_w = width + 2 * N_STATE
    return pl.pallas_call(
        functools.partial(fwd_kernel, heads),
        grid=(count,),
        in_specs=[
            pl.BlockSpec((CHUNK, 2 * width), lambda i: (i, 0)),
            pl.BlockSpec((CHUNK, 3 * LANES), lambda i: (i, 0)),
            pl.BlockSpec((8, LANES), lambda i: (0, 0)),
            pl.BlockSpec((8, all_w), lambda i: (0, 0)),
        ],
        out_specs=[
            pl.BlockSpec((CHUNK, width), lambda i: (i, 0)),
            pl.BlockSpec((CHUNK, width), lambda i: (i, 0)),
            pl.BlockSpec((1, N_STATE, width), lambda i: (i, 0, 0)),
        ],
        out_shape=[
            jax.ShapeDtypeStruct((length, width), bf16),
            jax.ShapeDtypeStruct((length, width), f32),
            jax.ShapeDtypeStruct((count, N_STATE, width), f32),
        ],
        scratch_shapes=[
            pltpu.VMEM((N_STATE, width), f32),
            pltpu.VMEM((CHUNK + 8, all_w), f32),
        ],
        cost_estimate=pl.CostEstimate(
            flops=0, bytes_accessed=70_000_000, transcendentals=0
        ),
        name="mixer_forward",
    )(main, small, head, taps)


def bwd_kernel(heads, offset, count, has_before, is_last, *refs):
    refs = list(refs)
    main_ref, small_ref, main_prev, small_prev, head_ref, taps_ref = refs[:6]
    y_ref, states_ref, dgated_ref = refs[6:9]
    refs = refs[9:]
    if has_before:
        dmain_before, dbc_before = refs[:2]
        refs = refs[2:]
    dmain_ref, dstep_ref, dtaps_ref, dhead_ref = refs[:4]
    refs = refs[4:]
    if is_last:
        dshared_ref = refs.pop(0)
        if has_before:
            dall_ref = refs.pop(0)
    else:
        dbc_ref = refs.pop(0)
    dstate, cat, dcat = refs
    rows, width = y_ref.shape
    base = 2 * N_STATE if is_last else 0
    skip_cols = 2 * N_STATE - base
    step = pl.program_id(0)

    @pl.when(step == 0)
    def _():
        dstate[...] = jnp.zeros_like(dstate)
        dcat[rows : rows + 8] = jnp.zeros((8, dcat.shape[1]), f32)
        dtaps_ref[...] = jnp.zeros_like(dtaps_ref)
        dhead_ref[...] = jnp.zeros_like(dhead_ref)

    _, inner_prev = split_pairs(main_prev[8:16].astype(f32), heads)
    prev = jnp.concatenate(
        [small_prev[8:16].astype(f32)[:, : 2 * N_STATE], inner_prev], axis=1
    )
    cat[0:8] = jnp.where(step == count - 1, 0.0, prev)
    gate, conv, step_in, dt, neg_rate, decay_log, cumul, r, c = chunk_common(
        heads,
        main_ref[...].astype(f32),
        small_ref[...].astype(f32),
        cat,
        head_ref,
        taps_ref,
    )
    sig = jax.nn.sigmoid(conv)
    act = conv * sig
    conv_s = conv[:, skip_cols:]
    sig_s = sig[:, skip_cols:]
    dsilu = sig_s * (1.0 + conv_s * (1.0 - sig_s))
    b2 = two_parts(act[:, :N_STATE])
    c2 = two_parts(act[:, N_STATE : 2 * N_STATE])
    inner = act[:, 2 * N_STATE :]
    dt_x = expand(dt, heads, offset)
    scaled = inner * dt_x
    scaled2 = two_parts(scaled)
    skip = expand(head_ref[2:3], heads, offset)
    y = y_ref[...]
    sgate = jax.nn.sigmoid(gate)
    dgated = dgated_ref[...].astype(f32)
    dgate = dgated * (y + skip * inner) * (sgate * (1.0 + gate * (1.0 - sgate)))
    dy = dgated * (gate * sgate)
    dy2 = two_parts(dy)

    scores_t = mm3(b2, c2, NT)
    upper = c >= r
    cumul_t = cumul.T
    low = low_half(rows)
    parts = []
    dscores_t = None
    for h in range(heads):
        at = offset + h
        spread = cumul_t[at : at + 1, :] - cumul[:, at : at + 1]
        decay = jnp.exp(jnp.where(upper, spread, -1e30))
        weights = two_parts(scores_t * decay)
        dy_pair = tuple(pair_of(part, h, heads) for part in dy2)
        parts.append(mm3(weights, dy_pair, NN))
        own = pair_of(scaled, h, heads)
        if own.shape[1] == LANES:
            own = jnp.where(low == (h % 2 == 0), own, 0.0)
        term = mm3(two_parts(own), dy_pair, NT) * decay
        dscores_t = term if dscores_t is None else dscores_t + term
    s_in = states_ref[0]
    s2 = two_parts(s_in)
    ds = dstate[...]
    ds2 = two_parts(ds)
    last = cumul[rows - 1 : rows]
    tail = expand(jnp.exp(last - cumul), heads, offset)
    ecum = expand(jnp.exp(cumul), heads, offset)
    elast = expand(jnp.exp(last), heads, offset)
    tail_b = tail * mm3(b2, ds2, NN)
    z = merge_pairs(parts, heads) + tail_b
    extra = jnp.sum(tail_b * scaled, axis=0, keepdims=True) + elast * jnp.sum(
        ds * s_in, axis=0, keepdims=True
    )
    at_end = lax.broadcasted_iota(jnp.int32, (rows, width), 0) == rows - 1
    u = dy * y - scaled * z + jnp.where(at_end, extra, 0.0)
    pick = (
        lax.broadcasted_iota(jnp.int32, (width, LANES), 0) // P_SIZE + offset
        == lax.broadcasted_iota(jnp.int32, (width, LANES), 1)
    ).astype(f32)
    dcumul = mm_high(u, pick)
    suffix = jnp.where(c >= r, 1.0, 0.0).astype(f32)
    ddecay = mm_high(suffix, dcumul)
    dstep = (mm_high(inner * z, pick) + neg_rate * ddecay) * jax.nn.sigmoid(step_in)
    dstep_ref[...] = dstep.T[: dstep_ref.shape[0]].astype(bf16)
    dhead_ref[0:1] += jnp.sum(dstep, axis=0, keepdims=True)
    dhead_ref[1:2] += jnp.sum(decay_log * ddecay, axis=0, keepdims=True)

    dact = dt_x * z + skip * dy
    dscores2 = two_parts(dscores_t)
    edy2 = two_parts(ecum * dy)
    db = mm3(dscores2, c2, NN) + mm3(two_parts(tail * scaled), ds2, NT)
    dc = mm3(dscores2, b2, TN) + mm3(edy2, s2, NT)
    dstate[...] = elast * ds + mm3(c2, edy2, TN)
    dbc = jnp.concatenate([db, dc], axis=1)
    if has_before:
        dbc = dbc + dbc_before[...]
    if is_last:
        dact = jnp.concatenate([dbc, dact], axis=1)
    else:
        dbc_ref[...] = dbc

    dconv = dact * dsilu
    dcat[0:rows] = dconv
    draw = taps_ref[3:4, skip_cols:] * dconv
    for k in range(3):
        draw = draw + taps_ref[k : k + 1, skip_cols:] * dcat[3 - k : 3 - k + rows]
    for k in range(4):
        dtaps_ref[k : k + 1] += jnp.sum(
            dconv * cat[5 + k : 5 + k + rows, skip_cols:], axis=0, keepdims=True
        )
    dtaps_ref[4:5] += jnp.sum(dconv, axis=0, keepdims=True)
    dtaps_ref[5:6, base:] += jnp.sum(dy * inner, axis=0, keepdims=True)
    dcat[rows : rows + 8] = dconv[0:8]
    dmain = join_pairs(dgate, draw[:, base:], heads).astype(bf16)
    dmain_ref[...] = dmain
    if is_last:
        dshared_ref[...] = draw[:, : 2 * N_STATE].T.astype(bf16)
        if has_before:
            dall_ref[...] = jnp.concatenate([dmain_before[...], dmain], axis=1)


def mixer_backward(main, small, head, taps, y, states, dgated, heads, offset, before):
    length, all_width = y.shape
    all_heads = all_width // P_SIZE
    width = heads * P_SIZE
    is_last = offset + heads == all_heads
    has_before = before is not None
    place = offset * P_SIZE // width
    count = length // CHUNK
    cat_w = width + 2 * N_STATE
    dcat_w = cat_w if is_last else width
    per = CHUNK // 16

    def at(i):
        return (count - 1 - i, 0)

    def own(i):
        return (count - 1 - i, place)

    def turned(i):
        return (0, count - 1 - i)

    def ahead(col):
        return lambda i: (jnp.maximum((count - 1 - i) * per - 1, 0), col)

    def fixed(i):
        return (0, 0)

    taps = jnp.concatenate(
        [
            taps[:, : 2 * N_STATE],
            taps[:, 2 * N_STATE + offset * P_SIZE : 2 * N_STATE + offset * P_SIZE + width],
        ],
        axis=1,
    )
    args = [main, small, main, small, head, taps, y, states, dgated]
    in_specs = [
        pl.BlockSpec((CHUNK, 2 * width), own),
        pl.BlockSpec((CHUNK, 3 * LANES), at),
        pl.BlockSpec((16, 2 * width), ahead(place)),
        pl.BlockSpec((16, 3 * LANES), ahead(0)),
        pl.BlockSpec((8, LANES), fixed),
        pl.BlockSpec((8, cat_w), fixed),
        pl.BlockSpec((CHUNK, width), own),
        pl.BlockSpec((1, N_STATE, width), lambda i: (count - 1 - i, 0, place)),
        pl.BlockSpec((CHUNK, width), own),
    ]
    if has_before:
        args += list(before)
        in_specs += [
            pl.BlockSpec((CHUNK, before[0].shape[1]), at),
            pl.BlockSpec((CHUNK, 2 * N_STATE), at),
        ]
    outs = [
        (pl.BlockSpec((CHUNK, 2 * width), at), (length, 2 * width), bf16),
        (pl.BlockSpec((STEP_ROWS, CHUNK), turned), (STEP_ROWS, length), bf16),
        (pl.BlockSpec((8, dcat_w), fixed), (8, dcat_w), f32),
        (pl.BlockSpec((8, LANES), fixed), (8, LANES), f32),
    ]
    if is_last:
        outs.append(
            (pl.BlockSpec((2 * N_STATE, CHUNK), turned), (2 * N_STATE, length), bf16)
        )
        if has_before:
            outs.append(
                (pl.BlockSpec((CHUNK, 2 * all_width), at), (length, 2 * all_width), bf16)
            )
    else:
        outs.append((pl.BlockSpec((CHUNK, 2 * N_STATE), at), (length, 2 * N_STATE), f32))
    return pl.pallas_call(
        functools.partial(bwd_kernel, heads, offset, count, has_before, is_last),
        grid=(count,),
        in_specs=in_specs,
        out_specs=[spec for spec, _, _ in outs],
        out_shape=[jax.ShapeDtypeStruct(shape, dtype) for _, shape, dtype in outs],
        scratch_shapes=[
            pltpu.VMEM((N_STATE, width), f32),
            pltpu.VMEM((CHUNK + 8, cat_w), f32),
            pltpu.VMEM((CHUNK + 8, dcat_w), f32),
        ],
        cost_estimate=pl.CostEstimate(
            flops=0, bytes_accessed=30_000_000 * (heads + 1), transcendentals=0
        ),
        name="mixer_backward_last" if is_last else "mixer_backward_first",
    )(*args)


MESH = pl.DeviceIdType.MESH


def greet(peers, count):
    barrier = pltpu.get_barrier_semaphore()
    for peer in peers:
        pl.semaphore_signal(barrier, inc=1, device_id=peer, device_id_type=MESH)
    pl.semaphore_wait(barrier, count)


def wire(src, dst, send, recv, peer):
    return pltpu.make_async_remote_copy(
        src_ref=src,
        dst_ref=dst,
        send_sem=send,
        recv_sem=recv,
        device_id=peer,
        device_id_type=MESH,
    )


def weights_kernel(n_seq, n_wsh, main, small, w_main, w_small, *sems):
    send_a, recv_a, send_b, recv_b, send_e, recv_e, send_r, recv_r, send_l, recv_l, own = sems
    s = lax.axis_index("seq")
    w = lax.axis_index("wshard")
    row = [(lax.rem(s + k, n_seq), w) for k in range(1, n_seq)]
    col = [(s, lax.rem(w + j, n_wsh)) for j in range(1, n_wsh)]
    greet(row + col, n_seq + n_wsh - 2)
    first = [
        wire(main.at[peer[0]], w_main.at[s, w], send_a.at[k], recv_a.at[k], peer)
        for k, peer in enumerate(row)
    ]
    spread = [
        wire(small, w_small.at[s, w], send_b.at[j], recv_b.at[j], peer)
        for j, peer in enumerate(col)
    ]
    third = [
        wire(w_small.at[s], w_small.at[s], send_e.at[k], recv_e.at[k], peer)
        for k, peer in enumerate(row)
    ]
    mine = [
        pltpu.make_async_copy(main.at[s], w_main.at[s, w], own.at[0]),
        pltpu.make_async_copy(small, w_small.at[s, w], own.at[1]),
    ]

    def right(t):
        block = w_main.at[:, jnp.maximum(w - t, 0)]
        peer = (s, jnp.minimum(w + 1, n_wsh - 1))
        return wire(block, block, send_r.at[t], recv_r.at[t], peer)

    def left(t):
        block = w_main.at[:, jnp.minimum(w + t, n_wsh - 1)]
        peer = (s, jnp.maximum(w - 1, 0))
        return wire(block, block, send_l.at[t], recv_l.at[t], peer)

    for copy in mine + first + spread:
        copy.start()
    mine[0].wait()
    for copy in first:
        copy.wait_recv()
    last = n_wsh - 1
    for t in range(n_wsh):
        if t > 0:
            pl.when(w >= t)(lambda t=t: right(t - 1).wait_recv())
        if t < last:
            pl.when((w >= t) & (w < last))(lambda t=t: right(t).start())
        if t > 0:
            pl.when(w + t <= last)(lambda t=t: left(t - 1).wait_recv())
        if t < last:
            pl.when((w + t <= last) & (w > 0))(lambda t=t: left(t).start())
        if t == 0:
            mine[1].wait()
            for copy in spread:
                copy.wait_recv()
            for copy in third:
                copy.start()
    for copy in first + spread:
        copy.wait_send()
    for copy in third:
        copy.wait()
    for t in range(last):
        pl.when((w >= t) & (w < last))(lambda t=t: right(t).wait_send())
        pl.when((w + t <= last) & (w > 0))(lambda t=t: left(t).wait_send())


def spread_weights(main, small, n_seq, n_wsh):
    rows_in, cols = main.shape[1:]
    anywhere = pl.BlockSpec(memory_space=pl.ANY)
    dma = pltpu.SemaphoreType.DMA
    a, c = n_seq - 1, n_wsh - 1
    return pl.pallas_call(
        functools.partial(weights_kernel, n_seq, n_wsh),
        in_specs=[anywhere] * 2,
        out_specs=[anywhere] * 2,
        out_shape=[
            jax.ShapeDtypeStruct((n_seq, n_wsh, rows_in, cols), bf16),
            jax.ShapeDtypeStruct((n_seq, n_wsh) + small.shape, bf16),
        ],
        scratch_shapes=[dma((n,)) for n in (a, a, c, c, a, a, c, c, c, c, 2)],
        compiler_params=pltpu.CompilerParams(collective_id=0, has_side_effects=True),
        cost_estimate=pl.CostEstimate(
            flops=0, bytes_accessed=200_000_000, transcendentals=0
        ),
        name="spread_weights",
    )(main, small)


def swap_kernel(plan, n_seq, n_wsh, *refs):
    n = len(plan)
    ins, outs, sems = refs[:n], refs[n : 2 * n], refs[2 * n :]
    s = lax.axis_index("seq")
    w = lax.axis_index("wshard")
    total = n_seq * n_wsh
    me_all = s * n_wsh + w
    size = {"seq": n_seq, "wshard": n_wsh, "both": total}
    me_of = {"seq": s, "wshard": w, "both": me_all}

    def peer_at(axis, k):
        if axis == "seq":
            index = lax.rem(s + k, n_seq)
            return index, (index, w)
        if axis == "wshard":
            index = lax.rem(w + k, n_wsh)
            return index, (s, index)
        index = lax.rem(me_all + k, total)
        return index, (lax.div(index, n_wsh), lax.rem(index, n_wsh))

    def block(kind, ref, index):
        if kind == "all":
            return ref
        return ref.at[index] if kind == 0 else ref.at[:, index]

    def copy_of(i, k):
        kind, axis = plan[i]
        index, peer = peer_at(axis, k)
        return wire(
            block(kind, ins[i], index),
            outs[i].at[me_of[axis]],
            sems[3 * i].at[k],
            sems[3 * i + 1].at[k],
            peer,
        )

    widest = "both" if any(axis == "both" for _, axis in plan) else plan[0][1]
    barrier = pltpu.get_barrier_semaphore()

    def hail(k, _):
        pl.semaphore_signal(
            barrier, inc=1, device_id=peer_at(widest, k)[1], device_id_type=MESH
        )
        return 0

    lax.fori_loop(1, size[widest], hail, 0)
    pl.semaphore_wait(barrier, size[widest] - 1)
    own = []
    for i, (kind, axis) in enumerate(plan):
        me = me_of[axis]
        own.append(
            pltpu.make_async_copy(
                block(kind, ins[i], me), outs[i].at[me], sems[3 * i + 2].at[0]
            )
        )

        def begin(k, _, i=i):
            copy_of(i, k).start()
            return 0

        lax.fori_loop(1, size[axis], begin, 0)
    for copy in own:
        copy.start()
    for i, (kind, axis) in enumerate(plan):
        own[i].wait()

        def finish(k, _, i=i):
            copy_of(i, k).wait()
            return 0

        lax.fori_loop(1, size[axis], finish, 0)


def swap(arrays, plan, n_seq, n_wsh, collective_id):
    anywhere = pl.BlockSpec(memory_space=pl.ANY)
    size = {"seq": n_seq, "wshard": n_wsh, "both": n_seq * n_wsh}
    shapes, sems = [], []
    for x, (kind, axis) in zip(arrays, plan):
        n = size[axis]
        shape = x.shape
        if kind == 0:
            shape = shape[1:]
        elif kind == 1:
            shape = shape[:1] + shape[2:]
        shapes.append(jax.ShapeDtypeStruct((n,) + shape, x.dtype))
        sems += [
            pltpu.SemaphoreType.DMA((n,)),
            pltpu.SemaphoreType.DMA((n,)),
            pltpu.SemaphoreType.DMA((1,)),
        ]
    return pl.pallas_call(
        functools.partial(swap_kernel, plan, n_seq, n_wsh),
        in_specs=[anywhere] * len(arrays),
        out_specs=[anywhere] * len(arrays),
        out_shape=shapes,
        scratch_shapes=sems,
        compiler_params=pltpu.CompilerParams(
            collective_id=collective_id, has_side_effects=True
        ),
    )(*arrays)


def stats_kernel(n_seq, x_ref, out_ref, slots, send, recv):
    s = lax.axis_index("seq")
    w = lax.axis_index("wshard")
    row = [(lax.rem(s + k, n_seq), w) for k in range(1, n_seq)]
    greet(row, n_seq - 1)
    copies = [
        wire(x_ref, slots.at[s], send.at[k], recv.at[k], peer)
        for k, peer in enumerate(row)
    ]
    for copy in copies:
        copy.start()
    slots[s] = x_ref[...]
    for copy in copies:
        copy.wait()
    total = slots[0]
    for k in range(1, n_seq):
        total = total + slots[k]
    out_ref[...] = total


def sum_over_seq(x, n_seq):
    vmem = pl.BlockSpec(memory_space=pltpu.VMEM)
    dma = pltpu.SemaphoreType.DMA
    return pl.pallas_call(
        functools.partial(stats_kernel, n_seq),
        in_specs=[vmem],
        out_specs=vmem,
        out_shape=jax.ShapeDtypeStruct(x.shape, f32),
        scratch_shapes=[
            pltpu.VMEM((n_seq,) + x.shape, f32),
            dma((n_seq - 1,)),
            dma((n_seq - 1,)),
        ],
        compiler_params=pltpu.CompilerParams(collective_id=1, has_side_effects=True),
        name="sum_over_seq",
    )(x)


def adamw(param, grad, first, second_moment, rate, decay):
    first_new = beta_one * first + (1.0 - beta_one) * grad
    second_new = beta_two * second_moment + (1.0 - beta_two) * grad * grad
    corrected = (
        first_new
        / (1.0 - beta_one**adam_step)
        / (jnp.sqrt(second_new / (1.0 - beta_two**adam_step)) + adam_eps)
    )
    return (param - rate * (corrected + decay * param), first_new, second_new)


def shift(x, j, n_wsh):
    return lax.ppermute(x, "wshard", [(i, (i + j) % n_wsh) for i in range(n_wsh)])


def two_groups(heads):
    return heads % 2 == 0 and heads >= 4 and (heads - 2) % 2 == 0


def adam_kernel(count, groups, *refs):
    g_refs, (ext_ref, p_ref, m_ref, v_ref, grad_ref, *out_refs) = refs[:groups], refs[groups:]
    at_ext = pl.program_id(0) == count
    own = jnp.concatenate([ref[0] for ref in g_refs], axis=1)
    grad = jnp.where(at_ext, ext_ref[...].astype(f32), own.astype(f32))
    grad_ref[...] = grad
    news = adamw(
        p_ref[...], grad, m_ref[...], v_ref[...], weight_learning_rate, matrix_decay
    )
    for ref, new in zip(out_refs, news):
        ref[...] = new


def adam_in(g_main, g_ext, param, first, second):
    count, rows = g_main[0].shape[:2]
    cols = g_ext.shape[1]
    wide = pl.BlockSpec((rows, cols), lambda i: (0, i))
    return pl.pallas_call(
        functools.partial(adam_kernel, count, len(g_main)),
        grid=(count + 1,),
        in_specs=[
            *(
                pl.BlockSpec((1,) + g.shape[1:], lambda i: (jnp.minimum(i, count - 1), 0, 0))
                for g in g_main
            ),
            pl.BlockSpec((rows, cols), lambda i: (0, 0)),
            wide,
            wide,
            wide,
        ],
        out_specs=[wide] * 4,
        out_shape=[jax.ShapeDtypeStruct(param.shape, f32)] * 4,
        name="adam_in",
    )(*g_main, g_ext, param, first, second)


def local(
    block_in,
    cotangent,
    in_weight,
    out_weight,
    in_gain,
    out_gain,
    conv_inner,
    conv_shared,
    head_params,
    first_in_weight,
    first_out_weight,
    first_in_gain,
    first_out_gain,
    first_conv_inner,
    first_conv_shared,
    first_head_params,
    second_in_weight,
    second_out_weight,
    second_in_gain,
    second_out_gain,
    second_conv_inner,
    second_conv_shared,
    second_head_params,
):
    seq_index = lax.axis_index("seq")
    wsh_index = lax.axis_index("wshard")
    n_seq = lax.axis_size("seq")
    n_wsh = lax.axis_size("wshard")
    rows_in, _ = in_weight.shape
    rows_out = out_weight.shape[0]
    _, width_in = block_in.shape[1:]
    heads = head_params.shape[1] // n_seq
    width = heads * P_SIZE
    inner_all = out_gain.shape[0]
    share = 2 * N_STATE // n_seq

    inputs = block_in[0].astype(f32)
    rms_in = lax.rsqrt(jnp.mean(inputs * inputs, axis=-1, keepdims=True) + norm_eps)
    normed = (inputs * rms_in * in_gain).astype(bf16)
    normed_all = lax.all_gather(normed, "seq", axis=0, tiled=True)
    cot = cotangent[0]
    cot_all = lax.all_gather(cot, "seq", axis=0, tiled=True)
    in_w16 = in_weight.astype(bf16)
    main_send = in_w16[:, : 2 * inner_all].reshape(rows_in, n_seq, 2 * width)
    main_send = jnp.swapaxes(main_send, 0, 1)
    small_send = in_w16[:, 2 * inner_all :]
    small_send = jnp.pad(small_send, ((0, 0), (0, -small_send.shape[1] % LANES)))
    w_main, w_small = spread_weights(main_send, small_send, n_seq, n_wsh)
    out_w16, w_main = lax.optimization_barrier((out_weight.astype(bf16), w_main))
    w_main = w_main.reshape(width_in, 2 * width)
    w_small = w_small.reshape(width_in, small_send.shape[1])
    w_out = jnp.zeros((n_wsh,) + out_w16.shape, bf16)
    w_out = lax.dynamic_update_index_in_dim(w_out, out_w16, wsh_index, 0)
    for j in range(1, n_wsh):
        got = shift(out_w16, j, n_wsh)
        w_out = lax.dynamic_update_index_in_dim(
            w_out, got, lax.rem(wsh_index - j + n_wsh, n_wsh), 0
        )
    w_out = w_out.reshape(width, width_in)

    def pick(first, count, width_to):
        col = lax.broadcasted_iota(jnp.int32, (w_small.shape[1], width_to), 0)
        lane = lax.broadcasted_iota(jnp.int32, (w_small.shape[1], width_to), 1)
        return jnp.where((col == lane + first) & (lane < count), 1.0, 0.0)

    first_step = 2 * N_STATE + seq_index * heads
    to_step = pick(first_step, heads, LANES)
    to_fwd = jnp.concatenate([pick(0, 2 * N_STATE, 2 * N_STATE), to_step], axis=1)
    to_ext = jnp.concatenate(
        [pick(seq_index * share, share, share), to_step[:, :STEP_ROWS]], axis=1
    )
    w_fwd = mm(w_small, to_fwd.astype(bf16), NN).astype(bf16)
    w_ext = mm(w_small, to_ext.astype(bf16), NN).astype(bf16)

    main = mm(normed_all, w_main, NN).astype(bf16)
    small = mm(normed_all, w_fwd, NN).astype(bf16)
    head_local = lax.dynamic_slice_in_dim(head_params, seq_index * heads, heads, 1)
    head = jnp.pad(head_local, ((0, 5), (0, LANES - heads)))
    conv_local = lax.dynamic_slice_in_dim(conv_inner, seq_index * width, width, 1)
    taps = jnp.pad(jnp.concatenate([conv_shared, conv_local], axis=1), ((0, 3), (0, 0)))
    gain_local = lax.dynamic_slice_in_dim(out_gain, seq_index * width, width, 0)
    gated, y, states = mixer_forward(main, small, head, taps, heads)
    d_gnormed = mm(cot_all, w_out, NT)
    gated32 = gated.astype(f32)
    scaled = d_gnormed * gain_local
    stats = jnp.stack(
        [jnp.sum(gated32 * gated32, axis=-1), jnp.sum(scaled * gated32, axis=-1)]
    )
    stats = sum_over_seq(stats.reshape(-1, LANES), n_seq).reshape(stats.shape)
    rms_out = lax.rsqrt(stats[0] / inner_all + norm_eps)[:, None]
    mean_sg = (stats[1] / inner_all)[:, None]
    gnormed = (gated32 * rms_out * gain_local).astype(bf16)
    d_gated = (rms_out * scaled - gated32 * rms_out**3 * mean_sg).astype(bf16)
    d_out_gain = jnp.sum(d_gnormed * gated32 * rms_out, axis=0)

    g_out = mm(gnormed, cot_all, TN)
    mixed = mm(gnormed, w_out, NN).astype(bf16)
    g_out, mixed, d_gated = lax.optimization_barrier((g_out, mixed, d_gated))
    mixed = lax.psum_scatter(mixed, "seq", scatter_dimension=0, tiled=True)
    out_parts = [lax.dynamic_slice_in_dim(g_out, wsh_index * rows_out, rows_out, 0)]
    for j in range(1, n_wsh):
        to = lax.rem(wsh_index + j, n_wsh)
        part = lax.dynamic_slice_in_dim(g_out, to * rows_out, rows_out, 0)
        out_parts.append(shift(part, j, n_wsh))

    def send_grad(d_part):
        grad = mm(normed_all, d_part, TN)
        blocks = grad.astype(bf16).reshape(n_seq, n_wsh, rows_in, grad.shape[1])
        got = [lax.dynamic_index_in_dim(blocks, wsh_index, 1, keepdims=False)]
        for j in range(1, n_wsh):
            to = lax.rem(wsh_index + j, n_wsh)
            part = lax.dynamic_index_in_dim(blocks, to, 1, keepdims=False)
            got.append(shift(part, j, n_wsh))
        return grad, got

    back_args = (main, small, head, taps, y, states, d_gated)
    if two_groups(heads):
        early = heads - 2
        d_first, step_a, taps_a, head_a, dbc = mixer_backward(*back_args, early, 0, None)
        grad_a, got_a = send_grad(d_first)
        d_last, step_b, taps_b, head_b, dshared_t, dmain = mixer_backward(
            *back_args, 2, early, (d_first, dbc)
        )
        dstep_t = step_a + step_b
        dhead = head_a + head_b
        dtaps = jnp.concatenate(
            [taps_b[:, : 2 * N_STATE], taps_a, taps_b[:, 2 * N_STATE :]], axis=1
        )
    else:
        d_last, dstep_t, dtaps, dhead, dshared_t = mixer_backward(
            *back_args, heads, 0, None
        )
        dmain = d_last

    (shared_parts,) = swap(
        (dshared_t.reshape(n_seq, share, -1),), ((0, "seq"),), n_seq, n_wsh, 2
    )
    shared_sum = jnp.sum(shared_parts.astype(f32), axis=0).astype(bf16)
    d_ext = jnp.concatenate([shared_sum, dstep_t], axis=0)
    d_normed = mm(dmain, w_main, NT) + lax.dot_general(
        d_ext, w_ext, (((0,), (1,)), ((), ())), preferred_element_type=f32
    )
    d_normed, mixed, d_last = lax.optimization_barrier(
        (d_normed.astype(bf16), mixed, d_last)
    )
    block_out = (inputs + mixed.astype(f32))[None]
    d_normed = lax.psum_scatter(d_normed, "seq", scatter_dimension=0, tiled=True)
    d_normed = d_normed.astype(f32)
    scaled_in = d_normed * in_gain
    grad_in = (
        cot.astype(f32)
        + rms_in * scaled_in
        - inputs * rms_in**3 * jnp.mean(scaled_in * inputs, axis=-1, keepdims=True)
    )[None]

    grad_b, got_b = send_grad(d_last)
    if two_groups(heads):
        grad_b, d_ext, out_parts, got_a = lax.optimization_barrier(
            (grad_b, d_ext, out_parts, got_a)
        )
    grad_out_weight = sum(out_parts)
    g_ext = lax.dot_general(
        normed_all, d_ext, (((0,), (1,)), ((), ())), preferred_element_type=f32
    )
    d_gain_part = jnp.sum(g_ext * w_ext.astype(f32), axis=1)
    if two_groups(heads):
        grads, got = [grad_a, grad_b], [got_a, got_b]
    else:
        grads, got = [grad_b], [got_b]
    first = 0
    for grad in grads:
        part = w_main[:, first : first + grad.shape[1]].astype(f32)
        d_gain_part = d_gain_part + jnp.sum(grad * part, axis=1)
        first += grad.shape[1]
    g_ext = jnp.pad(g_ext.astype(bf16), ((0, 0), (0, -g_ext.shape[1] % LANES)))
    g_ext = g_ext.reshape(n_seq, n_wsh, rows_in, LANES)

    d_skip = dtaps[5, 2 * N_STATE :].reshape(heads, P_SIZE).sum(-1)
    d_head = jnp.concatenate([dhead[:2, :heads], d_skip[None]], axis=0)
    pieces = (
        d_gain_part,
        dtaps[:5, : 2 * N_STATE],
        d_out_gain,
        dtaps[:5, 2 * N_STATE :],
        d_head,
    )
    flat = jnp.concatenate([p.reshape(-1) for p in pieces])
    flat = jnp.pad(flat, (0, -flat.shape[0] % (8 * LANES))).reshape(-1, LANES)
    g_ext, flat = swap(
        (g_ext, flat), ((1, "wshard"), ("all", "wshard")), n_seq, n_wsh, 3
    )
    g_ext = jnp.sum(g_ext.astype(f32), axis=0)
    (flat,) = swap((jnp.sum(flat, axis=0),), (("all", "seq"),), n_seq, n_wsh, 4)
    flat = flat.reshape(n_seq, -1)
    sums, at = [], 0
    for p in pieces:
        sums.append(flat[:, at : at + p.size].reshape((n_seq,) + p.shape))
        at += p.size
    grad_in_gain = jnp.sum(sums[0], axis=0) / in_gain
    grad_conv_shared = jnp.sum(sums[1], axis=0)
    grad_out_gain = sums[2].reshape(-1)
    grad_conv_inner = jnp.swapaxes(sums[3], 0, 1).reshape(conv_inner.shape)
    grad_head_params = jnp.swapaxes(sums[4], 0, 1).reshape(head_params.shape)

    sums = [sum(part.astype(f32) for part in parts).astype(bf16) for parts in got]
    *g_main, g_ext = swap(
        (*sums, g_ext.astype(bf16)), ((0, "seq"),) * (len(sums) + 1), n_seq, n_wsh, 5
    )
    g_ext = jnp.swapaxes(g_ext, 0, 1)
    g_ext = jnp.concatenate(
        [
            g_ext[:, :, :share].reshape(rows_in, 2 * N_STATE),
            g_ext[:, :, share : share + heads].reshape(rows_in, heads * n_seq),
        ],
        axis=1,
    )
    g_ext = jnp.pad(g_ext, ((0, 0), (0, 2 * width - g_ext.shape[1])))
    grad_in_weight, new_in_weight, new_first_in_weight, new_second_in_weight = adam_in(
        g_main, g_ext, in_weight, first_in_weight, second_in_weight
    )
    new_out_weight, new_first_out_weight, new_second_out_weight = adamw(
        out_weight,
        grad_out_weight,
        first_out_weight,
        second_out_weight,
        weight_learning_rate,
        matrix_decay,
    )
    updated_input_gain, new_first_in_gain, new_second_in_gain = adamw(
        in_gain, grad_in_gain, first_in_gain, second_in_gain, small_rate, 0.0
    )
    new_out_gain, new_first_out_gain, new_second_out_gain = adamw(
        out_gain, grad_out_gain, first_out_gain, second_out_gain, small_rate, 0.0
    )
    new_conv_inner, new_first_conv_inner, new_second_conv_inner = adamw(
        conv_inner, grad_conv_inner, first_conv_inner, second_conv_inner, small_rate, 0.0
    )
    new_conv_shared, new_first_conv_shared, new_second_conv_shared = adamw(
        conv_shared, grad_conv_shared, first_conv_shared, second_conv_shared, small_rate, 0.0
    )
    new_head_params, updated_head_first_moment, head_second_all = adamw(
        head_params, grad_head_params, first_head_params, second_head_params, small_rate, 0.0
    )
    return (
        block_out,
        grad_in,
        grad_in_weight,
        grad_out_weight,
        grad_in_gain,
        grad_out_gain,
        grad_conv_inner,
        grad_conv_shared,
        grad_head_params,
        new_in_weight,
        new_out_weight,
        updated_input_gain,
        new_out_gain,
        new_conv_inner,
        new_conv_shared,
        new_head_params,
        new_first_in_weight,
        new_first_out_weight,
        new_first_in_gain,
        new_first_out_gain,
        new_first_conv_inner,
        new_first_conv_shared,
        updated_head_first_moment,
        new_second_in_weight,
        new_second_out_weight,
        new_second_in_gain,
        new_second_out_gain,
        new_second_conv_inner,
        new_second_conv_shared,
        head_second_all[0:2],
        head_second_all[2],
    )


def solution(mesh):
    return jax.shard_map(
        local,
        mesh=mesh,
        in_specs=(
            P("wshard", "seq", None),
            P("wshard", "seq", None),
            P(("seq", "wshard"), None),
            P(("seq", "wshard"), None),
            P(),
            P(),
            P(),
            P(),
            P(),
            P(("seq", "wshard"), None),
            P(("seq", "wshard"), None),
            P(),
            P(),
            P(),
            P(),
            P(),
            P(("seq", "wshard"), None),
            P(("seq", "wshard"), None),
            P(),
            P(),
            P(),
            P(),
            P(),
        ),
        out_specs=(
            P("wshard", "seq", None),
            P("wshard", "seq", None),
            P(("seq", "wshard"), None),
            P(("seq", "wshard"), None),
            P(),
            P(),
            P(),
            P(),
            P(),
            P(("seq", "wshard"), None),
            P(("seq", "wshard"), None),
            P(),
            P(),
            P(),
            P(),
            P(),
            P(("seq", "wshard"), None),
            P(("seq", "wshard"), None),
            P(),
            P(),
            P(),
            P(),
            P(),
            P(("seq", "wshard"), None),
            P(("seq", "wshard"), None),
            P(),
            P(),
            P(),
            P(),
            P(),
            P(),
        ),
        check_vma=False,
    )
```

```python
import functools

import jax
import jax.numpy as jnp
from jax import lax
from jax.experimental import pallas as pl
from jax.experimental.pallas import tpu as pltpu
from jax.sharding import PartitionSpec as P


P_SIZE = 64
N_STATE = 128
LANES = 128
CHUNK = 128
STEP_ROWS = 16

norm_eps = 1e-05
beta_one = 0.9
beta_two = 0.95
adam_eps = 1e-08
adam_step = 3.0
weight_learning_rate = 0.01
matrix_decay = 0.1
small_rate = 0.1


f32 = jnp.float32
bf16 = jnp.bfloat16
NN = (((1,), (0,)), ((), ()))
NT = (((1,), (1,)), ((), ()))
TN = (((0,), (0,)), ((), ()))


def mm(a, b, dims):
    return lax.dot_general(a, b, dims, preferred_element_type=f32)


def mm_high(a, b):
    return lax.dot_general(
        a, b, NN, precision=lax.Precision.HIGHEST, preferred_element_type=f32
    )


def two_parts(a):
    hi = a.astype(bf16)
    return hi, (a - hi.astype(f32)).astype(bf16)


def mm3(a, b, dims):
    return mm(a[0], b[0], dims) + (mm(a[0], b[1], dims) + mm(a[1], b[0], dims))


def low_half(rows):
    return lax.broadcasted_iota(jnp.int32, (rows, LANES), 1) < P_SIZE


def split_pairs(values, heads):
    low = low_half(values.shape[0])
    gates, inners = [], []
    for h in range(0, heads, 2):
        a = values[:, h * LANES : (h + 1) * LANES]
        a_r = pltpu.roll(a, P_SIZE, 1)
        if h + 1 < heads:
            b = values[:, (h + 1) * LANES : (h + 2) * LANES]
            b_r = pltpu.roll(b, P_SIZE, 1)
            gates.append(jnp.where(low, a, b_r))
            inners.append(jnp.where(low, a_r, b))
        else:
            gates.append(a[:, :P_SIZE])
            inners.append(a_r[:, :P_SIZE])
    return jnp.concatenate(gates, axis=1), jnp.concatenate(inners, axis=1)


def join_pairs(gate, inner, heads):
    low = low_half(gate.shape[0])
    out = []
    for h in range(0, heads, 2):
        if h + 1 < heads:
            g = gate[:, h * P_SIZE : (h + 2) * P_SIZE]
            x = inner[:, h * P_SIZE : (h + 2) * P_SIZE]
            out.append(jnp.where(low, g, pltpu.roll(x, P_SIZE, 1)))
            out.append(jnp.where(low, pltpu.roll(g, P_SIZE, 1), x))
        else:
            out.append(
                jnp.concatenate(
                    [gate[:, h * P_SIZE :], inner[:, h * P_SIZE :]], axis=1
                )
            )
    return jnp.concatenate(out, axis=1)


def expand(cols, heads):
    rows = cols.shape[0]
    low = low_half(rows)
    out = []
    for h in range(0, heads, 2):
        if h + 1 < heads:
            one = jnp.broadcast_to(cols[:, h : h + 1], (rows, LANES))
            two = jnp.broadcast_to(cols[:, h + 1 : h + 2], (rows, LANES))
            out.append(jnp.where(low, one, two))
        else:
            out.append(jnp.broadcast_to(cols[:, h : h + 1], (rows, P_SIZE)))
    return jnp.concatenate(out, axis=1)


def pair_of(values, h, heads):
    first = h - h % 2
    return values[:, first * P_SIZE : min(first + 2, heads) * P_SIZE]


def merge_pairs(parts, heads):
    low = low_half(parts[0].shape[0])
    out = []
    for h in range(0, heads, 2):
        if h + 1 < heads:
            out.append(jnp.where(low, parts[h], parts[h + 1]))
        else:
            out.append(parts[h])
    return jnp.concatenate(out, axis=1)


def chunk_common(heads, main, small16, sel_ref, cat, head_ref, taps_ref):
    rows = main.shape[0]
    gate, inner = split_pairs(main, heads)
    raw = jnp.concatenate([small16[:, : 2 * N_STATE].astype(f32), inner], axis=1)
    cat[8 : 8 + rows] = raw
    conv = taps_ref[4:5] + taps_ref[0:1] * cat[5 : 5 + rows]
    for k in range(1, 4):
        conv = conv + taps_ref[k : k + 1] * cat[5 + k : 5 + k + rows]
    step_in = mm(small16[:, 2 * N_STATE :], sel_ref[...], NN) + head_ref[0:1]
    dt = jnp.maximum(step_in, 0.0) + jnp.log1p(jnp.exp(-jnp.abs(step_in)))
    neg_rate = -jnp.exp(head_ref[1:2])
    decay_log = neg_rate * dt
    r = lax.broadcasted_iota(jnp.int32, (rows, rows), 0)
    c = lax.broadcasted_iota(jnp.int32, (rows, rows), 1)
    tri = jnp.where(r >= c, 1.0, 0.0).astype(f32)
    cumul = mm_high(tri, decay_log)
    return gate, conv, step_in, dt, neg_rate, decay_log, cumul, r, c


def fwd_kernel(
    heads, main_ref, small_ref, sel_ref, head_ref, taps_ref, gated_ref, y_ref, states_ref, state, cat
):
    rows = main_ref.shape[0]

    @pl.when(pl.program_id(0) == 0)
    def _():
        state[...] = jnp.zeros_like(state)
        cat[0:8] = jnp.zeros((8, cat.shape[1]), f32)

    gate, conv, _, dt, _, _, cumul, r, c = chunk_common(
        heads,
        main_ref[...].astype(f32),
        small_ref[...],
        sel_ref,
        cat,
        head_ref,
        taps_ref,
    )
    cat[0:8] = cat[rows : rows + 8]
    act = conv * jax.nn.sigmoid(conv)
    b2 = two_parts(act[:, :N_STATE])
    c2 = two_parts(act[:, N_STATE : 2 * N_STATE])
    inner = act[:, 2 * N_STATE :]
    scaled = inner * expand(dt, heads)
    scaled2 = two_parts(scaled)
    scores = mm3(c2, b2, NT)
    lower = r >= c
    cumul_t = cumul.T
    parts = []
    for h in range(heads):
        spread = cumul[:, h : h + 1] - cumul_t[h : h + 1, :]
        weights = two_parts(scores * jnp.exp(jnp.where(lower, spread, -1e30)))
        own = tuple(pair_of(part, h, heads) for part in scaled2)
        parts.append(mm3(weights, own, NN))
    s2 = two_parts(state[...])
    states_ref[0] = state[...]
    last = cumul[rows - 1 : rows]
    y = merge_pairs(parts, heads) + expand(jnp.exp(cumul), heads) * mm3(c2, s2, NN)
    y_ref[...] = y
    tail = expand(jnp.exp(last - cumul), heads)
    fresh = mm3(b2, two_parts(tail * scaled), TN)
    state[...] = expand(jnp.exp(last), heads) * state[...] + fresh
    full = y + expand(head_ref[2:3], heads) * inner
    gated_ref[...] = (full * (gate * jax.nn.sigmoid(gate))).astype(bf16)


def mixer_forward(proj, sel, head, taps, heads):
    length = proj.shape[0]
    width = heads * P_SIZE
    count = length // CHUNK
    all_w = width + 2 * N_STATE
    return pl.pallas_call(
        functools.partial(fwd_kernel, heads),
        grid=(count,),
        in_specs=[
            pl.BlockSpec((CHUNK, 2 * width), lambda i: (i, 0)),
            pl.BlockSpec((CHUNK, 3 * LANES), lambda i: (i, 2 * width // (3 * LANES))),
            pl.BlockSpec((LANES, LANES), lambda i: (0, 0)),
            pl.BlockSpec((8, LANES), lambda i: (0, 0)),
            pl.BlockSpec((8, all_w), lambda i: (0, 0)),
        ],
        out_specs=[
            pl.BlockSpec((CHUNK, width), lambda i: (i, 0)),
            pl.BlockSpec((CHUNK, width), lambda i: (i, 0)),
            pl.BlockSpec((1, N_STATE, width), lambda i: (i, 0, 0)),
        ],
        out_shape=[
            jax.ShapeDtypeStruct((length, width), bf16),
            jax.ShapeDtypeStruct((length, width), f32),
            jax.ShapeDtypeStruct((count, N_STATE, width), f32),
        ],
        scratch_shapes=[
            pltpu.VMEM((N_STATE, width), f32),
            pltpu.VMEM((CHUNK + 8, all_w), f32),
        ],
        cost_estimate=pl.CostEstimate(
            flops=0, bytes_accessed=70_000_000, transcendentals=0
        ),
        name="mixer_forward",
    )(proj, proj, sel, head, taps)


def bwd_kernel(
    heads,
    count,
    main_ref,
    small_ref,
    main_prev,
    small_prev,
    sel_ref,
    head_ref,
    taps_ref,
    y_ref,
    states_ref,
    dgated_ref,
    dmain_ref,
    dshared_ref,
    dstep_ref,
    dtaps_ref,
    dhead_ref,
    dstate,
    cat,
    dcat,
):
    rows, width = y_ref.shape
    step = pl.program_id(0)

    @pl.when(step == 0)
    def _():
        dstate[...] = jnp.zeros_like(dstate)
        dcat[rows : rows + 8] = jnp.zeros((8, dcat.shape[1]), f32)
        dtaps_ref[...] = jnp.zeros_like(dtaps_ref)
        dhead_ref[...] = jnp.zeros_like(dhead_ref)

    _, inner_prev = split_pairs(main_prev[8:16].astype(f32), heads)
    prev = jnp.concatenate(
        [small_prev[8:16].astype(f32)[:, : 2 * N_STATE], inner_prev], axis=1
    )
    cat[0:8] = jnp.where(step == count - 1, 0.0, prev)
    gate, conv, step_in, dt, neg_rate, decay_log, cumul, r, c = chunk_common(
        heads,
        main_ref[...].astype(f32),
        small_ref[...],
        sel_ref,
        cat,
        head_ref,
        taps_ref,
    )
    sig = jax.nn.sigmoid(conv)
    act = conv * sig
    dsilu = sig * (1.0 + conv * (1.0 - sig))
    b2 = two_parts(act[:, :N_STATE])
    c2 = two_parts(act[:, N_STATE : 2 * N_STATE])
    inner = act[:, 2 * N_STATE :]
    dt_x = expand(dt, heads)
    scaled = inner * dt_x
    scaled2 = two_parts(scaled)
    skip = expand(head_ref[2:3], heads)
    y = y_ref[...]
    sgate = jax.nn.sigmoid(gate)
    dgated = dgated_ref[...].astype(f32)
    dgate = dgated * (y + skip * inner) * (sgate * (1.0 + gate * (1.0 - sgate)))
    dy = dgated * (gate * sgate)
    dy2 = two_parts(dy)

    scores_t = mm3(b2, c2, NT)
    upper = c >= r
    cumul_t = cumul.T
    low = low_half(rows)
    parts = []
    dscores_t = None
    for h in range(heads):
        spread = cumul_t[h : h + 1, :] - cumul[:, h : h + 1]
        decay = jnp.exp(jnp.where(upper, spread, -1e30))
        weights = two_parts(scores_t * decay)
        dy_pair = tuple(pair_of(part, h, heads) for part in dy2)
        parts.append(mm3(weights, dy_pair, NN))
        own = pair_of(scaled, h, heads)
        if own.shape[1] == LANES:
            own = jnp.where(low == (h % 2 == 0), own, 0.0)
        term = mm3(two_parts(own), dy_pair, NT) * decay
        dscores_t = term if dscores_t is None else dscores_t + term
    s_in = states_ref[0]
    s2 = two_parts(s_in)
    ds = dstate[...]
    ds2 = two_parts(ds)
    last = cumul[rows - 1 : rows]
    tail = expand(jnp.exp(last - cumul), heads)
    ecum = expand(jnp.exp(cumul), heads)
    elast = expand(jnp.exp(last), heads)
    tail_b = tail * mm3(b2, ds2, NN)
    z = merge_pairs(parts, heads) + tail_b
    extra = jnp.sum(tail_b * scaled, axis=0, keepdims=True) + elast * jnp.sum(
        ds * s_in, axis=0, keepdims=True
    )
    at_end = lax.broadcasted_iota(jnp.int32, (rows, width), 0) == rows - 1
    u = dy * y - scaled * z + jnp.where(at_end, extra, 0.0)
    pick = (
        lax.broadcasted_iota(jnp.int32, (width, LANES), 0) // P_SIZE
        == lax.broadcasted_iota(jnp.int32, (width, LANES), 1)
    ).astype(f32)
    dcumul = mm_high(u, pick)
    suffix = jnp.where(c >= r, 1.0, 0.0).astype(f32)
    ddecay = mm_high(suffix, dcumul)
    dstep = (mm_high(inner * z, pick) + neg_rate * ddecay) * jax.nn.sigmoid(step_in)
    dstep_ref[...] = dstep.T[: dstep_ref.shape[0]].astype(bf16)
    dhead_ref[0:1] += jnp.sum(dstep, axis=0, keepdims=True)
    dhead_ref[1:2] += jnp.sum(decay_log * ddecay, axis=0, keepdims=True)

    dinner = dt_x * z + skip * dy
    dscores2 = two_parts(dscores_t)
    edy2 = two_parts(ecum * dy)
    db = mm3(dscores2, c2, NN) + mm3(two_parts(tail * scaled), ds2, NT)
    dc = mm3(dscores2, b2, TN) + mm3(edy2, s2, NT)
    dstate[...] = elast * ds + mm3(c2, edy2, TN)

    dconv = jnp.concatenate([db, dc, dinner], axis=1) * dsilu
    dcat[0:rows] = dconv
    draw = taps_ref[3:4] * dconv
    for k in range(3):
        draw = draw + taps_ref[k : k + 1] * dcat[3 - k : 3 - k + rows]
    for k in range(4):
        dtaps_ref[k : k + 1] += jnp.sum(
            dconv * cat[5 + k : 5 + k + rows], axis=0, keepdims=True
        )
    dtaps_ref[4:5] += jnp.sum(dconv, axis=0, keepdims=True)
    dtaps_ref[5:6, 2 * N_STATE :] += jnp.sum(dy * inner, axis=0, keepdims=True)
    dcat[rows : rows + 8] = dconv[0:8]
    dshared_ref[...] = draw[:, : 2 * N_STATE].T.astype(bf16)
    dmain_ref[...] = join_pairs(dgate, draw[:, 2 * N_STATE :], heads).astype(bf16)


def mixer_backward(proj, sel, head, taps, y, states, dgated, heads):
    length, width = y.shape
    count = length // CHUNK
    all_w = width + 2 * N_STATE
    per = CHUNK // 16

    def at(i):
        return (count - 1 - i, 0)

    small_at = 2 * width // (3 * LANES)

    def at_small(i):
        return (count - 1 - i, small_at)

    def before(i):
        return (jnp.maximum((count - 1 - i) * per - 1, 0), 0)

    def before_small(i):
        return (jnp.maximum((count - 1 - i) * per - 1, 0), small_at)

    def fixed(i):
        return (0, 0)

    return pl.pallas_call(
        functools.partial(bwd_kernel, heads, count),
        grid=(count,),
        in_specs=[
            pl.BlockSpec((CHUNK, 2 * width), at),
            pl.BlockSpec((CHUNK, 3 * LANES), at_small),
            pl.BlockSpec((16, 2 * width), before),
            pl.BlockSpec((16, 3 * LANES), before_small),
            pl.BlockSpec((LANES, LANES), fixed),
            pl.BlockSpec((8, LANES), fixed),
            pl.BlockSpec((8, all_w), fixed),
            pl.BlockSpec((CHUNK, width), at),
            pl.BlockSpec((1, N_STATE, width), lambda i: (count - 1 - i, 0, 0)),
            pl.BlockSpec((CHUNK, width), at),
        ],
        out_specs=[
            pl.BlockSpec((CHUNK, 2 * width), at),
            pl.BlockSpec((2 * N_STATE, CHUNK), lambda i: (0, count - 1 - i)),
            pl.BlockSpec((STEP_ROWS, CHUNK), lambda i: (0, count - 1 - i)),
            pl.BlockSpec((8, all_w), fixed),
            pl.BlockSpec((8, LANES), fixed),
        ],
        out_shape=[
            jax.ShapeDtypeStruct((length, 2 * width), bf16),
            jax.ShapeDtypeStruct((2 * N_STATE, length), bf16),
            jax.ShapeDtypeStruct((STEP_ROWS, length), bf16),
            jax.ShapeDtypeStruct((8, all_w), f32),
            jax.ShapeDtypeStruct((8, LANES), f32),
        ],
        scratch_shapes=[
            pltpu.VMEM((N_STATE, width), f32),
            pltpu.VMEM((CHUNK + 8, all_w), f32),
            pltpu.VMEM((CHUNK + 8, all_w), f32),
        ],
        cost_estimate=pl.CostEstimate(
            flops=0, bytes_accessed=160_000_000, transcendentals=0
        ),
        name="mixer_backward",
    )(proj, proj, proj, proj, sel, head, taps, y, states, dgated)


MESH = pl.DeviceIdType.MESH


def greet(peers, count):
    barrier = pltpu.get_barrier_semaphore()
    for peer in peers:
        pl.semaphore_signal(barrier, inc=1, device_id=peer, device_id_type=MESH)
    pl.semaphore_wait(barrier, count)


def wire(src, dst, send, recv, peer):
    return pltpu.make_async_remote_copy(
        src_ref=src,
        dst_ref=dst,
        send_sem=send,
        recv_sem=recv,
        device_id=peer,
        device_id_type=MESH,
    )


def weights_kernel(n_seq, n_wsh, main, small, w_all, *sems):
    send_a, recv_a, send_b, recv_b, send_e, recv_e, send_r, recv_r, send_l, recv_l, own = sems
    cols = main.shape[2]

    def main_at(i, j):
        return w_all.at[i, j, :, :cols]

    def small_at(i, j):
        return w_all.at[i, j, :, cols:]

    s = lax.axis_index("seq")
    w = lax.axis_index("wshard")
    row = [(lax.rem(s + k, n_seq), w) for k in range(1, n_seq)]
    col = [(s, lax.rem(w + j, n_wsh)) for j in range(1, n_wsh)]
    greet(row + col, n_seq + n_wsh - 2)
    first = [
        wire(main.at[peer[0]], main_at(s, w), send_a.at[k], recv_a.at[k], peer)
        for k, peer in enumerate(row)
    ]
    spread = [
        wire(small, small_at(s, w), send_b.at[j], recv_b.at[j], peer)
        for j, peer in enumerate(col)
    ]
    plane = w_all.at[s, :, :, cols:]
    third = [
        wire(plane, plane, send_e.at[k], recv_e.at[k], peer)
        for k, peer in enumerate(row)
    ]
    mine = [
        pltpu.make_async_copy(main.at[s], main_at(s, w), own.at[0]),
        pltpu.make_async_copy(small, small_at(s, w), own.at[1]),
    ]

    def right(t):
        block = w_all.at[:, jnp.maximum(w - t, 0), :, :cols]
        peer = (s, jnp.minimum(w + 1, n_wsh - 1))
        return wire(block, block, send_r.at[t], recv_r.at[t], peer)

    def left(t):
        block = w_all.at[:, jnp.minimum(w + t, n_wsh - 1), :, :cols]
        peer = (s, jnp.maximum(w - 1, 0))
        return wire(block, block, send_l.at[t], recv_l.at[t], peer)

    for copy in mine + first + spread:
        copy.start()
    mine[0].wait()
    for copy in first:
        copy.wait_recv()
    last = n_wsh - 1
    for t in range(n_wsh):
        if t > 0:
            pl.when(w >= t)(lambda t=t: right(t - 1).wait_recv())
        if t < last:
            pl.when((w >= t) & (w < last))(lambda t=t: right(t).start())
        if t > 0:
            pl.when(w + t <= last)(lambda t=t: left(t - 1).wait_recv())
        if t < last:
            pl.when((w + t <= last) & (w > 0))(lambda t=t: left(t).start())
        if t == 0:
            mine[1].wait()
            for copy in spread:
                copy.wait_recv()
            for copy in third:
                copy.start()
    for copy in first + spread:
        copy.wait_send()
    for copy in third:
        copy.wait()
    for t in range(last):
        pl.when((w >= t) & (w < last))(lambda t=t: right(t).wait_send())
        pl.when((w + t <= last) & (w > 0))(lambda t=t: left(t).wait_send())


def spread_weights(main, small, n_seq, n_wsh):
    rows_in, cols = main.shape[1:]
    anywhere = pl.BlockSpec(memory_space=pl.ANY)
    dma = pltpu.SemaphoreType.DMA
    a, c = n_seq - 1, n_wsh - 1
    return pl.pallas_call(
        functools.partial(weights_kernel, n_seq, n_wsh),
        in_specs=[anywhere] * 2,
        out_specs=anywhere,
        out_shape=jax.ShapeDtypeStruct(
            (n_seq, n_wsh, rows_in, cols + small.shape[1]), bf16
        ),
        scratch_shapes=[dma((n,)) for n in (a, a, c, c, a, a, c, c, c, c, 2)],
        compiler_params=pltpu.CompilerParams(collective_id=0, has_side_effects=True),
        cost_estimate=pl.CostEstimate(
            flops=0, bytes_accessed=200_000_000, transcendentals=0
        ),
        name="spread_weights",
    )(main, small)


def swap_kernel(plan, n_seq, n_wsh, *refs):
    n = len(plan)
    ins, outs, sems = refs[:n], refs[n : 2 * n], refs[2 * n :]
    s = lax.axis_index("seq")
    w = lax.axis_index("wshard")
    total = n_seq * n_wsh
    me_all = s * n_wsh + w
    size = {"seq": n_seq, "wshard": n_wsh, "both": total}
    me_of = {"seq": s, "wshard": w, "both": me_all}

    def peer_at(axis, k):
        if axis == "seq":
            index = lax.rem(s + k, n_seq)
            return index, (index, w)
        if axis == "wshard":
            index = lax.rem(w + k, n_wsh)
            return index, (s, index)
        index = lax.rem(me_all + k, total)
        return index, (lax.div(index, n_wsh), lax.rem(index, n_wsh))

    def block(kind, ref, index):
        if kind == "all":
            return ref
        return ref.at[index] if kind == 0 else ref.at[:, index]

    def copy_of(i, k):
        kind, axis = plan[i]
        index, peer = peer_at(axis, k)
        return wire(
            block(kind, ins[i], index),
            outs[i].at[me_of[axis]],
            sems[3 * i].at[k],
            sems[3 * i + 1].at[k],
            peer,
        )

    widest = "both" if any(axis == "both" for _, axis in plan) else plan[0][1]
    barrier = pltpu.get_barrier_semaphore()

    def hail(k, _):
        pl.semaphore_signal(
            barrier, inc=1, device_id=peer_at(widest, k)[1], device_id_type=MESH
        )
        return 0

    lax.fori_loop(1, size[widest], hail, 0)
    pl.semaphore_wait(barrier, size[widest] - 1)
    own = []
    for i, (kind, axis) in enumerate(plan):
        me = me_of[axis]
        own.append(
            pltpu.make_async_copy(
                block(kind, ins[i], me), outs[i].at[me], sems[3 * i + 2].at[0]
            )
        )

        def begin(k, _, i=i):
            copy_of(i, k).start()
            return 0

        lax.fori_loop(1, size[axis], begin, 0)
    for copy in own:
        copy.start()
    for i, (kind, axis) in enumerate(plan):
        own[i].wait()

        def finish(k, _, i=i):
            copy_of(i, k).wait()
            return 0

        lax.fori_loop(1, size[axis], finish, 0)


def swap(arrays, plan, n_seq, n_wsh, collective_id):
    anywhere = pl.BlockSpec(memory_space=pl.ANY)
    size = {"seq": n_seq, "wshard": n_wsh, "both": n_seq * n_wsh}
    shapes, sems = [], []
    for x, (kind, axis) in zip(arrays, plan):
        n = size[axis]
        shape = x.shape
        if kind == 0:
            shape = shape[1:]
        elif kind == 1:
            shape = shape[:1] + shape[2:]
        shapes.append(jax.ShapeDtypeStruct((n,) + shape, x.dtype))
        sems += [
            pltpu.SemaphoreType.DMA((n,)),
            pltpu.SemaphoreType.DMA((n,)),
            pltpu.SemaphoreType.DMA((1,)),
        ]
    return pl.pallas_call(
        functools.partial(swap_kernel, plan, n_seq, n_wsh),
        in_specs=[anywhere] * len(arrays),
        out_specs=[anywhere] * len(arrays),
        out_shape=shapes,
        scratch_shapes=sems,
        compiler_params=pltpu.CompilerParams(
            collective_id=collective_id, has_side_effects=True
        ),
    )(*arrays)


def stats_kernel(n_seq, x_ref, out_ref, slots, send, recv):
    s = lax.axis_index("seq")
    w = lax.axis_index("wshard")
    row = [(lax.rem(s + k, n_seq), w) for k in range(1, n_seq)]
    greet(row, n_seq - 1)
    copies = [
        wire(x_ref, slots.at[s], send.at[k], recv.at[k], peer)
        for k, peer in enumerate(row)
    ]
    for copy in copies:
        copy.start()
    slots[s] = x_ref[...]
    for copy in copies:
        copy.wait()
    total = slots[0]
    for k in range(1, n_seq):
        total = total + slots[k]
    out_ref[...] = total


def sum_over_seq(x, n_seq):
    vmem = pl.BlockSpec(memory_space=pltpu.VMEM)
    dma = pltpu.SemaphoreType.DMA
    return pl.pallas_call(
        functools.partial(stats_kernel, n_seq),
        in_specs=[vmem],
        out_specs=vmem,
        out_shape=jax.ShapeDtypeStruct(x.shape, f32),
        scratch_shapes=[
            pltpu.VMEM((n_seq,) + x.shape, f32),
            dma((n_seq - 1,)),
            dma((n_seq - 1,)),
        ],
        compiler_params=pltpu.CompilerParams(collective_id=1, has_side_effects=True),
        name="sum_over_seq",
    )(x)


def adamw(param, grad, first, second_moment, rate, decay):
    first_new = beta_one * first + (1.0 - beta_one) * grad
    second_new = beta_two * second_moment + (1.0 - beta_two) * grad * grad
    corrected = (
        first_new
        / (1.0 - beta_one**adam_step)
        / (jnp.sqrt(second_new / (1.0 - beta_two**adam_step)) + adam_eps)
    )
    return (param - rate * (corrected + decay * param), first_new, second_new)


def shift(x, j, n_wsh):
    return lax.ppermute(x, "wshard", [(i, (i + j) % n_wsh) for i in range(n_wsh)])


def adam_kernel(count, g_ref, ext_ref, p_ref, m_ref, v_ref, grad_ref, *out_refs):
    at_ext = pl.program_id(0) == count
    grad = jnp.where(at_ext, ext_ref[...].astype(f32), g_ref[0].astype(f32))
    grad_ref[...] = grad
    news = adamw(
        p_ref[...], grad, m_ref[...], v_ref[...], weight_learning_rate, matrix_decay
    )
    for ref, new in zip(out_refs, news):
        ref[...] = new


def adam_in(g_main, g_ext, param, first, second):
    count, rows, cols = g_main.shape
    wide = pl.BlockSpec((rows, cols), lambda i: (0, i))
    return pl.pallas_call(
        functools.partial(adam_kernel, count),
        grid=(count + 1,),
        in_specs=[
            pl.BlockSpec((1, rows, cols), lambda i: (jnp.minimum(i, count - 1), 0, 0)),
            pl.BlockSpec((rows, cols), lambda i: (0, 0)),
            wide,
            wide,
            wide,
        ],
        out_specs=[wide] * 4,
        out_shape=[jax.ShapeDtypeStruct(param.shape, f32)] * 4,
        name="adam_in",
    )(g_main, g_ext, param, first, second)


def local(
    block_in,
    cotangent,
    in_weight,
    out_weight,
    in_gain,
    out_gain,
    conv_inner,
    conv_shared,
    head_params,
    first_in_weight,
    first_out_weight,
    first_in_gain,
    first_out_gain,
    first_conv_inner,
    first_conv_shared,
    first_head_params,
    second_in_weight,
    second_out_weight,
    second_in_gain,
    second_out_gain,
    second_conv_inner,
    second_conv_shared,
    second_head_params,
):
    seq_index = lax.axis_index("seq")
    wsh_index = lax.axis_index("wshard")
    n_seq = lax.axis_size("seq")
    n_wsh = lax.axis_size("wshard")
    rows_in, _ = in_weight.shape
    rows_out = out_weight.shape[0]
    _, width_in = block_in.shape[1:]
    heads = head_params.shape[1] // n_seq
    width = heads * P_SIZE
    inner_all = out_gain.shape[0]
    share = 2 * N_STATE // n_seq

    inputs = block_in[0].astype(f32)
    rms_in = lax.rsqrt(jnp.mean(inputs * inputs, axis=-1, keepdims=True) + norm_eps)
    normed = (inputs * rms_in * in_gain).astype(bf16)
    normed_all = lax.all_gather(normed, "seq", axis=0, tiled=True)
    cot = cotangent[0]
    cot_all = lax.all_gather(cot, "seq", axis=0, tiled=True)
    in_w16 = in_weight.astype(bf16)
    main_send = in_w16[:, : 2 * inner_all].reshape(rows_in, n_seq, 2 * width)
    main_send = jnp.swapaxes(main_send, 0, 1)
    small_send = in_w16[:, 2 * inner_all :]
    small_send = jnp.pad(small_send, ((0, 0), (0, -small_send.shape[1] % LANES)))
    w_all = spread_weights(main_send, small_send, n_seq, n_wsh)
    out_w16, w_all = lax.optimization_barrier((out_weight.astype(bf16), w_all))
    w_all = w_all.reshape(width_in, 2 * width + small_send.shape[1])
    proj = mm(normed_all, w_all, NN).astype(bf16)
    w_main = w_all[:, : 2 * width]
    w_small = w_all[:, 2 * width :]
    w_out = jnp.zeros((n_wsh,) + out_w16.shape, bf16)
    w_out = lax.dynamic_update_index_in_dim(w_out, out_w16, wsh_index, 0)
    for j in range(1, n_wsh):
        got = shift(out_w16, j, n_wsh)
        w_out = lax.dynamic_update_index_in_dim(
            w_out, got, lax.rem(wsh_index - j + n_wsh, n_wsh), 0
        )
    w_out = w_out.reshape(width, width_in)

    def pick(first, count, width_to):
        col = lax.broadcasted_iota(jnp.int32, (w_small.shape[1], width_to), 0)
        lane = lax.broadcasted_iota(jnp.int32, (w_small.shape[1], width_to), 1)
        return jnp.where((col == lane + first) & (lane < count), 1.0, 0.0)

    to_step = pick(2 * N_STATE + seq_index * heads, heads, LANES)
    to_ext = jnp.concatenate(
        [pick(seq_index * share, share, share), to_step[:, :STEP_ROWS]], axis=1
    )
    w_ext = mm(w_small, to_ext.astype(bf16), NN).astype(bf16)
    sel = to_step[2 * N_STATE :].astype(bf16)

    head_local = lax.dynamic_slice_in_dim(head_params, seq_index * heads, heads, 1)
    head = jnp.pad(head_local, ((0, 5), (0, LANES - heads)))
    conv_local = lax.dynamic_slice_in_dim(conv_inner, seq_index * width, width, 1)
    taps = jnp.pad(jnp.concatenate([conv_shared, conv_local], axis=1), ((0, 3), (0, 0)))
    gain_local = lax.dynamic_slice_in_dim(out_gain, seq_index * width, width, 0)
    gated, y, states = mixer_forward(proj, sel, head, taps, heads)
    d_gnormed = mm(cot_all, w_out, NT)
    gated32 = gated.astype(f32)
    scaled = d_gnormed * gain_local
    stats = jnp.stack(
        [jnp.sum(gated32 * gated32, axis=-1), jnp.sum(scaled * gated32, axis=-1)]
    )
    stats = sum_over_seq(stats.reshape(-1, LANES), n_seq).reshape(stats.shape)
    rms_out = lax.rsqrt(stats[0] / inner_all + norm_eps)[:, None]
    mean_sg = (stats[1] / inner_all)[:, None]
    gnormed = (gated32 * rms_out * gain_local).astype(bf16)
    d_gated = (rms_out * scaled - gated32 * rms_out**3 * mean_sg).astype(bf16)
    d_out_gain = jnp.sum(d_gnormed * gated32 * rms_out, axis=0)

    g_out = mm(gnormed, cot_all, TN)
    mixed = mm(gnormed, w_out, NN).astype(bf16)
    g_out, mixed, d_gated = lax.optimization_barrier((g_out, mixed, d_gated))
    mixed = lax.psum_scatter(mixed, "seq", scatter_dimension=0, tiled=True)
    out_parts = [lax.dynamic_slice_in_dim(g_out, wsh_index * rows_out, rows_out, 0)]
    for j in range(1, n_wsh):
        to = lax.rem(wsh_index + j, n_wsh)
        part = lax.dynamic_slice_in_dim(g_out, to * rows_out, rows_out, 0)
        out_parts.append(shift(part, j, n_wsh))
    dmain, dshared_t, dstep_t, dtaps, dhead = mixer_backward(
        proj, sel, head, taps, y, states, d_gated, heads
    )

    g_main = mm(normed_all, dmain, TN)
    g_full = g_main
    g_main = g_main.astype(bf16).reshape(n_seq, n_wsh, rows_in, 2 * width)
    g_parts = [lax.dynamic_index_in_dim(g_main, wsh_index, 1, keepdims=False)]
    for j in range(1, n_wsh):
        to = lax.rem(wsh_index + j, n_wsh)
        part = lax.dynamic_index_in_dim(g_main, to, 1, keepdims=False)
        g_parts.append(shift(part, j, n_wsh))

    (shared_parts,) = swap(
        (dshared_t.reshape(n_seq, share, -1),), ((0, "seq"),), n_seq, n_wsh, 2
    )
    shared_sum = jnp.sum(shared_parts.astype(f32), axis=0).astype(bf16)
    d_ext = jnp.concatenate([shared_sum, dstep_t], axis=0)
    d_normed = mm(dmain, w_main, NT) + lax.dot_general(
        d_ext, w_ext, (((0,), (1,)), ((), ())), preferred_element_type=f32
    )
    d_normed, mixed, g_full, d_ext = lax.optimization_barrier(
        (d_normed.astype(bf16), mixed, g_full, d_ext)
    )
    block_out = (inputs + mixed.astype(f32))[None]
    d_normed = lax.psum_scatter(d_normed, "seq", scatter_dimension=0, tiled=True)
    d_normed = d_normed.astype(f32)
    scaled_in = d_normed * in_gain
    grad_in = (
        cot.astype(f32)
        + rms_in * scaled_in
        - inputs * rms_in**3 * jnp.mean(scaled_in * inputs, axis=-1, keepdims=True)
    )[None]

    g_ext = lax.dot_general(
        normed_all, d_ext, (((0,), (1,)), ((), ())), preferred_element_type=f32
    )
    d_gain_part = jnp.sum(g_full * w_main.astype(f32), axis=1) + jnp.sum(
        g_ext * w_ext.astype(f32), axis=1
    )
    g_ext = jnp.pad(g_ext.astype(bf16), ((0, 0), (0, -g_ext.shape[1] % LANES)))
    g_ext = g_ext.reshape(n_seq, n_wsh, rows_in, LANES)

    d_skip = dtaps[5, 2 * N_STATE :].reshape(heads, P_SIZE).sum(-1)
    d_head = jnp.concatenate([dhead[:2, :heads], d_skip[None]], axis=0)
    pieces = (
        d_gain_part,
        dtaps[:5, : 2 * N_STATE],
        d_out_gain,
        dtaps[:5, 2 * N_STATE :],
        d_head,
    )
    flat = jnp.concatenate([p.reshape(-1) for p in pieces])
    flat = jnp.pad(flat, (0, -flat.shape[0] % (8 * LANES))).reshape(-1, LANES)
    g_ext, flat = swap(
        (g_ext, flat), ((1, "wshard"), ("all", "wshard")), n_seq, n_wsh, 3
    )
    g_ext = jnp.sum(g_ext.astype(f32), axis=0)
    (flat,) = swap((jnp.sum(flat, axis=0),), (("all", "seq"),), n_seq, n_wsh, 4)
    flat = flat.reshape(n_seq, -1)
    sums, at = [], 0
    for p in pieces:
        sums.append(flat[:, at : at + p.size].reshape((n_seq,) + p.shape))
        at += p.size
    grad_in_gain = jnp.sum(sums[0], axis=0) / in_gain
    grad_conv_shared = jnp.sum(sums[1], axis=0)
    grad_out_gain = sums[2].reshape(-1)
    grad_conv_inner = jnp.swapaxes(sums[3], 0, 1).reshape(conv_inner.shape)
    grad_head_params = jnp.swapaxes(sums[4], 0, 1).reshape(head_params.shape)

    flat, out_parts = lax.optimization_barrier((flat, out_parts))
    grad_out_weight = sum(out_parts)
    new_out_weight, new_first_out_weight, new_second_out_weight = adamw(
        out_weight,
        grad_out_weight,
        first_out_weight,
        second_out_weight,
        weight_learning_rate,
        matrix_decay,
    )
    ready = (new_out_weight, new_first_out_weight, new_second_out_weight, grad_out_weight)
    ready, g_parts = lax.optimization_barrier((ready, g_parts))
    new_out_weight, new_first_out_weight, new_second_out_weight, grad_out_weight = ready
    g_main = g_parts[0].astype(f32)
    for part in g_parts[1:]:
        g_main = g_main + part.astype(f32)
    g_main, g_ext = swap(
        (g_main.astype(bf16), g_ext.astype(bf16)),
        ((0, "seq"), (0, "seq")),
        n_seq,
        n_wsh,
        5,
    )
    g_ext = jnp.swapaxes(g_ext, 0, 1)
    g_ext = jnp.concatenate(
        [
            g_ext[:, :, :share].reshape(rows_in, 2 * N_STATE),
            g_ext[:, :, share : share + heads].reshape(rows_in, heads * n_seq),
        ],
        axis=1,
    )
    g_ext = jnp.pad(g_ext, ((0, 0), (0, 2 * width - g_ext.shape[1])))
    grad_in_weight, new_in_weight, new_first_in_weight, new_second_in_weight = adam_in(
        g_main, g_ext, in_weight, first_in_weight, second_in_weight
    )
    updated_input_gain, new_first_in_gain, new_second_in_gain = adamw(
        in_gain, grad_in_gain, first_in_gain, second_in_gain, small_rate, 0.0
    )
    new_out_gain, new_first_out_gain, new_second_out_gain = adamw(
        out_gain, grad_out_gain, first_out_gain, second_out_gain, small_rate, 0.0
    )
    new_conv_inner, new_first_conv_inner, new_second_conv_inner = adamw(
        conv_inner, grad_conv_inner, first_conv_inner, second_conv_inner, small_rate, 0.0
    )
    new_conv_shared, new_first_conv_shared, new_second_conv_shared = adamw(
        conv_shared, grad_conv_shared, first_conv_shared, second_conv_shared, small_rate, 0.0
    )
    new_head_params, updated_head_first_moment, head_second_all = adamw(
        head_params, grad_head_params, first_head_params, second_head_params, small_rate, 0.0
    )
    return (
        block_out,
        grad_in,
        grad_in_weight,
        grad_out_weight,
        grad_in_gain,
        grad_out_gain,
        grad_conv_inner,
        grad_conv_shared,
        grad_head_params,
        new_in_weight,
        new_out_weight,
        updated_input_gain,
        new_out_gain,
        new_conv_inner,
        new_conv_shared,
        new_head_params,
        new_first_in_weight,
        new_first_out_weight,
        new_first_in_gain,
        new_first_out_gain,
        new_first_conv_inner,
        new_first_conv_shared,
        updated_head_first_moment,
        new_second_in_weight,
        new_second_out_weight,
        new_second_in_gain,
        new_second_out_gain,
        new_second_conv_inner,
        new_second_conv_shared,
        head_second_all[0:2],
        head_second_all[2],
    )


def solution(mesh):
    return jax.shard_map(
        local,
        mesh=mesh,
        in_specs=(
            P("wshard", "seq", None),
            P("wshard", "seq", None),
            P(("seq", "wshard"), None),
            P(("seq", "wshard"), None),
            P(),
            P(),
            P(),
            P(),
            P(),
            P(("seq", "wshard"), None),
            P(("seq", "wshard"), None),
            P(),
            P(),
            P(),
            P(),
            P(),
            P(("seq", "wshard"), None),
            P(("seq", "wshard"), None),
            P(),
            P(),
            P(),
            P(),
            P(),
        ),
        out_specs=(
            P("wshard", "seq", None),
            P("wshard", "seq", None),
            P(("seq", "wshard"), None),
            P(("seq", "wshard"), None),
            P(),
            P(),
            P(),
            P(),
            P(),
            P(("seq", "wshard"), None),
            P(("seq", "wshard"), None),
            P(),
            P(),
            P(),
            P(),
            P(),
            P(("seq", "wshard"), None),
            P(("seq", "wshard"), None),
            P(),
            P(),
            P(),
            P(),
            P(),
            P(("seq", "wshard"), None),
            P(("seq", "wshard"), None),
            P(),
            P(),
            P(),
            P(),
            P(),
            P(),
        ),
        check_vma=False,
    )
```

```python
import functools

import jax
import jax.numpy as jnp
from jax import lax
from jax.experimental import pallas as pl
from jax.experimental.pallas import tpu as pltpu
from jax.sharding import PartitionSpec as P


P_SIZE = 64
N_STATE = 128
LANES = 128
CHUNK = 128
STEP_ROWS = 16

norm_eps = 1e-05
beta_one = 0.9
beta_two = 0.95
adam_eps = 1e-08
adam_step = 3.0
weight_learning_rate = 0.01
matrix_decay = 0.1
small_rate = 0.1


f32 = jnp.float32
bf16 = jnp.bfloat16
NN = (((1,), (0,)), ((), ()))
NT = (((1,), (1,)), ((), ()))
TN = (((0,), (0,)), ((), ()))


def mm(a, b, dims):
    return lax.dot_general(a, b, dims, preferred_element_type=f32)


def mm_high(a, b):
    return lax.dot_general(
        a, b, NN, precision=lax.Precision.HIGHEST, preferred_element_type=f32
    )


def two_parts(a):
    hi = a.astype(bf16)
    return hi, (a - hi.astype(f32)).astype(bf16)


def mm3(a, b, dims):
    return mm(a[0], b[0], dims) + (mm(a[0], b[1], dims) + mm(a[1], b[0], dims))


def low_half(rows):
    return lax.broadcasted_iota(jnp.int32, (rows, LANES), 1) < P_SIZE


def split_pairs(values, heads):
    low = low_half(values.shape[0])
    gates, inners = [], []
    for h in range(0, heads, 2):
        a = values[:, h * LANES : (h + 1) * LANES]
        a_r = pltpu.roll(a, P_SIZE, 1)
        if h + 1 < heads:
            b = values[:, (h + 1) * LANES : (h + 2) * LANES]
            b_r = pltpu.roll(b, P_SIZE, 1)
            gates.append(jnp.where(low, a, b_r))
            inners.append(jnp.where(low, a_r, b))
        else:
            gates.append(a[:, :P_SIZE])
            inners.append(a_r[:, :P_SIZE])
    return jnp.concatenate(gates, axis=1), jnp.concatenate(inners, axis=1)


def join_pairs(gate, inner, heads):
    low = low_half(gate.shape[0])
    out = []
    for h in range(0, heads, 2):
        if h + 1 < heads:
            g = gate[:, h * P_SIZE : (h + 2) * P_SIZE]
            x = inner[:, h * P_SIZE : (h + 2) * P_SIZE]
            out.append(jnp.where(low, g, pltpu.roll(x, P_SIZE, 1)))
            out.append(jnp.where(low, pltpu.roll(g, P_SIZE, 1), x))
        else:
            out.append(
                jnp.concatenate(
                    [gate[:, h * P_SIZE :], inner[:, h * P_SIZE :]], axis=1
                )
            )
    return jnp.concatenate(out, axis=1)


def expand(cols, heads):
    rows = cols.shape[0]
    low = low_half(rows)
    out = []
    for h in range(0, heads, 2):
        if h + 1 < heads:
            one = jnp.broadcast_to(cols[:, h : h + 1], (rows, LANES))
            two = jnp.broadcast_to(cols[:, h + 1 : h + 2], (rows, LANES))
            out.append(jnp.where(low, one, two))
        else:
            out.append(jnp.broadcast_to(cols[:, h : h + 1], (rows, P_SIZE)))
    return jnp.concatenate(out, axis=1)


def pair_of(values, h, heads):
    first = h - h % 2
    return values[:, first * P_SIZE : min(first + 2, heads) * P_SIZE]


def merge_pairs(parts, heads):
    low = low_half(parts[0].shape[0])
    out = []
    for h in range(0, heads, 2):
        if h + 1 < heads:
            out.append(jnp.where(low, parts[h], parts[h + 1]))
        else:
            out.append(parts[h])
    return jnp.concatenate(out, axis=1)


def chunk_common(heads, main, small16, sel_ref, cat, head_ref, taps_ref):
    rows = main.shape[0]
    gate, inner = split_pairs(main, heads)
    raw = jnp.concatenate([small16[:, : 2 * N_STATE].astype(f32), inner], axis=1)
    cat[8 : 8 + rows] = raw
    conv = taps_ref[4:5] + taps_ref[0:1] * cat[5 : 5 + rows]
    for k in range(1, 4):
        conv = conv + taps_ref[k : k + 1] * cat[5 + k : 5 + k + rows]
    step_in = mm(small16[:, 2 * N_STATE :], sel_ref[...], NN) + head_ref[0:1]
    dt = jnp.maximum(step_in, 0.0) + jnp.log1p(jnp.exp(-jnp.abs(step_in)))
    neg_rate = -jnp.exp(head_ref[1:2])
    decay_log = neg_rate * dt
    r = lax.broadcasted_iota(jnp.int32, (rows, rows), 0)
    c = lax.broadcasted_iota(jnp.int32, (rows, rows), 1)
    tri = jnp.where(r >= c, 1.0, 0.0).astype(f32)
    cumul = mm_high(tri, decay_log)
    return gate, conv, step_in, dt, neg_rate, decay_log, cumul, r, c


def fwd_kernel(
    heads, main_ref, small_ref, sel_ref, head_ref, taps_ref, gated_ref, y_ref, states_ref, state, cat
):
    rows = main_ref.shape[0]

    @pl.when(pl.program_id(0) == 0)
    def _():
        state[...] = jnp.zeros_like(state)
        cat[0:8] = jnp.zeros((8, cat.shape[1]), f32)

    gate, conv, _, dt, _, _, cumul, r, c = chunk_common(
        heads,
        main_ref[...].astype(f32),
        small_ref[...],
        sel_ref,
        cat,
        head_ref,
        taps_ref,
    )
    cat[0:8] = cat[rows : rows + 8]
    act = conv * jax.nn.sigmoid(conv)
    b2 = two_parts(act[:, :N_STATE])
    c2 = two_parts(act[:, N_STATE : 2 * N_STATE])
    inner = act[:, 2 * N_STATE :]
    scaled = inner * expand(dt, heads)
    scaled2 = two_parts(scaled)
    scores = mm3(c2, b2, NT)
    lower = r >= c
    cumul_t = cumul.T
    parts = []
    for h in range(heads):
        spread = cumul[:, h : h + 1] - cumul_t[h : h + 1, :]
        weights = two_parts(scores * jnp.exp(jnp.where(lower, spread, -1e30)))
        own = tuple(pair_of(part, h, heads) for part in scaled2)
        parts.append(mm3(weights, own, NN))
    s2 = two_parts(state[...])
    states_ref[0] = state[...]
    last = cumul[rows - 1 : rows]
    y = merge_pairs(parts, heads) + expand(jnp.exp(cumul), heads) * mm3(c2, s2, NN)
    y_ref[...] = y
    tail = expand(jnp.exp(last - cumul), heads)
    fresh = mm3(b2, two_parts(tail * scaled), TN)
    state[...] = expand(jnp.exp(last), heads) * state[...] + fresh
    full = y + expand(head_ref[2:3], heads) * inner
    gated_ref[...] = (full * (gate * jax.nn.sigmoid(gate))).astype(bf16)


def mixer_forward(proj, sel, head, taps, heads):
    length = proj.shape[0]
    width = heads * P_SIZE
    count = length // CHUNK
    all_w = width + 2 * N_STATE
    return pl.pallas_call(
        functools.partial(fwd_kernel, heads),
        grid=(count,),
        in_specs=[
            pl.BlockSpec((CHUNK, 2 * width), lambda i: (i, 0)),
            pl.BlockSpec((CHUNK, 3 * LANES), lambda i: (i, 2 * width // (3 * LANES))),
            pl.BlockSpec((LANES, LANES), lambda i: (0, 0)),
            pl.BlockSpec((8, LANES), lambda i: (0, 0)),
            pl.BlockSpec((8, all_w), lambda i: (0, 0)),
        ],
        out_specs=[
            pl.BlockSpec((CHUNK, width), lambda i: (i, 0)),
            pl.BlockSpec((CHUNK, width), lambda i: (i, 0)),
            pl.BlockSpec((1, N_STATE, width), lambda i: (i, 0, 0)),
        ],
        out_shape=[
            jax.ShapeDtypeStruct((length, width), bf16),
            jax.ShapeDtypeStruct((length, width), f32),
            jax.ShapeDtypeStruct((count, N_STATE, width), f32),
        ],
        scratch_shapes=[
            pltpu.VMEM((N_STATE, width), f32),
            pltpu.VMEM((CHUNK + 8, all_w), f32),
        ],
        cost_estimate=pl.CostEstimate(
            flops=0, bytes_accessed=70_000_000, transcendentals=0
        ),
        name="mixer_forward",
    )(proj, proj, sel, head, taps)


def bwd_kernel(
    heads,
    count,
    main_ref,
    small_ref,
    main_prev,
    small_prev,
    sel_ref,
    head_ref,
    taps_ref,
    y_ref,
    states_ref,
    dgated_ref,
    dmain_ref,
    dshared_ref,
    dstep_ref,
    dtaps_ref,
    dhead_ref,
    dstate,
    cat,
    dcat,
):
    rows, width = y_ref.shape
    step = pl.program_id(0)

    @pl.when(step == 0)
    def _():
        dstate[...] = jnp.zeros_like(dstate)
        dcat[rows : rows + 8] = jnp.zeros((8, dcat.shape[1]), f32)
        dtaps_ref[...] = jnp.zeros_like(dtaps_ref)
        dhead_ref[...] = jnp.zeros_like(dhead_ref)

    _, inner_prev = split_pairs(main_prev[8:16].astype(f32), heads)
    prev = jnp.concatenate(
        [small_prev[8:16].astype(f32)[:, : 2 * N_STATE], inner_prev], axis=1
    )
    cat[0:8] = jnp.where(step == count - 1, 0.0, prev)
    gate, conv, step_in, dt, neg_rate, decay_log, cumul, r, c = chunk_common(
        heads,
        main_ref[...].astype(f32),
        small_ref[...],
        sel_ref,
        cat,
        head_ref,
        taps_ref,
    )
    sig = jax.nn.sigmoid(conv)
    act = conv * sig
    dsilu = sig * (1.0 + conv * (1.0 - sig))
    b2 = two_parts(act[:, :N_STATE])
    c2 = two_parts(act[:, N_STATE : 2 * N_STATE])
    inner = act[:, 2 * N_STATE :]
    dt_x = expand(dt, heads)
    scaled = inner * dt_x
    scaled2 = two_parts(scaled)
    skip = expand(head_ref[2:3], heads)
    y = y_ref[...]
    sgate = jax.nn.sigmoid(gate)
    dgated = dgated_ref[...].astype(f32)
    dgate = dgated * (y + skip * inner) * (sgate * (1.0 + gate * (1.0 - sgate)))
    dy = dgated * (gate * sgate)
    dy2 = two_parts(dy)

    scores_t = mm3(b2, c2, NT)
    upper = c >= r
    cumul_t = cumul.T
    low = low_half(rows)
    parts = []
    dscores_t = None
    for h in range(heads):
        spread = cumul_t[h : h + 1, :] - cumul[:, h : h + 1]
        decay = jnp.exp(jnp.where(upper, spread, -1e30))
        weights = two_parts(scores_t * decay)
        dy_pair = tuple(pair_of(part, h, heads) for part in dy2)
        parts.append(mm3(weights, dy_pair, NN))
        own = pair_of(scaled, h, heads)
        if own.shape[1] == LANES:
            own = jnp.where(low == (h % 2 == 0), own, 0.0)
        term = mm3(two_parts(own), dy_pair, NT) * decay
        dscores_t = term if dscores_t is None else dscores_t + term
    s_in = states_ref[0]
    s2 = two_parts(s_in)
    ds = dstate[...]
    ds2 = two_parts(ds)
    last = cumul[rows - 1 : rows]
    tail = expand(jnp.exp(last - cumul), heads)
    ecum = expand(jnp.exp(cumul), heads)
    elast = expand(jnp.exp(last), heads)
    tail_b = tail * mm3(b2, ds2, NN)
    z = merge_pairs(parts, heads) + tail_b
    extra = jnp.sum(tail_b * scaled, axis=0, keepdims=True) + elast * jnp.sum(
        ds * s_in, axis=0, keepdims=True
    )
    at_end = lax.broadcasted_iota(jnp.int32, (rows, width), 0) == rows - 1
    u = dy * y - scaled * z + jnp.where(at_end, extra, 0.0)
    pick = (
        lax.broadcasted_iota(jnp.int32, (width, LANES), 0) // P_SIZE
        == lax.broadcasted_iota(jnp.int32, (width, LANES), 1)
    ).astype(f32)
    dcumul = mm_high(u, pick)
    suffix = jnp.where(c >= r, 1.0, 0.0).astype(f32)
    ddecay = mm_high(suffix, dcumul)
    dstep = (mm_high(inner * z, pick) + neg_rate * ddecay) * jax.nn.sigmoid(step_in)
    dstep_ref[...] = dstep.T[: dstep_ref.shape[0]].astype(bf16)
    dhead_ref[0:1] += jnp.sum(dstep, axis=0, keepdims=True)
    dhead_ref[1:2] += jnp.sum(decay_log * ddecay, axis=0, keepdims=True)

    dinner = dt_x * z + skip * dy
    dscores2 = two_parts(dscores_t)
    edy2 = two_parts(ecum * dy)
    db = mm3(dscores2, c2, NN) + mm3(two_parts(tail * scaled), ds2, NT)
    dc = mm3(dscores2, b2, TN) + mm3(edy2, s2, NT)
    dstate[...] = elast * ds + mm3(c2, edy2, TN)

    dconv = jnp.concatenate([db, dc, dinner], axis=1) * dsilu
    dcat[0:rows] = dconv
    draw = taps_ref[3:4] * dconv
    for k in range(3):
        draw = draw + taps_ref[k : k + 1] * dcat[3 - k : 3 - k + rows]
    for k in range(4):
        dtaps_ref[k : k + 1] += jnp.sum(
            dconv * cat[5 + k : 5 + k + rows], axis=0, keepdims=True
        )
    dtaps_ref[4:5] += jnp.sum(dconv, axis=0, keepdims=True)
    dtaps_ref[5:6, 2 * N_STATE :] += jnp.sum(dy * inner, axis=0, keepdims=True)
    dcat[rows : rows + 8] = dconv[0:8]
    dshared_ref[...] = draw[:, : 2 * N_STATE].T.astype(bf16)
    dmain_ref[...] = join_pairs(dgate, draw[:, 2 * N_STATE :], heads).astype(bf16)


def mixer_backward(proj, sel, head, taps, y, states, dgated, heads):
    length, width = y.shape
    count = length // CHUNK
    all_w = width + 2 * N_STATE
    per = CHUNK // 16

    def at(i):
        return (count - 1 - i, 0)

    small_at = 2 * width // (3 * LANES)

    def at_small(i):
        return (count - 1 - i, small_at)

    def before(i):
        return (jnp.maximum((count - 1 - i) * per - 1, 0), 0)

    def before_small(i):
        return (jnp.maximum((count - 1 - i) * per - 1, 0), small_at)

    def fixed(i):
        return (0, 0)

    return pl.pallas_call(
        functools.partial(bwd_kernel, heads, count),
        grid=(count,),
        in_specs=[
            pl.BlockSpec((CHUNK, 2 * width), at),
            pl.BlockSpec((CHUNK, 3 * LANES), at_small),
            pl.BlockSpec((16, 2 * width), before),
            pl.BlockSpec((16, 3 * LANES), before_small),
            pl.BlockSpec((LANES, LANES), fixed),
            pl.BlockSpec((8, LANES), fixed),
            pl.BlockSpec((8, all_w), fixed),
            pl.BlockSpec((CHUNK, width), at),
            pl.BlockSpec((1, N_STATE, width), lambda i: (count - 1 - i, 0, 0)),
            pl.BlockSpec((CHUNK, width), at),
        ],
        out_specs=[
            pl.BlockSpec((CHUNK, 2 * width), at),
            pl.BlockSpec((2 * N_STATE, CHUNK), lambda i: (0, count - 1 - i)),
            pl.BlockSpec((STEP_ROWS, CHUNK), lambda i: (0, count - 1 - i)),
            pl.BlockSpec((8, all_w), fixed),
            pl.BlockSpec((8, LANES), fixed),
        ],
        out_shape=[
            jax.ShapeDtypeStruct((length, 2 * width), bf16),
            jax.ShapeDtypeStruct((2 * N_STATE, length), bf16),
            jax.ShapeDtypeStruct((STEP_ROWS, length), bf16),
            jax.ShapeDtypeStruct((8, all_w), f32),
            jax.ShapeDtypeStruct((8, LANES), f32),
        ],
        scratch_shapes=[
            pltpu.VMEM((N_STATE, width), f32),
            pltpu.VMEM((CHUNK + 8, all_w), f32),
            pltpu.VMEM((CHUNK + 8, all_w), f32),
        ],
        cost_estimate=pl.CostEstimate(
            flops=0, bytes_accessed=160_000_000, transcendentals=0
        ),
        name="mixer_backward",
    )(proj, proj, proj, proj, sel, head, taps, y, states, dgated)


MESH = pl.DeviceIdType.MESH


def greet(peers, count):
    barrier = pltpu.get_barrier_semaphore()
    for peer in peers:
        pl.semaphore_signal(barrier, inc=1, device_id=peer, device_id_type=MESH)
    pl.semaphore_wait(barrier, count)


def wire(src, dst, send, recv, peer):
    return pltpu.make_async_remote_copy(
        src_ref=src,
        dst_ref=dst,
        send_sem=send,
        recv_sem=recv,
        device_id=peer,
        device_id_type=MESH,
    )


def weights_kernel(n_seq, n_wsh, main, small, w_all, *sems):
    send_a, recv_a, send_b, recv_b, send_e, recv_e, send_r, recv_r, send_l, recv_l, own = sems
    cols = main.shape[2]

    def main_at(i, j):
        return w_all.at[i, j, :, :cols]

    def small_at(i, j):
        return w_all.at[i, j, :, cols:]

    s = lax.axis_index("seq")
    w = lax.axis_index("wshard")
    row = [(lax.rem(s + k, n_seq), w) for k in range(1, n_seq)]
    col = [(s, lax.rem(w + j, n_wsh)) for j in range(1, n_wsh)]
    greet(row + col, n_seq + n_wsh - 2)
    first = [
        wire(main.at[peer[0]], main_at(s, w), send_a.at[k], recv_a.at[k], peer)
        for k, peer in enumerate(row)
    ]
    spread = [
        wire(small, small_at(s, w), send_b.at[j], recv_b.at[j], peer)
        for j, peer in enumerate(col)
    ]
    plane = w_all.at[s, :, :, cols:]
    third = [
        wire(plane, plane, send_e.at[k], recv_e.at[k], peer)
        for k, peer in enumerate(row)
    ]
    mine = [
        pltpu.make_async_copy(main.at[s], main_at(s, w), own.at[0]),
        pltpu.make_async_copy(small, small_at(s, w), own.at[1]),
    ]

    def right(t):
        block = w_all.at[:, jnp.maximum(w - t, 0), :, :cols]
        peer = (s, jnp.minimum(w + 1, n_wsh - 1))
        return wire(block, block, send_r.at[t], recv_r.at[t], peer)

    def left(t):
        block = w_all.at[:, jnp.minimum(w + t, n_wsh - 1), :, :cols]
        peer = (s, jnp.maximum(w - 1, 0))
        return wire(block, block, send_l.at[t], recv_l.at[t], peer)

    for copy in mine + first + spread:
        copy.start()
    mine[0].wait()
    for copy in first:
        copy.wait_recv()
    last = n_wsh - 1
    for t in range(n_wsh):
        if t > 0:
            pl.when(w >= t)(lambda t=t: right(t - 1).wait_recv())
        if t < last:
            pl.when((w >= t) & (w < last))(lambda t=t: right(t).start())
        if t > 0:
            pl.when(w + t <= last)(lambda t=t: left(t - 1).wait_recv())
        if t < last:
            pl.when((w + t <= last) & (w > 0))(lambda t=t: left(t).start())
        if t == 0:
            mine[1].wait()
            for copy in spread:
                copy.wait_recv()
            for copy in third:
                copy.start()
    for copy in first + spread:
        copy.wait_send()
    for copy in third:
        copy.wait()
    for t in range(last):
        pl.when((w >= t) & (w < last))(lambda t=t: right(t).wait_send())
        pl.when((w + t <= last) & (w > 0))(lambda t=t: left(t).wait_send())


def spread_weights(main, small, n_seq, n_wsh):
    rows_in, cols = main.shape[1:]
    anywhere = pl.BlockSpec(memory_space=pl.ANY)
    dma = pltpu.SemaphoreType.DMA
    a, c = n_seq - 1, n_wsh - 1
    return pl.pallas_call(
        functools.partial(weights_kernel, n_seq, n_wsh),
        in_specs=[anywhere] * 2,
        out_specs=anywhere,
        out_shape=jax.ShapeDtypeStruct(
            (n_seq, n_wsh, rows_in, cols + small.shape[1]), bf16
        ),
        scratch_shapes=[dma((n,)) for n in (a, a, c, c, a, a, c, c, c, c, 2)],
        compiler_params=pltpu.CompilerParams(collective_id=0, has_side_effects=True),
        cost_estimate=pl.CostEstimate(
            flops=0, bytes_accessed=200_000_000, transcendentals=0
        ),
        name="spread_weights",
    )(main, small)


def swap_kernel(plan, n_seq, n_wsh, *refs):
    n = len(plan)
    ins, outs, sems = refs[:n], refs[n : 2 * n], refs[2 * n :]
    s = lax.axis_index("seq")
    w = lax.axis_index("wshard")
    total = n_seq * n_wsh
    me_all = s * n_wsh + w
    size = {"seq": n_seq, "wshard": n_wsh, "both": total}
    me_of = {"seq": s, "wshard": w, "both": me_all}

    def peer_at(axis, k):
        if axis == "seq":
            index = lax.rem(s + k, n_seq)
            return index, (index, w)
        if axis == "wshard":
            index = lax.rem(w + k, n_wsh)
            return index, (s, index)
        index = lax.rem(me_all + k, total)
        return index, (lax.div(index, n_wsh), lax.rem(index, n_wsh))

    def block(kind, ref, index):
        if kind == "all":
            return ref
        return ref.at[index] if kind == 0 else ref.at[:, index]

    def copy_of(i, k):
        kind, axis = plan[i]
        index, peer = peer_at(axis, k)
        return wire(
            block(kind, ins[i], index),
            outs[i].at[me_of[axis]],
            sems[3 * i].at[k],
            sems[3 * i + 1].at[k],
            peer,
        )

    widest = "both" if any(axis == "both" for _, axis in plan) else plan[0][1]
    barrier = pltpu.get_barrier_semaphore()

    def hail(k, _):
        pl.semaphore_signal(
            barrier, inc=1, device_id=peer_at(widest, k)[1], device_id_type=MESH
        )
        return 0

    lax.fori_loop(1, size[widest], hail, 0)
    pl.semaphore_wait(barrier, size[widest] - 1)
    own = []
    for i, (kind, axis) in enumerate(plan):
        me = me_of[axis]
        own.append(
            pltpu.make_async_copy(
                block(kind, ins[i], me), outs[i].at[me], sems[3 * i + 2].at[0]
            )
        )

        def begin(k, _, i=i):
            copy_of(i, k).start()
            return 0

        lax.fori_loop(1, size[axis], begin, 0)
    for copy in own:
        copy.start()
    for i, (kind, axis) in enumerate(plan):
        own[i].wait()

        def finish(k, _, i=i):
            copy_of(i, k).wait()
            return 0

        lax.fori_loop(1, size[axis], finish, 0)


def swap(arrays, plan, n_seq, n_wsh, collective_id):
    anywhere = pl.BlockSpec(memory_space=pl.ANY)
    size = {"seq": n_seq, "wshard": n_wsh, "both": n_seq * n_wsh}
    shapes, sems = [], []
    for x, (kind, axis) in zip(arrays, plan):
        n = size[axis]
        shape = x.shape
        if kind == 0:
            shape = shape[1:]
        elif kind == 1:
            shape = shape[:1] + shape[2:]
        shapes.append(jax.ShapeDtypeStruct((n,) + shape, x.dtype))
        sems += [
            pltpu.SemaphoreType.DMA((n,)),
            pltpu.SemaphoreType.DMA((n,)),
            pltpu.SemaphoreType.DMA((1,)),
        ]
    return pl.pallas_call(
        functools.partial(swap_kernel, plan, n_seq, n_wsh),
        in_specs=[anywhere] * len(arrays),
        out_specs=[anywhere] * len(arrays),
        out_shape=shapes,
        scratch_shapes=sems,
        compiler_params=pltpu.CompilerParams(
            collective_id=collective_id, has_side_effects=True
        ),
    )(*arrays)


def stats_kernel(n_seq, x_ref, out_ref, slots, send, recv):
    s = lax.axis_index("seq")
    w = lax.axis_index("wshard")
    row = [(lax.rem(s + k, n_seq), w) for k in range(1, n_seq)]
    greet(row, n_seq - 1)
    copies = [
        wire(x_ref, slots.at[s], send.at[k], recv.at[k], peer)
        for k, peer in enumerate(row)
    ]
    for copy in copies:
        copy.start()
    slots[s] = x_ref[...]
    for copy in copies:
        copy.wait()
    total = slots[0]
    for k in range(1, n_seq):
        total = total + slots[k]
    out_ref[...] = total


def sum_over_seq(x, n_seq):
    vmem = pl.BlockSpec(memory_space=pltpu.VMEM)
    dma = pltpu.SemaphoreType.DMA
    return pl.pallas_call(
        functools.partial(stats_kernel, n_seq),
        in_specs=[vmem],
        out_specs=vmem,
        out_shape=jax.ShapeDtypeStruct(x.shape, f32),
        scratch_shapes=[
            pltpu.VMEM((n_seq,) + x.shape, f32),
            dma((n_seq - 1,)),
            dma((n_seq - 1,)),
        ],
        compiler_params=pltpu.CompilerParams(collective_id=1, has_side_effects=True),
        name="sum_over_seq",
    )(x)


def adamw(param, grad, first, second_moment, rate, decay):
    first_new = beta_one * first + (1.0 - beta_one) * grad
    second_new = beta_two * second_moment + (1.0 - beta_two) * grad * grad
    corrected = (
        first_new
        / (1.0 - beta_one**adam_step)
        / (jnp.sqrt(second_new / (1.0 - beta_two**adam_step)) + adam_eps)
    )
    return (param - rate * (corrected + decay * param), first_new, second_new)


def shift(x, j, n_wsh):
    return lax.ppermute(x, "wshard", [(i, (i + j) % n_wsh) for i in range(n_wsh)])


def adam_kernel(count, g_ref, ext_ref, p_ref, m_ref, v_ref, grad_ref, *out_refs):
    at_ext = pl.program_id(0) == count
    grad = jnp.where(at_ext, ext_ref[...].astype(f32), g_ref[0].astype(f32))
    grad_ref[...] = grad
    news = adamw(
        p_ref[...], grad, m_ref[...], v_ref[...], weight_learning_rate, matrix_decay
    )
    for ref, new in zip(out_refs, news):
        ref[...] = new


def adam_in(g_main, g_ext, param, first, second):
    count, rows, cols = g_main.shape
    wide = pl.BlockSpec((rows, cols), lambda i: (0, i))
    return pl.pallas_call(
        functools.partial(adam_kernel, count),
        grid=(count + 1,),
        in_specs=[
            pl.BlockSpec((1, rows, cols), lambda i: (jnp.minimum(i, count - 1), 0, 0)),
            pl.BlockSpec((rows, cols), lambda i: (0, 0)),
            wide,
            wide,
            wide,
        ],
        out_specs=[wide] * 4,
        out_shape=[jax.ShapeDtypeStruct(param.shape, f32)] * 4,
        name="adam_in",
    )(g_main, g_ext, param, first, second)


def local(
    block_in,
    cotangent,
    in_weight,
    out_weight,
    in_gain,
    out_gain,
    conv_inner,
    conv_shared,
    head_params,
    first_in_weight,
    first_out_weight,
    first_in_gain,
    first_out_gain,
    first_conv_inner,
    first_conv_shared,
    first_head_params,
    second_in_weight,
    second_out_weight,
    second_in_gain,
    second_out_gain,
    second_conv_inner,
    second_conv_shared,
    second_head_params,
):
    seq_index = lax.axis_index("seq")
    wsh_index = lax.axis_index("wshard")
    n_seq = lax.axis_size("seq")
    n_wsh = lax.axis_size("wshard")
    rows_in, _ = in_weight.shape
    rows_out = out_weight.shape[0]
    _, width_in = block_in.shape[1:]
    heads = head_params.shape[1] // n_seq
    width = heads * P_SIZE
    inner_all = out_gain.shape[0]
    share = 2 * N_STATE // n_seq

    inputs = block_in[0].astype(f32)
    rms_in = lax.rsqrt(jnp.mean(inputs * inputs, axis=-1, keepdims=True) + norm_eps)
    normed = (inputs * rms_in * in_gain).astype(bf16)
    normed_all = lax.all_gather(normed, "seq", axis=0, tiled=True)
    cot = cotangent[0]
    cot_all = lax.all_gather(cot, "seq", axis=0, tiled=True)
    in_w16 = in_weight.astype(bf16)
    main_send = in_w16[:, : 2 * inner_all].reshape(rows_in, n_seq, 2 * width)
    main_send = jnp.swapaxes(main_send, 0, 1)
    small_send = in_w16[:, 2 * inner_all :]
    small_send = jnp.pad(small_send, ((0, 0), (0, -small_send.shape[1] % LANES)))
    w_all = spread_weights(main_send, small_send, n_seq, n_wsh)
    out_w16, w_all = lax.optimization_barrier((out_weight.astype(bf16), w_all))
    w_all = w_all.reshape(width_in, 2 * width + small_send.shape[1])
    proj = mm(normed_all, w_all, NN).astype(bf16)
    w_main = w_all[:, : 2 * width]
    w_small = w_all[:, 2 * width :]
    w_out = jnp.zeros((n_wsh,) + out_w16.shape, bf16)
    w_out = lax.dynamic_update_index_in_dim(w_out, out_w16, wsh_index, 0)
    for j in range(1, n_wsh):
        got = shift(out_w16, j, n_wsh)
        w_out = lax.dynamic_update_index_in_dim(
            w_out, got, lax.rem(wsh_index - j + n_wsh, n_wsh), 0
        )
    w_out = w_out.reshape(width, width_in)

    def pick(first, count, width_to):
        col = lax.broadcasted_iota(jnp.int32, (w_small.shape[1], width_to), 0)
        lane = lax.broadcasted_iota(jnp.int32, (w_small.shape[1], width_to), 1)
        return jnp.where((col == lane + first) & (lane < count), 1.0, 0.0)

    to_step = pick(2 * N_STATE + seq_index * heads, heads, LANES)
    to_ext = jnp.concatenate(
        [pick(seq_index * share, share, share), to_step[:, :STEP_ROWS]], axis=1
    )
    w_ext = mm(w_small, to_ext.astype(bf16), NN).astype(bf16)
    sel = to_step[2 * N_STATE :].astype(bf16)

    head_local = lax.dynamic_slice_in_dim(head_params, seq_index * heads, heads, 1)
    head = jnp.pad(head_local, ((0, 5), (0, LANES - heads)))
    conv_local = lax.dynamic_slice_in_dim(conv_inner, seq_index * width, width, 1)
    taps = jnp.pad(jnp.concatenate([conv_shared, conv_local], axis=1), ((0, 3), (0, 0)))
    gain_local = lax.dynamic_slice_in_dim(out_gain, seq_index * width, width, 0)
    gated, y, states = mixer_forward(proj, sel, head, taps, heads)
    d_gnormed = mm(cot_all, w_out, NT)
    gated32 = gated.astype(f32)
    scaled = d_gnormed * gain_local
    stats = jnp.stack(
        [jnp.sum(gated32 * gated32, axis=-1), jnp.sum(scaled * gated32, axis=-1)]
    )
    stats = sum_over_seq(stats.reshape(-1, LANES), n_seq).reshape(stats.shape)
    rms_out = lax.rsqrt(stats[0] / inner_all + norm_eps)[:, None]
    mean_sg = (stats[1] / inner_all)[:, None]
    gnormed = (gated32 * rms_out * gain_local).astype(bf16)
    d_gated = (rms_out * scaled - gated32 * rms_out**3 * mean_sg).astype(bf16)
    d_out_gain = jnp.sum(d_gnormed * gated32 * rms_out, axis=0)

    g_out = mm(gnormed, cot_all, TN)
    mixed = mm(gnormed, w_out, NN).astype(bf16)
    g_out, mixed, d_gated = lax.optimization_barrier((g_out, mixed, d_gated))
    mixed = lax.psum_scatter(mixed, "seq", scatter_dimension=0, tiled=True)
    out_parts = [lax.dynamic_slice_in_dim(g_out, wsh_index * rows_out, rows_out, 0)]
    for j in range(1, n_wsh):
        to = lax.rem(wsh_index + j, n_wsh)
        part = lax.dynamic_slice_in_dim(g_out, to * rows_out, rows_out, 0)
        out_parts.append(shift(part, j, n_wsh))
    dmain, dshared_t, dstep_t, dtaps, dhead = mixer_backward(
        proj, sel, head, taps, y, states, d_gated, heads
    )

    g_main = mm(normed_all, dmain, TN)
    d_gain_part = jnp.sum(g_main * w_main.astype(f32), axis=1)
    g_main, dmain = lax.optimization_barrier((g_main.astype(bf16), dmain))
    g_main = g_main.reshape(n_seq, n_wsh, rows_in, 2 * width)
    g_parts = [lax.dynamic_index_in_dim(g_main, wsh_index, 1, keepdims=False)]
    for j in range(1, n_wsh):
        to = lax.rem(wsh_index + j, n_wsh)
        part = lax.dynamic_index_in_dim(g_main, to, 1, keepdims=False)
        g_parts.append(shift(part, j, n_wsh))

    (shared_parts,) = swap(
        (dshared_t.reshape(n_seq, share, -1),), ((0, "seq"),), n_seq, n_wsh, 2
    )
    shared_sum = jnp.sum(shared_parts.astype(f32), axis=0).astype(bf16)
    d_ext = jnp.concatenate([shared_sum, dstep_t], axis=0)
    d_normed = mm(dmain, w_main, NT) + lax.dot_general(
        d_ext, w_ext, (((0,), (1,)), ((), ())), preferred_element_type=f32
    )
    d_normed, mixed = lax.optimization_barrier((d_normed.astype(bf16), mixed))
    block_out = (inputs + mixed.astype(f32))[None]
    d_normed = lax.psum_scatter(d_normed, "seq", scatter_dimension=0, tiled=True)
    d_normed = d_normed.astype(f32)
    scaled_in = d_normed * in_gain
    grad_in = (
        cot.astype(f32)
        + rms_in * scaled_in
        - inputs * rms_in**3 * jnp.mean(scaled_in * inputs, axis=-1, keepdims=True)
    )[None]

    g_ext = lax.dot_general(
        normed_all, d_ext, (((0,), (1,)), ((), ())), preferred_element_type=f32
    )
    d_gain_part = d_gain_part + jnp.sum(g_ext * w_ext.astype(f32), axis=1)
    g_ext = jnp.pad(g_ext.astype(bf16), ((0, 0), (0, -g_ext.shape[1] % LANES)))
    g_ext = g_ext.reshape(n_seq, n_wsh, rows_in, LANES)

    d_skip = dtaps[5, 2 * N_STATE :].reshape(heads, P_SIZE).sum(-1)
    d_head = jnp.concatenate([dhead[:2, :heads], d_skip[None]], axis=0)
    pieces = (
        d_gain_part,
        dtaps[:5, : 2 * N_STATE],
        d_out_gain,
        dtaps[:5, 2 * N_STATE :],
        d_head,
    )
    flat = jnp.concatenate([p.reshape(-1) for p in pieces])
    flat = jnp.pad(flat, (0, -flat.shape[0] % (8 * LANES))).reshape(-1, LANES)
    g_ext, flat = swap(
        (g_ext, flat), ((1, "wshard"), ("all", "wshard")), n_seq, n_wsh, 3
    )
    g_ext = jnp.sum(g_ext.astype(f32), axis=0)
    (flat,) = swap((jnp.sum(flat, axis=0),), (("all", "seq"),), n_seq, n_wsh, 4)
    flat = flat.reshape(n_seq, -1)
    sums, at = [], 0
    for p in pieces:
        sums.append(flat[:, at : at + p.size].reshape((n_seq,) + p.shape))
        at += p.size
    grad_in_gain = jnp.sum(sums[0], axis=0) / in_gain
    grad_conv_shared = jnp.sum(sums[1], axis=0)
    grad_out_gain = sums[2].reshape(-1)
    grad_conv_inner = jnp.swapaxes(sums[3], 0, 1).reshape(conv_inner.shape)
    grad_head_params = jnp.swapaxes(sums[4], 0, 1).reshape(head_params.shape)

    flat, out_parts = lax.optimization_barrier((flat, out_parts))
    grad_out_weight = sum(out_parts)
    new_out_weight, new_first_out_weight, new_second_out_weight = adamw(
        out_weight,
        grad_out_weight,
        first_out_weight,
        second_out_weight,
        weight_learning_rate,
        matrix_decay,
    )
    ready = (new_out_weight, new_first_out_weight, new_second_out_weight, grad_out_weight)
    ready, g_parts = lax.optimization_barrier((ready, g_parts))
    new_out_weight, new_first_out_weight, new_second_out_weight, grad_out_weight = ready
    g_main = g_parts[0].astype(f32)
    for part in g_parts[1:]:
        g_main = g_main + part.astype(f32)
    g_main, g_ext = swap(
        (g_main.astype(bf16), g_ext.astype(bf16)),
        ((0, "seq"), (0, "seq")),
        n_seq,
        n_wsh,
        5,
    )
    g_ext = jnp.swapaxes(g_ext, 0, 1)
    g_ext = jnp.concatenate(
        [
            g_ext[:, :, :share].reshape(rows_in, 2 * N_STATE),
            g_ext[:, :, share : share + heads].reshape(rows_in, heads * n_seq),
        ],
        axis=1,
    )
    g_ext = jnp.pad(g_ext, ((0, 0), (0, 2 * width - g_ext.shape[1])))
    grad_in_weight, new_in_weight, new_first_in_weight, new_second_in_weight = adam_in(
        g_main, g_ext, in_weight, first_in_weight, second_in_weight
    )
    updated_input_gain, new_first_in_gain, new_second_in_gain = adamw(
        in_gain, grad_in_gain, first_in_gain, second_in_gain, small_rate, 0.0
    )
    new_out_gain, new_first_out_gain, new_second_out_gain = adamw(
        out_gain, grad_out_gain, first_out_gain, second_out_gain, small_rate, 0.0
    )
    new_conv_inner, new_first_conv_inner, new_second_conv_inner = adamw(
        conv_inner, grad_conv_inner, first_conv_inner, second_conv_inner, small_rate, 0.0
    )
    new_conv_shared, new_first_conv_shared, new_second_conv_shared = adamw(
        conv_shared, grad_conv_shared, first_conv_shared, second_conv_shared, small_rate, 0.0
    )
    new_head_params, updated_head_first_moment, head_second_all = adamw(
        head_params, grad_head_params, first_head_params, second_head_params, small_rate, 0.0
    )
    return (
        block_out,
        grad_in,
        grad_in_weight,
        grad_out_weight,
        grad_in_gain,
        grad_out_gain,
        grad_conv_inner,
        grad_conv_shared,
        grad_head_params,
        new_in_weight,
        new_out_weight,
        updated_input_gain,
        new_out_gain,
        new_conv_inner,
        new_conv_shared,
        new_head_params,
        new_first_in_weight,
        new_first_out_weight,
        new_first_in_gain,
        new_first_out_gain,
        new_first_conv_inner,
        new_first_conv_shared,
        updated_head_first_moment,
        new_second_in_weight,
        new_second_out_weight,
        new_second_in_gain,
        new_second_out_gain,
        new_second_conv_inner,
        new_second_conv_shared,
        head_second_all[0:2],
        head_second_all[2],
    )


def solution(mesh):
    return jax.shard_map(
        local,
        mesh=mesh,
        in_specs=(
            P("wshard", "seq", None),
            P("wshard", "seq", None),
            P(("seq", "wshard"), None),
            P(("seq", "wshard"), None),
            P(),
            P(),
            P(),
            P(),
            P(),
            P(("seq", "wshard"), None),
            P(("seq", "wshard"), None),
            P(),
            P(),
            P(),
            P(),
            P(),
            P(("seq", "wshard"), None),
            P(("seq", "wshard"), None),
            P(),
            P(),
            P(),
            P(),
            P(),
        ),
        out_specs=(
            P("wshard", "seq", None),
            P("wshard", "seq", None),
            P(("seq", "wshard"), None),
            P(("seq", "wshard"), None),
            P(),
            P(),
            P(),
            P(),
            P(),
            P(("seq", "wshard"), None),
            P(("seq", "wshard"), None),
            P(),
            P(),
            P(),
            P(),
            P(),
            P(("seq", "wshard"), None),
            P(("seq", "wshard"), None),
            P(),
            P(),
            P(),
            P(),
            P(),
            P(("seq", "wshard"), None),
            P(("seq", "wshard"), None),
            P(),
            P(),
            P(),
            P(),
            P(),
            P(),
        ),
        check_vma=False,
    )
```
